32 devices in a mesh: gx: 4 (over z), gy: 4 (over x, core), gz: 2 (over y).
Axes of the slice: x: 2, y: 2, z: 4, core: 2. Of those that a mesh axis runs over, the one named last changes fastest.
Arguments:
- coords: float32 [3, 4, 1024, 128], P(None, 'gx', ('gy', 'gz')), may hold values from 0 to 11
- charges: float32 [4, 1024, 128], P('gx', ('gy', 'gz')), may hold values from -1.5 to 1.5
- atom_types: int32 [4, 1024, 128], P('gx', ('gy', 'gz')), may hold values from 0 to 63
- lj_sigma: float32 [64], replicated, may hold values from 2 to 4
- lj_epsilon: float32 [64], replicated, may hold values from 0.02 to 0.25
- tile_list: int32 [4, 4, 2, 2, 512], P('gx', 'gy', 'gz'), may hold values from -1 to 3455, as said below
Outputs:
- forces: float32 [3, 4, 1024, 128], P(None, 'gx', ('gy', 'gz'))
The draws below stay inside these ranges and needn't reach their ends.
Inputs may be any that keep to these rules, and one draw needn't show every extreme that they name: tile_list[x, y, z, 0, t] is a block of brick (x, y, z) (0 to 127) and tile_list[x, y, z, 1, t] a block of its neighbourhood whose cell touches the home block's cell or is that cell (cell indices differ by at most one along each dimension, counted across brick faces periodically); on each brick the listed tiles come first and the remaining slots hold -1 in both rows; at least 256 tiles are listed on every brick and all 512 on some brick; tiles may repeat.
All inputs are finite; a program needn't handle non-finite values.
Results may differ from the reference program's by a relative error of at most 0.0003.
Values sent between devices are 32-bit elements; how exact they have to be, the bound alone decides.
A program may use at most 128 MiB of HBM per device.

```python
import math
import jax
import jax.numpy as jnp
from jax import lax

GRID = 4
LAYERS = 8
BLOCKS = 128
TILES = 512
TYPES = 64
ATOMS_BLOCK = 128
SLAB = 1024
N_GX = 4
N_GY = 4
N_GZ = 2


def draw_tile_list(key, part):
    devices = N_GX * N_GY * N_GZ
    key_home, key_step, key_count, key_full = jax.random.split(jax.random.fold_in(key, 7), 4)
    home_ids = jax.random.randint(key_home, (devices, TILES), 0, BLOCKS)
    step = jax.random.randint(key_step, (devices, TILES), 0, 27)
    cell_x = home_ids // (GRID * LAYERS) + step // 9 - 1
    cell_y = home_ids // LAYERS % GRID + step // 3 % 3 - 1
    cell_z = home_ids % LAYERS + step % 3 - 1
    off_x = (cell_x >= GRID).astype(jnp.int32) - (cell_x < 0).astype(jnp.int32)
    off_y = (cell_y >= GRID).astype(jnp.int32) - (cell_y < 0).astype(jnp.int32)
    off_z = (cell_z >= LAYERS).astype(jnp.int32) - (cell_z < 0).astype(jnp.int32)
    cell_x = cell_x - off_x * GRID
    cell_y = cell_y - off_y * GRID
    cell_z = cell_z - off_z * LAYERS
    slot = 9 * (off_x + 1) + 3 * (off_y + 1) + (off_z + 1)
    source_ids = slot * BLOCKS + (cell_x * GRID + cell_y) * LAYERS + cell_z
    listed = jax.random.randint(key_count, (devices,), TILES // 2, TILES + 1)
    fullest = jax.random.randint(key_full, (), 0, devices)
    listed = jnp.where(jnp.arange(devices) == fullest, TILES, listed)
    alive = jnp.arange(TILES)[None, :] < listed[:, None]
    home_ids = jnp.where(alive, home_ids, -1)
    source_ids = jnp.where(alive, source_ids, -1)
    return jnp.stack([home_ids, source_ids], 1).reshape(N_GX, N_GY, N_GZ, 2, TILES).astype(jnp.int32)


def touch_ends(values, own_key, least, largest):
    index_at = [jax.random.randint(jax.random.fold_in(own_key, axis), (), 0, length) for axis, length in enumerate(values.shape)]
    main_axis = values.shape.index(max(values.shape))
    next_to = index_at[:main_axis] + [(index_at[main_axis] + 1) % values.shape[main_axis]] + index_at[main_axis + 1:]
    return values.at[tuple(index_at)].set(least).at[tuple(next_to)].set(largest)


def block_levels(own_key, extent, cuts, least, largest):
    def one(position, parts):
        draws = jax.random.uniform(jax.random.fold_in(jax.random.fold_in(own_key, 6), position), (parts,), jnp.float32, least / len(cuts), largest / len(cuts))
        return jnp.repeat(jnp.exp(draws), extent[position] // parts).reshape((-1,) + (1,) * (len(extent) - position - 1))

    gain = one(*cuts[0])
    for cut in cuts[1:]:
        gain = gain * one(*cut)
    return gain


def normal_values(own_key, extent, spread, bound, shards=(), kind=jnp.bfloat16):
    array = spread * jax.random.normal(own_key, extent, jnp.float32)
    if shards:
        array = array * block_levels(own_key, extent, shards, -0.22, 0.18)
    return jnp.clip(array, -bound, bound).astype(kind)


def setup_inputs(seed: int = 0) -> dict:
    splits = jax.random.split(jax.random.key(seed), 7)
    return {
        "coords": jnp.clip(11.0 * jax.random.uniform(splits[0], (3, N_GX, SLAB, ATOMS_BLOCK), jnp.float32) ** block_levels(splits[0], (3, N_GX, SLAB, ATOMS_BLOCK), ((1, 4), (2, 8)), -0.2, 0.2), 0.0, 11.0),
        "charges": normal_values(splits[1], (N_GX, SLAB, ATOMS_BLOCK), 0.3, 1.5, ((0, 4), (1, 8)), jnp.float32),
        "atom_types": touch_ends(jax.random.randint(splits[2], (N_GX, SLAB, ATOMS_BLOCK), 0, TYPES), jax.random.fold_in(splits[2], 1), 0, TYPES - 1).astype(jnp.int32),
        "lj_sigma": jnp.clip(jax.random.uniform(splits[3], (TYPES,), jnp.float32, 2.0, 4.0), 2.0, 4.0),
        "lj_epsilon": jnp.clip(jnp.exp(jax.random.uniform(splits[4], (TYPES,), jnp.float32, math.log(0.02), math.log(0.25))), 0.02, 0.25),
        "tile_list": draw_tile_list(jax.random.fold_in(splits[6], 71), 0),
    }


cell_edge = 11.0
cutoff = 9.0
soft_core = 16.0
coulomb = 332.0636

def radial(softened, sigma_pair, eps_pair, charge_pair):
    ratio = sigma_pair * sigma_pair / softened
    cubed = ratio * ratio * ratio
    return 24.0 * eps_pair * (2.0 * cubed * cubed - cubed) / softened + charge_pair / (softened * jnp.sqrt(softened))

def tile_forces(home_block, source_block):
    delta = home_block[:3, :, :, None] - source_block[:3, :, None, :]
    dist_sq = lax.optimization_barrier(jnp.sum(delta * delta, axis=0))
    softened = dist_sq + soft_core
    sigma_pair = 0.5 * (home_block[4][:, :, None] + source_block[4][:, None, :])
    eps_pair = home_block[5][:, :, None] * source_block[5][:, None, :]
    charge_pair = coulomb * home_block[3][:, :, None] * source_block[3][:, None, :]
    limit = jnp.full_like(softened, cutoff * cutoff + soft_core)
    shifted = radial(softened, sigma_pair, eps_pair, charge_pair) - radial(limit, sigma_pair, eps_pair, charge_pair)
    strength = jnp.where(dist_sq < cutoff * cutoff, shifted, jnp.zeros_like(shifted))
    return lax.optimization_barrier(jnp.sum(strength[None] * delta, axis=3))

def brick_forces(home_atoms, region, tile_ids):
    count = tile_ids.shape[1]
    group = min(64, count)
    grouped = tile_ids.reshape(2, count // group, group).transpose(1, 0, 2)
    blocks = home_atoms.shape[1]
    rows = jnp.arange(blocks, dtype=jnp.int32)

    def advance(totals, pair_ids):
        home_block = jnp.take(home_atoms, jnp.maximum(pair_ids[0], 0), axis=1)
        source_block = jnp.take(region, jnp.maximum(pair_ids[1], 0), axis=1)
        pushes = tile_forces(home_block, source_block)
        selector = (pair_ids[0][None, :] == rows[:, None]).astype(totals.dtype)
        added = jnp.einsum('bg,cga->cba', selector, pushes, precision=lax.Precision.HIGHEST)
        return (totals + added, None)
    start = jnp.zeros((3,) + home_atoms.shape[1:], home_atoms.dtype)
    return lax.scan(advance, start, grouped)[0]

def cell_corners(dtype, grid, layers):
    block = jnp.arange(grid * grid * layers, dtype=jnp.int32)
    return jnp.stack([block // (grid * layers), block // layers % grid, block % layers]).astype(dtype) * cell_edge

def slot_offsets(dtype, grid, layers):
    slot = jnp.arange(27, dtype=jnp.int32)
    steps = jnp.stack([(slot // 9 - 1) * grid, (slot // 3 % 3 - 1) * grid, (slot % 3 - 1) * layers])
    return steps.astype(dtype) * cell_edge

def reference(coords, charges, atom_types, lj_sigma, lj_epsilon, tile_list):
    atoms = jnp.concatenate([coords, charges[None], lj_sigma[atom_types][None], jnp.sqrt(lj_epsilon)[atom_types][None]], 0)
    per_brick = atoms.reshape(6, N_GX, BLOCKS, N_GY, N_GZ, ATOMS_BLOCK).transpose(1, 3, 4, 0, 2, 5)
    corners = cell_corners(coords.dtype, GRID, LAYERS)
    per_brick = jnp.concatenate([per_brick[:, :, :, :3] + corners[:, :, None], per_brick[:, :, :, 3:]], 3)
    offsets = slot_offsets(coords.dtype, GRID, LAYERS)
    slots = jnp.arange(27, dtype=jnp.int32)

    def one_brick(brick):
        xpos = brick // (N_GY * N_GZ)
        ypos = brick // N_GZ % N_GY
        zpos = brick % N_GZ
        nearby = per_brick[(xpos + slots // 9 - 1) % N_GX, (ypos + slots // 3 % 3 - 1) % N_GY, (zpos + slots % 3 - 1) % N_GZ]
        region = jnp.concatenate([nearby[:, :3] + offsets.T[:, :, None, None], nearby[:, 3:]], 1)
        region = region.transpose(1, 0, 2, 3).reshape(6, 27 * BLOCKS, ATOMS_BLOCK)
        return brick_forces(per_brick[xpos, ypos, zpos], region, tile_list[xpos, ypos, zpos])
    result = lax.map(one_brick, jnp.arange(N_GX * N_GY * N_GZ, dtype=jnp.int32))
    result = result.reshape(N_GX, N_GY, N_GZ, 3, BLOCKS, ATOMS_BLOCK).transpose(3, 0, 4, 1, 2, 5)
    return result.reshape(3, N_GX, BLOCKS * N_GY * N_GZ, ATOMS_BLOCK)
```

```python
import itertools
import math

import jax
import jax.numpy as jnp
from jax import lax
from jax.experimental import pallas as pl
from jax.experimental.pallas import tpu as pltpu
from jax.sharding import PartitionSpec as P

GRID = 4
ROWS = 8
BATCH = 8

cell_edge = 11.0
cutoff = 9.0
soft_core = 16.0
coulomb = 332.0636
limit = cutoff * cutoff + soft_core
sigma_scale = 0.5 * 2.0 ** (1.0 / 6.0)
charge_scale = (coulomb / 12.0) ** 0.5


def exchange_kernel(atoms, region, send_own, recv_own, send_rim, recv_rim, own_sem):
    stride, ranks = atoms.shape[:2]
    layers = region.shape[2] - 2
    spans = [lax.axis_size(name) for name in ("gx", "gy", "gz")]
    here = [lax.axis_index(name) for name in ("gx", "gy", "gz")]
    me = here[1] * spans[2] + here[2]
    chunk = math.gcd(stride, layers)
    pieces = stride // chunk

    def place(piece):
        cell = me * stride + piece * chunk
        return region.at[
            cell // (GRID * layers) + 1,
            lax.rem(cell // layers, GRID) + 1,
            pl.ds(lax.rem(cell, layers) + 1, chunk),
        ]

    copies = []
    for hop in range(1, ranks):
        to = lax.rem(me + hop, ranks)
        for piece in range(pieces):
            sem = (hop - 1) * pieces + piece
            copies.append(
                pltpu.make_async_remote_copy(
                    src_ref=atoms.at[pl.ds(piece * chunk, chunk), to],
                    dst_ref=place(piece),
                    send_sem=send_own.at[sem],
                    recv_sem=recv_own.at[sem],
                    device_id=(here[0], to // spans[2], lax.rem(to, spans[2])),
                    device_id_type=pl.DeviceIdType.MESH,
                )
            )
            copies[-1].start()
    for piece in range(pieces):
        kept = pltpu.make_async_copy(
            atoms.at[pl.ds(piece * chunk, chunk), me], place(piece), own_sem.at[piece]
        )
        kept.start()
        copies.append(kept)
    for copy in copies:
        copy.wait()

    lengths = (GRID, GRID, layers)
    rims = []
    offsets = [o for o in itertools.product((-1, 0, 1), repeat=3) if any(o)]
    for sem, offset in enumerate(offsets):
        source = tuple(
            pl.ds(1, n) if o == 0 else pl.ds(n if o > 0 else 1, 1)
            for o, n in zip(offset, lengths)
        )
        target = tuple(
            pl.ds(1, n) if o == 0 else pl.ds(0 if o > 0 else n + 1, 1)
            for o, n in zip(offset, lengths)
        )
        rims.append(
            pltpu.make_async_remote_copy(
                src_ref=region.at[source],
                dst_ref=region.at[target],
                send_sem=send_rim.at[sem],
                recv_sem=recv_rim.at[sem],
                device_id=tuple(
                    lax.rem(at + o + n, n) for at, o, n in zip(here, offset, spans)
                ),
                device_id_type=pl.DeviceIdType.MESH,
            )
        )
        rims[-1].start()
    for copy in rims:
        copy.wait()


def exchanged(atoms, layers):
    stride, ranks, rows, width = atoms.shape
    pieces = stride // math.gcd(stride, layers)
    own = pltpu.SemaphoreType.DMA(((ranks - 1) * pieces,))
    rim = pltpu.SemaphoreType.DMA((26,))
    return pl.pallas_call(
        exchange_kernel,
        out_shape=jax.ShapeDtypeStruct(
            (GRID + 2, GRID + 2, layers + 2, rows, width), atoms.dtype
        ),
        in_specs=[pl.BlockSpec(memory_space=pltpu.VMEM)],
        out_specs=pl.BlockSpec(memory_space=pltpu.VMEM),
        scratch_shapes=[own, own, rim, rim, pltpu.SemaphoreType.DMA((pieces,))],
        compiler_params=pltpu.CompilerParams(has_side_effects=True),
    )(atoms)


def split(value):
    high = value.astype(jnp.bfloat16).astype(jnp.float32)
    rest = value - high
    middle = rest.astype(jnp.bfloat16).astype(jnp.float32)
    return high, middle, rest - middle


def stacked(parts):
    return jnp.concatenate(parts, axis=0).astype(jnp.bfloat16)


def rows_of(shape):
    return lax.broadcasted_iota(jnp.int32, shape, 0)


def row_table(values, shape):
    rows = rows_of(shape)
    out = jnp.zeros(shape, jnp.float32)
    for k, value in enumerate(values):
        if value:
            out = jnp.where(rows == k, jnp.float32(value), out)
    return out


def rising_powers(base, rows):
    two = base * base
    four = two * two
    out = jnp.where(rows % 2 == 1, base, 1.0)
    out = out * jnp.where(rows // 2 % 2 == 1, two, 1.0)
    return out * jnp.where(rows // 4 % 2 == 1, four, 1.0)


def prepare_sources(region, sources, weights):
    shape = region.shape[1:]
    rows = rows_of(shape)
    ways = row_table([math.comb(6, k) for k in range(7)], shape)

    def one(line, carry):
        block = region[line]
        high, middle, low = split(block)
        sigma = jnp.broadcast_to(region[line, 5:6, :], shape)
        root = jnp.broadcast_to(region[line, 6:7, :], shape)
        charge = jnp.broadcast_to(region[line, 7:8, :], shape)
        terms = ways * rising_powers(sigma, 6 - jnp.minimum(rows, 6))
        top, rest, _ = split(terms)
        sources[line] = stacked([high, middle, high, middle, high, low, top, rest, top, rest])
        place = jnp.where(rows < 4, block, pltpu.roll(block, 4, 0))
        top, rest, _ = split(place * jnp.where(rows < 4, root, charge))
        weights[line] = stacked([top, rest])
        return carry

    lax.fori_loop(0, region.shape[0], one, 0, unroll=4)


def prepare_homes(region, distances, powers, scales, layers):
    shape = region.shape[1:]
    rows = rows_of(shape)
    blocks = distances.shape[0] - 1

    def one(block, carry):
        line = own_line(block, layers)
        home = region[line]
        distances[block] = jnp.where(rows < 3, -2.0 * home, jnp.where(rows == 4, 1.0, 0.0))
        top, rest, _ = split(rising_powers(jnp.broadcast_to(region[line, 5:6, :], shape), rows))
        powers[block] = stacked([top, top, rest, rest])
        root = jnp.broadcast_to(region[line, 6:7, :], shape)
        charge = jnp.broadcast_to(region[line, 7:8, :], shape)
        scales[block] = 12.0 * jnp.where(rows < 4, root, charge)
        return carry

    lax.fori_loop(0, blocks, one, 0, unroll=4)
    distances[blocks] = jnp.zeros(shape, jnp.float32)
    powers[blocks] = jnp.zeros(powers.shape[1:], powers.dtype)


def own_line(block, layers):
    x = block // (GRID * layers)
    y = lax.rem(block // layers, GRID)
    return ((x + 1) * (GRID + 2) + y + 1) * (layers + 2) + lax.rem(block, layers) + 1


def prepare_steps(offsets, shifts):
    shape = offsets.shape[1:]
    for step, cells in enumerate(itertools.product((-1, 0, 1), repeat=3)):
        moves = [cell_edge * c for c in cells]
        offsets[step] = row_table([2.0 * m for m in moves], shape)
        shifts[step] = row_table(moves + [0.0] + moves, shape)


def pair_terms(pairs, index, sources, distances, powers, offsets, terms):
    home = pairs[0, index]
    distance = distances[home] + offsets[pairs[2, index]]
    rows = rows_of(distance.shape)
    share = jnp.where(rows < 3, 0.25, jnp.where(rows == 4, soft_core, 0.0))
    square = jnp.sum(distance * distance * share, axis=0, keepdims=True)
    distance = jnp.where(rows == 3, square, distance)
    high, middle, low = split(distance)
    near = stacked([high, high, middle, middle, low, high])
    strong = powers[home]
    width = near.shape[1]
    right = jnp.concatenate(
        [
            jnp.concatenate([near, jnp.zeros((strong.shape[0], width), near.dtype)], axis=0),
            jnp.concatenate([jnp.zeros(near.shape, near.dtype), strong], axis=0),
        ],
        axis=1,
    )
    terms[...] = lax.dot_general(
        sources[pairs[1, index]],
        right,
        (((0,), (0,)), ((), ())),
        preferred_element_type=jnp.float32,
    )


def inverse_powers(softened):
    root = lax.rsqrt(softened)
    one = root * root
    near = one * root
    three = near * near
    four = three * one
    return near, four, three * four


def strengths(terms, halves, at_limit):
    width = terms.shape[0]
    near_at, four_at, seven_at = at_limit
    for start in range(0, width, 16):
        rows = pl.ds(start, 16)
        near, four, seven = inverse_powers(jnp.minimum(terms[rows, :width], limit))
        sixth = terms[rows, width:]
        pair = (
            near - near_at,
            sixth * (sixth * (seven - seven_at) - (four - four_at)),
        )
        for k, value in enumerate(pair):
            top = value.astype(jnp.bfloat16)
            halves[rows, k * width : (k + 1) * width] = top
            halves[pl.ds(width + start, 16), k * width : (k + 1) * width] = (
                value - top.astype(jnp.float32)
            ).astype(jnp.bfloat16)


def add_forces(pairs, index, weights, shifts, halves, totals):
    left = weights[pairs[1, index]]
    both = jnp.dot(
        jnp.concatenate([left, left], axis=1), halves[...], preferred_element_type=jnp.float32
    )
    both = both[:ROWS] + both[ROWS:]
    width = left.shape[1]
    rows = rows_of((ROWS, width))
    summed = jnp.where(rows < 4, both[:, width:], both[:, :width])
    plain = jnp.where(rows < 4, summed[3:4], summed[7:8])
    totals[pairs[0, index]] += summed + shifts[pairs[2, index]] * plain


def force_kernel(pairs, count, region, out, totals, sources, weights, distances, powers, scales, offsets, shifts, *slots):
    width = region.shape[2]
    blocks = out.shape[1]
    layers = blocks // (GRID * GRID)
    at_limit = inverse_powers(jnp.full((16, width), limit, jnp.float32))
    totals[...] = jnp.zeros_like(totals)
    prepare_steps(offsets, shifts)
    prepare_sources(region, sources, weights)
    prepare_homes(region, distances, powers, scales, layers)
    terms = (slots[:BATCH], slots[BATCH : 2 * BATCH])
    halves = (slots[2 * BATCH : 3 * BATCH], slots[3 * BATCH : 4 * BATCH])

    def step(index, carry):
        for turn in range(2):
            first = (2 * index + turn) * BATCH
            for t in range(BATCH):
                add_forces(pairs, first + t, weights, shifts, halves[turn][t], totals)
                strengths(terms[1 - turn][t], halves[1 - turn][t], at_limit)
                pair_terms(pairs, first + 2 * BATCH + t, sources, distances, powers, offsets, terms[turn][t])
        return carry

    groups = (count[0] + BATCH - 1) // BATCH
    lax.fori_loop(0, (groups + 3) // 2, step, 0)

    def finish(block, carry):
        home = region[own_line(block, layers)]
        rows = rows_of(home.shape)
        place = jnp.where(rows < 4, home, pltpu.roll(home, 4, 0))
        summed = totals[block]
        plain = jnp.where(rows < 4, summed[3:4], summed[7:8])
        force = (place * plain - summed) * scales[block]
        totals[block] = force + pltpu.roll(force, 4, 0)
        return carry

    lax.fori_loop(0, blocks, finish, 0, unroll=4)
    for axis in range(3):
        out[axis] = totals[:blocks, axis, :]


def brick_forces(region, pairs, count, blocks):
    lines, _, width = region.shape
    single = pltpu.VMEM((blocks + 1, ROWS, width), jnp.float32)
    table = pltpu.VMEM((27, ROWS, width), jnp.float32)
    return pl.pallas_call(
        force_kernel,
        out_shape=jax.ShapeDtypeStruct((3, blocks, width), jnp.float32),
        in_specs=[
            pl.BlockSpec(memory_space=pltpu.SMEM),
            pl.BlockSpec(memory_space=pltpu.SMEM),
            pl.BlockSpec(memory_space=pltpu.VMEM),
        ],
        out_specs=pl.BlockSpec(memory_space=pltpu.VMEM),
        scratch_shapes=[
            single,
            pltpu.VMEM((lines, 10 * ROWS, width), jnp.bfloat16),
            pltpu.VMEM((lines, 2 * ROWS, width), jnp.bfloat16),
            single,
            pltpu.VMEM((blocks + 1, 4 * ROWS, width), jnp.bfloat16),
            single,
            table,
            table,
        ]
        + [pltpu.VMEM((width, 2 * width), jnp.float32)] * (2 * BATCH)
        + [pltpu.VMEM((2 * width, 2 * width), jnp.bfloat16)] * (2 * BATCH),
    )(pairs, count, region)


def per_device(coords, charges, atom_types, lj_sigma, lj_epsilon, tile_list):
    span_y = lax.axis_size("gy")
    span_z = lax.axis_size("gz")
    blocks = coords.shape[2]
    width = coords.shape[3]
    layers = blocks // (GRID * GRID)
    ranks = span_y * span_z
    stride = blocks // ranks
    dtype = coords.dtype
    kinds = jnp.arange(lj_sigma.shape[0], dtype=jnp.int32)
    selector = (atom_types[0][:, :, None] == kinds).astype(dtype)
    sigma_atom = jnp.sum(selector * (lj_sigma * sigma_scale), axis=2)
    root_atom = jnp.sum(selector * (jnp.sqrt(lj_epsilon)), axis=2)
    inner = coords[:, 0] - 0.5 * cell_edge
    square = inner[0] * inner[0] + inner[1] * inner[1] + inner[2] * inner[2]
    atoms = jnp.stack(
        [inner[0], inner[1], inner[2], jnp.ones_like(square), square]
        + [sigma_atom, root_atom, charges[0] * charge_scale],
        axis=1,
    )
    outgoing = atoms.reshape(stride, ranks, ROWS, width)
    padded = exchanged(outgoing, layers)
    region = padded.reshape(-1, ROWS, width)
    pairs = jnp.pad(
        tile_list[0, 0, 0], ((0, 0), (2 * BATCH, 4 * BATCH)), constant_values=-1
    )
    dead = pairs[0] < 0

    def place(ids):
        slot = ids // blocks
        member = ids % blocks
        px = member // (GRID * layers) + (slot // 9 - 1) * GRID
        py = member // layers % GRID + (slot // 3 % 3 - 1) * GRID
        pz = member % layers + (slot % 3 - 1) * layers
        return px, py, pz

    own = place(jnp.where(dead, 0, pairs[0]) + 13 * blocks)
    other = place(jnp.where(dead, 13 * blocks, pairs[1]))
    x, y, z = other
    line = ((x + 1) * (GRID + 2) + y + 1) * (layers + 2) + z + 1
    dx, dy, dz = [b - a + 1 for a, b in zip(own, other)]
    table = jnp.stack([jnp.where(dead, blocks, pairs[0]), line, (dx * 3 + dy) * 3 + dz])
    count = jnp.sum((~dead).astype(jnp.int32)).reshape(1)
    totals = brick_forces(region, table, count, blocks)
    sending = totals.reshape(3, ranks, stride, width)[:, :, :, None]
    returned = lax.all_to_all(sending, ("gy", "gz"), split_axis=1, concat_axis=3, tiled=True)
    return returned.reshape(3, 1, blocks, width)


def solution(mesh):
    return jax.shard_map(
        per_device,
        mesh=mesh,
        in_specs=(
            P(None, "gx", ("gy", "gz"), None),
            P("gx", ("gy", "gz"), None),
            P("gx", ("gy", "gz"), None),
            P(),
            P(),
            P("gx", "gy", "gz", None, None),
        ),
        out_specs=P(None, "gx", ("gy", "gz"), None),
        check_vma=False,
    )
```

```python
import itertools
import math

import jax
import jax.numpy as jnp
from jax import lax
from jax.experimental import pallas as pl
from jax.experimental.pallas import tpu as pltpu
from jax.sharding import PartitionSpec as P

GRID = 4
ROWS = 8
BATCH = 8

cell_edge = 11.0
cutoff = 9.0
soft_core = 16.0
coulomb = 332.0636
limit = cutoff * cutoff + soft_core
sigma_scale = 0.5 * 2.0 ** (1.0 / 6.0)
charge_scale = (coulomb / 12.0) ** 0.5


def exchange_kernel(atoms, region, send_own, recv_own, send_rim, recv_rim, own_sem):
    stride, ranks = atoms.shape[:2]
    layers = region.shape[2] - 2
    spans = [lax.axis_size(name) for name in ("gx", "gy", "gz")]
    here = [lax.axis_index(name) for name in ("gx", "gy", "gz")]
    me = here[1] * spans[2] + here[2]
    chunk = math.gcd(stride, layers)
    pieces = stride // chunk

    def place(piece):
        cell = me * stride + piece * chunk
        return region.at[
            cell // (GRID * layers) + 1,
            lax.rem(cell // layers, GRID) + 1,
            pl.ds(lax.rem(cell, layers) + 1, chunk),
        ]

    copies = []
    for hop in range(1, ranks):
        to = lax.rem(me + hop, ranks)
        for piece in range(pieces):
            sem = (hop - 1) * pieces + piece
            copies.append(
                pltpu.make_async_remote_copy(
                    src_ref=atoms.at[pl.ds(piece * chunk, chunk), to],
                    dst_ref=place(piece),
                    send_sem=send_own.at[sem],
                    recv_sem=recv_own.at[sem],
                    device_id=(here[0], to // spans[2], lax.rem(to, spans[2])),
                    device_id_type=pl.DeviceIdType.MESH,
                )
            )
            copies[-1].start()
    for piece in range(pieces):
        kept = pltpu.make_async_copy(
            atoms.at[pl.ds(piece * chunk, chunk), me], place(piece), own_sem.at[piece]
        )
        kept.start()
        copies.append(kept)
    for copy in copies:
        copy.wait()

    lengths = (GRID, GRID, layers)
    rims = []
    offsets = [o for o in itertools.product((-1, 0, 1), repeat=3) if any(o)]
    for sem, offset in enumerate(offsets):
        source = tuple(
            pl.ds(1, n) if o == 0 else pl.ds(n if o > 0 else 1, 1)
            for o, n in zip(offset, lengths)
        )
        target = tuple(
            pl.ds(1, n) if o == 0 else pl.ds(0 if o > 0 else n + 1, 1)
            for o, n in zip(offset, lengths)
        )
        rims.append(
            pltpu.make_async_remote_copy(
                src_ref=region.at[source],
                dst_ref=region.at[target],
                send_sem=send_rim.at[sem],
                recv_sem=recv_rim.at[sem],
                device_id=tuple(
                    lax.rem(at + o + n, n) for at, o, n in zip(here, offset, spans)
                ),
                device_id_type=pl.DeviceIdType.MESH,
            )
        )
        rims[-1].start()
    for copy in rims:
        copy.wait()


def exchanged(atoms, layers):
    stride, ranks, rows, width = atoms.shape
    pieces = stride // math.gcd(stride, layers)
    own = pltpu.SemaphoreType.DMA(((ranks - 1) * pieces,))
    rim = pltpu.SemaphoreType.DMA((26,))
    return pl.pallas_call(
        exchange_kernel,
        out_shape=jax.ShapeDtypeStruct(
            (GRID + 2, GRID + 2, layers + 2, rows, width), atoms.dtype
        ),
        in_specs=[pl.BlockSpec(memory_space=pltpu.VMEM)],
        out_specs=pl.BlockSpec(memory_space=pltpu.VMEM),
        scratch_shapes=[own, own, rim, rim, pltpu.SemaphoreType.DMA((pieces,))],
        compiler_params=pltpu.CompilerParams(has_side_effects=True),
    )(atoms)


def split(value):
    high = value.astype(jnp.bfloat16).astype(jnp.float32)
    rest = value - high
    middle = rest.astype(jnp.bfloat16).astype(jnp.float32)
    return high, middle, rest - middle


def stacked(parts):
    return jnp.concatenate(parts, axis=0).astype(jnp.bfloat16)


def quotient(value, size):
    if size & (size - 1):
        return lax.div(value, size)
    return lax.shift_right_logical(value, size.bit_length() - 1)


def remainder(value, size):
    if size & (size - 1):
        return lax.rem(value, size)
    return value & (size - 1)


def rows_of(shape):
    return lax.broadcasted_iota(jnp.int32, shape, 0)


def row_table(values, shape):
    rows = rows_of(shape)
    out = jnp.zeros(shape, jnp.float32)
    for k, value in enumerate(values):
        if value:
            out = jnp.where(rows == k, jnp.float32(value), out)
    return out


def rising_powers(base, rows):
    two = base * base
    four = two * two
    out = jnp.where(rows % 2 == 1, base, 1.0)
    out = out * jnp.where(rows // 2 % 2 == 1, two, 1.0)
    return out * jnp.where(rows // 4 % 2 == 1, four, 1.0)


def prepare_sources(region, sources, weights, moments):
    shape = region.shape[1:]
    rows = rows_of(shape)
    count = moments.shape[2]
    ways = row_table([math.comb(6, k) for k in range(7)], shape)
    edge = 1.0 / limit
    high_at = row_table([edge**7 * math.comb(12, k) for k in range(7)], shape)
    low_at = row_table([-(edge**4) * math.comb(6, k) for k in range(7)], shape)
    wide_at = row_table([0.0] + [edge**7 * math.comb(12, k + 6) for k in range(1, 7)], shape)
    near_at = jnp.where(rows == 7, inverse_powers(jnp.full(shape, limit, jnp.float32))[1], 0.0)
    lanes = lax.broadcasted_iota(jnp.int32, (ROWS, count), 1)
    kept = (rows_of((ROWS, count)) >= 4) == (lanes % (2 * ROWS) == 7)

    def one(line, carry):
        block = region[line]
        high, middle, low = split(block)
        sigma = jnp.broadcast_to(region[line, 5:6, :], shape)
        root = jnp.broadcast_to(region[line, 6:7, :], shape)
        charge = jnp.broadcast_to(region[line, 7:8, :], shape)
        falling = rising_powers(sigma, 6 - jnp.minimum(rows, 6))
        square = sigma * sigma
        top, rest, _ = split(ways * falling)
        sources[line] = stacked([high, middle, high, middle, high, low, top, rest, top, rest])
        place = jnp.where(rows < 4, block, pltpu.roll(block, 4, 0))
        top, rest, _ = split(place * jnp.where(rows < 4, root, charge))
        left = stacked([top, rest])
        weights[line] = left
        first = split(falling * (high_at * (square * square * square) + low_at) + near_at)
        second = split(falling * wide_at)
        both = lax.dot_general(
            left,
            stacked([first[0], second[0], first[1], second[1]]),
            (((1,), (1,)), ((), ())),
            preferred_element_type=jnp.float32,
        )
        moments[line] = jnp.where(kept, both[:ROWS] + both[ROWS:], 0.0)
        return carry

    lax.fori_loop(0, region.shape[0], one, 0, unroll=4)


def prepare_homes(region, distances, powers, scales, layers):
    shape = region.shape[1:]
    rows = rows_of(shape)
    blocks = distances.shape[0] - 1

    def one(block, carry):
        line = own_line(block, layers)
        home = region[line]
        distances[block] = jnp.where(rows < 3, -2.0 * home, jnp.where(rows == 4, 1.0, 0.0))
        top, rest, _ = split(rising_powers(jnp.broadcast_to(region[line, 5:6, :], shape), rows))
        powers[block] = stacked([top, top, rest, rest])
        root = jnp.broadcast_to(region[line, 6:7, :], shape)
        charge = jnp.broadcast_to(region[line, 7:8, :], shape)
        scales[block] = 12.0 * jnp.where(rows < 4, root, charge)
        return carry

    lax.fori_loop(0, blocks, one, 0, unroll=4)
    distances[blocks] = jnp.zeros(shape, jnp.float32)
    powers[blocks] = jnp.zeros(powers.shape[1:], powers.dtype)


def own_line(block, layers):
    x = quotient(block, GRID * layers)
    y = remainder(quotient(block, layers), GRID)
    return ((x + 1) * (GRID + 2) + y + 1) * (layers + 2) + remainder(block, layers) + 1


def prepare_steps(offsets, shifts):
    shape = offsets.shape[1:]
    for step, cells in enumerate(itertools.product((-1, 0, 1), repeat=3)):
        moves = [cell_edge * c for c in cells]
        offsets[step] = row_table([2.0 * m for m in moves], shape)
        shifts[step] = row_table(moves + [0.0] + moves, shape)


def pair_terms(pairs, index, sources, distances, powers, offsets, terms):
    home = pairs[0, index]
    distance = distances[home] + offsets[pairs[2, index]]
    rows = rows_of(distance.shape)
    share = jnp.where(rows < 3, 0.25, jnp.where(rows == 4, soft_core, 0.0))
    square = jnp.sum(distance * distance * share, axis=0, keepdims=True)
    distance = jnp.where(rows == 3, square, distance)
    high, middle, low = split(distance)
    near = stacked([high, high, middle, middle, low, high])
    strong = powers[home]
    width = near.shape[1]
    right = jnp.concatenate(
        [
            jnp.concatenate([near, jnp.zeros((strong.shape[0], width), near.dtype)], axis=0),
            jnp.concatenate([jnp.zeros(near.shape, near.dtype), strong], axis=0),
        ],
        axis=1,
    )
    terms[...] = lax.dot_general(
        sources[pairs[1, index]],
        right,
        (((0,), (0,)), ((), ())),
        preferred_element_type=jnp.float32,
    )


def inverse_powers(softened):
    root = lax.rsqrt(softened)
    one = root * root
    return one, one * root


def strengths(terms, nears, strongs):
    width = terms.shape[0]
    for start in range(0, width, 16):
        rows = pl.ds(start, 16)
        one, near = inverse_powers(jnp.minimum(terms[rows, :width], limit))
        sixth = terms[rows, width:] * (near * near)
        for halves, value in ((nears, near), (strongs, one * (sixth * (sixth - 1.0)))):
            top = value.astype(jnp.bfloat16)
            halves[rows, :] = top
            halves[pl.ds(width + start, 16), :] = (value - top.astype(jnp.float32)).astype(jnp.bfloat16)


def add_forces(pairs, index, weights, moments, shifts, nears, strongs, totals, edges):
    line = pairs[1, index]
    left = weights[line]
    both = jnp.dot(
        jnp.concatenate([left, left], axis=1),
        jnp.concatenate([nears[...], strongs[...]], axis=1),
        preferred_element_type=jnp.float32,
    )
    both = both[:ROWS] + both[ROWS:]
    width = left.shape[1]
    rows = rows_of((ROWS, width))
    summed = jnp.where(rows < 4, both[:, width:], both[:, :width])
    plain = jnp.where(rows < 4, summed[3:4], summed[7:8])
    shift = shifts[pairs[2, index]]
    home = pairs[0, index]
    totals[home] += summed + shift * plain
    shape = moments.shape[1:]
    count = shape[1]
    plain = jnp.where(
        rows[:, :count] < 4,
        jnp.broadcast_to(moments[line, 3:4, :], shape),
        jnp.broadcast_to(moments[line, 7:8, :], shape),
    )
    edges[home] += moments[line] + shift[:, :count] * plain


def force_kernel(
    pairs, count, region, out, totals, sources, weights, moments, distances, powers, scales, edges, offsets, shifts, *slots
):
    blocks = out.shape[1]
    layers = blocks // (GRID * GRID)
    totals[...] = jnp.zeros_like(totals)
    edges[...] = jnp.zeros_like(edges)
    prepare_steps(offsets, shifts)
    prepare_sources(region, sources, weights, moments)
    prepare_homes(region, distances, powers, scales, layers)
    terms, nears, strongs = [
        (slots[k : k + BATCH], slots[k + BATCH : k + 2 * BATCH]) for k in range(0, 6 * BATCH, 2 * BATCH)
    ]

    def step(index, carry):
        for turn in range(2):
            first = (2 * index + turn) * BATCH
            for t in range(BATCH):
                add_forces(
                    pairs, first + t, weights, moments, shifts, nears[turn][t], strongs[turn][t], totals, edges
                )
                strengths(terms[1 - turn][t], nears[1 - turn][t], strongs[1 - turn][t])
                pair_terms(pairs, first + 2 * BATCH + t, sources, distances, powers, offsets, terms[turn][t])
        return carry

    groups = (count[0] + BATCH - 1) // BATCH
    lax.fori_loop(0, (groups + 3) // 2, step, 0)

    def finish(block, carry):
        home = region[own_line(block, layers)]
        rows = rows_of(home.shape)
        place = jnp.where(rows < 4, home, pltpu.roll(home, 4, 0))
        sigma = jnp.broadcast_to(home[5:6], home.shape)
        rising = rising_powers(sigma, rows)
        square = sigma * sigma
        first = split(jnp.where(rows == 7, 1.0, rising))
        second = split(rising * (square * square * square))
        right = stacked([first[0], second[0], first[0], second[0], first[1], second[1], first[1], second[1]])
        edge = edges[block]
        left = stacked([*split(edge), jnp.zeros_like(edge)])
        both = jnp.dot(jnp.concatenate([left, left], axis=1), right, preferred_element_type=jnp.float32)
        summed = totals[block] - (both[:ROWS] + both[ROWS : 2 * ROWS] + both[2 * ROWS : 3 * ROWS])
        plain = jnp.where(rows < 4, summed[3:4], summed[7:8])
        force = (place * plain - summed) * scales[block]
        totals[block] = force + pltpu.roll(force, 4, 0)
        return carry

    lax.fori_loop(0, blocks, finish, 0, unroll=4)
    for axis in range(3):
        out[axis] = totals[:blocks, axis, :]


def brick_forces(region, pairs, count, blocks):
    lines, _, width = region.shape
    single = pltpu.VMEM((blocks + 1, ROWS, width), jnp.float32)
    table = pltpu.VMEM((27, ROWS, width), jnp.float32)
    return pl.pallas_call(
        force_kernel,
        out_shape=jax.ShapeDtypeStruct((3, blocks, width), jnp.float32),
        in_specs=[
            pl.BlockSpec(memory_space=pltpu.SMEM),
            pl.BlockSpec(memory_space=pltpu.SMEM),
            pl.BlockSpec(memory_space=pltpu.VMEM),
        ],
        out_specs=pl.BlockSpec(memory_space=pltpu.VMEM),
        scratch_shapes=[
            single,
            pltpu.VMEM((lines, 10 * ROWS, width), jnp.bfloat16),
            pltpu.VMEM((lines, 2 * ROWS, width), jnp.bfloat16),
            pltpu.VMEM((lines, ROWS, 4 * ROWS), jnp.float32),
            single,
            pltpu.VMEM((blocks + 1, 4 * ROWS, width), jnp.bfloat16),
            single,
            pltpu.VMEM((blocks + 1, ROWS, 4 * ROWS), jnp.float32),
            table,
            table,
        ]
        + [pltpu.VMEM((width, 2 * width), jnp.float32)] * (2 * BATCH)
        + [pltpu.VMEM((2 * width, width), jnp.bfloat16)] * (4 * BATCH),
    )(pairs, count, region)


def per_device(coords, charges, atom_types, lj_sigma, lj_epsilon, tile_list):
    span_y = lax.axis_size("gy")
    span_z = lax.axis_size("gz")
    blocks = coords.shape[2]
    width = coords.shape[3]
    layers = blocks // (GRID * GRID)
    ranks = span_y * span_z
    stride = blocks // ranks
    dtype = coords.dtype
    kinds = jnp.arange(lj_sigma.shape[0], dtype=jnp.int32)
    selector = (atom_types[0][:, :, None] == kinds).astype(dtype)
    sigma_atom = jnp.sum(selector * (lj_sigma * sigma_scale), axis=2)
    root_atom = jnp.sum(selector * (jnp.sqrt(lj_epsilon)), axis=2)
    inner = coords[:, 0] - 0.5 * cell_edge
    square = inner[0] * inner[0] + inner[1] * inner[1] + inner[2] * inner[2]
    atoms = jnp.stack(
        [inner[0], inner[1], inner[2], jnp.ones_like(square), square]
        + [sigma_atom, root_atom, charges[0] * charge_scale],
        axis=1,
    )
    outgoing = atoms.reshape(stride, ranks, ROWS, width)
    padded = exchanged(outgoing, layers)
    region = padded.reshape(-1, ROWS, width)
    pairs = jnp.pad(
        tile_list[0, 0, 0], ((0, 0), (2 * BATCH, 4 * BATCH)), constant_values=-1
    )
    dead = pairs[0] < 0

    def place(ids):
        slot = ids // blocks
        member = ids % blocks
        px = member // (GRID * layers) + (slot // 9 - 1) * GRID
        py = member // layers % GRID + (slot // 3 % 3 - 1) * GRID
        pz = member % layers + (slot % 3 - 1) * layers
        return px, py, pz

    own = place(jnp.where(dead, 0, pairs[0]) + 13 * blocks)
    other = place(jnp.where(dead, 13 * blocks, pairs[1]))
    x, y, z = other
    line = ((x + 1) * (GRID + 2) + y + 1) * (layers + 2) + z + 1
    dx, dy, dz = [b - a + 1 for a, b in zip(own, other)]
    table = jnp.stack([jnp.where(dead, blocks, pairs[0]), line, (dx * 3 + dy) * 3 + dz])
    count = jnp.sum((~dead).astype(jnp.int32)).reshape(1)
    totals = brick_forces(region, table, count, blocks)
    sending = totals.reshape(3, ranks, stride, width)[:, :, :, None]
    returned = lax.all_to_all(sending, ("gy", "gz"), split_axis=1, concat_axis=3, tiled=True)
    return returned.reshape(3, 1, blocks, width)


def solution(mesh):
    return jax.shard_map(
        per_device,
        mesh=mesh,
        in_specs=(
            P(None, "gx", ("gy", "gz"), None),
            P("gx", ("gy", "gz"), None),
            P("gx", ("gy", "gz"), None),
            P(),
            P(),
            P("gx", "gy", "gz", None, None),
        ),
        out_specs=P(None, "gx", ("gy", "gz"), None),
        check_vma=False,
    )
```

```python
import itertools
import math

import jax
import jax.numpy as jnp
from jax import lax
from jax.experimental import pallas as pl
from jax.experimental.pallas import tpu as pltpu
from jax.sharding import PartitionSpec as P

GRID = 4
ROWS = 8
BATCH = 4
EDGE = 128

cell_edge = 11.0
cutoff = 9.0
soft_core = 16.0
coulomb = 332.0636
limit = cutoff * cutoff + soft_core
sigma_scale = 0.5 * 2.0 ** (1.0 / 6.0)
charge_scale = (coulomb / 12.0) ** 0.5


def spans_of():
    names = ("gx", "gy", "gz")
    return [lax.axis_size(n) for n in names], [lax.axis_index(n) for n in names]


def plane_peers(spans, here):
    ranks = spans[1] * spans[2]
    me = here[1] * spans[2] + here[2]
    for hop in range(1, ranks):
        to = lax.rem(me + hop, ranks)
        yield hop, to, (here[0], quotient(to, spans[2]), remainder(to, spans[2]))


def brick_neighbours(spans, here):
    for offset in itertools.product((-1, 0, 1), repeat=3):
        if any(offset):
            yield offset, tuple(lax.rem(at + o + n, n) for at, o, n in zip(here, offset, spans))


def greet(devices):
    barrier = pltpu.get_barrier_semaphore()
    for device in devices:
        pl.semaphore_signal(barrier, inc=1, device_id=device, device_id_type=pl.DeviceIdType.MESH)
    return barrier, len(devices)


def looked_up(values, kinds):
    padded = jnp.concatenate([values, jnp.zeros((1, kinds.shape[1] - values.shape[1]), values.dtype)], axis=1)
    return jnp.take_along_axis(jnp.broadcast_to(padded, kinds.shape), kinds, axis=1)


def pack_atoms(coords, charges, kinds, sigma, epsilon, atoms):
    stride, ranks = atoms.shape[:2]
    sigmas = sigma[...] * sigma_scale
    roots = jnp.sqrt(epsilon[...])
    for group in range(stride):
        rows = pl.ds(group * ranks, ranks)
        inner = [coords[axis, rows, :] - 0.5 * cell_edge for axis in range(3)]
        kind = kinds[rows, :]
        square = inner[0] * inner[0] + inner[1] * inner[1] + inner[2] * inner[2]
        values = inner + [jnp.ones_like(square), square, looked_up(sigmas, kind), looked_up(roots, kind)]
        values.append(charges[rows, :] * charge_scale)
        for row, value in enumerate(values):
            atoms[group, :, row, :] = value


def cell_of(member, layers):
    return (
        quotient(member, GRID * layers),
        remainder(quotient(member, layers), GRID),
        remainder(member, layers),
    )


def thirds(value, size):
    return sum((value >= k * size).astype(jnp.int32) for k in (1, 2))


def tile_table(tiles, table, blocks, layers):
    home, other = tiles[0:1, :], tiles[1:2, :]
    dead = home < 0
    slot = quotient(jnp.where(dead, 13 * blocks, other), blocks)
    member = remainder(jnp.where(dead, 0, other), blocks)
    far = thirds(slot, 9)
    slot = slot - 9 * far
    middle = thirds(slot, 3)
    steps = (far - 1, middle - 1, slot - 3 * middle - 1)
    sizes = (GRID, GRID, layers)
    own = cell_of(jnp.where(dead, 0, home), layers)
    there = [c + s * n for c, s, n in zip(cell_of(member, layers), steps, sizes)]
    line = ((there[0] + 1) * (GRID + 2) + there[1] + 1) * (layers + 2) + there[2] + 1
    delta = [t - o + 1 for t, o in zip(there, own)]
    width = tiles.shape[1]
    table[...] = jnp.where(rows_of(table.shape) == 0, blocks, 0)
    table[0:1, EDGE : EDGE + width] = jnp.where(dead, blocks, home)
    table[1:2, EDGE : EDGE + width] = line
    table[2:3, EDGE : EDGE + width] = (delta[0] * 3 + delta[1]) * 3 + delta[2]


def exchange_kernel(
    coords, charges, kinds, sigma, epsilon, tiles, region, table, atoms, send_own, recv_own, send_rim, recv_rim, own_sem
):
    stride, ranks = atoms.shape[:2]
    layers = region.shape[2] - 2
    blocks = stride * ranks
    spans, here = spans_of()
    me = here[1] * spans[2] + here[2]
    peers = list(plane_peers(spans, here))
    neighbours = list(brick_neighbours(spans, here))
    barrier, greeted = greet([p[2] for p in peers] + [n[1] for n in neighbours])
    pack_atoms(coords, charges, kinds, sigma, epsilon, atoms)
    tile_table(tiles, table, blocks, layers)
    pl.semaphore_wait(barrier, greeted)
    chunk = math.gcd(stride, layers)
    pieces = stride // chunk

    def place(piece):
        x, y, z = cell_of(me * stride + piece * chunk, layers)
        return region.at[x + 1, y + 1, pl.ds(z + 1, chunk)]

    copies = []
    for hop, to, device in peers:
        for piece in range(pieces):
            sem = (hop - 1) * pieces + piece
            copies.append(
                pltpu.make_async_remote_copy(
                    src_ref=atoms.at[pl.ds(piece * chunk, chunk), to],
                    dst_ref=place(piece),
                    send_sem=send_own.at[sem],
                    recv_sem=recv_own.at[sem],
                    device_id=device,
                    device_id_type=pl.DeviceIdType.MESH,
                )
            )
            copies[-1].start()
    for piece in range(pieces):
        kept = pltpu.make_async_copy(
            atoms.at[pl.ds(piece * chunk, chunk), me], place(piece), own_sem.at[piece]
        )
        kept.start()
        copies.append(kept)
    for copy in copies:
        copy.wait()

    lengths = (GRID, GRID, layers)
    rims = []
    for sem, (offset, device) in enumerate(neighbours):
        source = tuple(
            pl.ds(1, n) if o == 0 else pl.ds(n if o > 0 else 1, 1)
            for o, n in zip(offset, lengths)
        )
        target = tuple(
            pl.ds(1, n) if o == 0 else pl.ds(0 if o > 0 else n + 1, 1)
            for o, n in zip(offset, lengths)
        )
        rims.append(
            pltpu.make_async_remote_copy(
                src_ref=region.at[source],
                dst_ref=region.at[target],
                send_sem=send_rim.at[sem],
                recv_sem=recv_rim.at[sem],
                device_id=device,
                device_id_type=pl.DeviceIdType.MESH,
            )
        )
        rims[-1].start()
    for copy in rims:
        copy.wait()


def exchanged(coords, charges, kinds, sigma, epsilon, tiles, ranks):
    blocks, width = charges.shape
    layers = blocks // (GRID * GRID)
    stride = blocks // ranks
    pieces = stride // math.gcd(stride, layers)
    own = pltpu.SemaphoreType.DMA(((ranks - 1) * pieces,))
    rim = pltpu.SemaphoreType.DMA((26,))
    vmem = pl.BlockSpec(memory_space=pltpu.VMEM)
    return pl.pallas_call(
        exchange_kernel,
        out_shape=(
            jax.ShapeDtypeStruct((GRID + 2, GRID + 2, layers + 2, ROWS, width), coords.dtype),
            jax.ShapeDtypeStruct((ROWS, tiles.shape[1] + 2 * EDGE), jnp.int32),
        ),
        in_specs=[vmem] * 6,
        out_specs=(vmem, vmem),
        scratch_shapes=[
            pltpu.VMEM((stride, ranks, ROWS, width), coords.dtype),
            own,
            own,
            rim,
            rim,
            pltpu.SemaphoreType.DMA((pieces,)),
        ],
        compiler_params=pltpu.CompilerParams(
            has_side_effects=True, collective_id=0, vmem_limit_bytes=8 << 20
        ),
    )(coords, charges, kinds, sigma, epsilon, tiles)


def return_kernel(forces, out, send, recv, own_sem):
    spans, here = spans_of()
    me = here[1] * spans[2] + here[2]
    peers = list(plane_peers(spans, here))
    barrier, greeted = greet([p[2] for p in peers])
    kept = pltpu.make_async_copy(forces.at[:, me], out.at[:, :, me], own_sem.at[0])
    kept.start()
    pl.semaphore_wait(barrier, greeted)
    copies = [kept]
    for hop, to, device in peers:
        copies.append(
            pltpu.make_async_remote_copy(
                src_ref=forces.at[:, to],
                dst_ref=out.at[:, :, me],
                send_sem=send.at[hop - 1],
                recv_sem=recv.at[hop - 1],
                device_id=device,
                device_id_type=pl.DeviceIdType.MESH,
            )
        )
        copies[-1].start()
    for copy in copies:
        copy.wait()


def returned(forces, ranks):
    axes, blocks, width = forces.shape
    stride = blocks // ranks
    sems = pltpu.SemaphoreType.DMA((ranks - 1,))
    vmem = pl.BlockSpec(memory_space=pltpu.VMEM)
    out = pl.pallas_call(
        return_kernel,
        out_shape=jax.ShapeDtypeStruct((axes, stride, ranks, 1, width), forces.dtype),
        in_specs=[vmem],
        out_specs=vmem,
        scratch_shapes=[sems, sems, pltpu.SemaphoreType.DMA((1,))],
        compiler_params=pltpu.CompilerParams(
            has_side_effects=True, collective_id=1, vmem_limit_bytes=4 << 20
        ),
    )(forces.reshape(axes, ranks, stride, 1, width))
    return out.reshape(axes, 1, blocks, width)


def split(value):
    high = value.astype(jnp.bfloat16).astype(jnp.float32)
    rest = value - high
    middle = rest.astype(jnp.bfloat16).astype(jnp.float32)
    return high, middle, rest - middle


def stacked(parts):
    return jnp.concatenate(parts, axis=0).astype(jnp.bfloat16)


def quotient(value, size):
    if size & (size - 1):
        return lax.div(value, size)
    return lax.shift_right_logical(value, size.bit_length() - 1)


def remainder(value, size):
    if size & (size - 1):
        return lax.rem(value, size)
    return value & (size - 1)


def rows_of(shape):
    return lax.broadcasted_iota(jnp.int32, shape, 0)


def row_table(values, shape):
    rows = rows_of(shape)
    out = jnp.zeros(shape, jnp.float32)
    for k, value in enumerate(values):
        if value:
            out = jnp.where(rows == k, jnp.float32(value), out)
    return out


def rising_powers(base, rows):
    two = base * base
    four = two * two
    out = jnp.where(rows % 2 == 1, base, 1.0)
    out = out * jnp.where(rows // 2 % 2 == 1, two, 1.0)
    return out * jnp.where(rows // 4 % 2 == 1, four, 1.0)


def prepare_sources(region, sources, weights, moments, edge_terms):
    shape = region.shape[1:]
    rows = rows_of(shape)
    count = moments.shape[2]
    ways = row_table([math.comb(6, k) for k in range(7)], shape)
    edge = 1.0 / limit
    high_at = row_table([edge**7 * math.comb(12, k) for k in range(7)], shape)
    low_at = row_table([-(edge**4) * math.comb(6, k) for k in range(7)], shape)
    wide_at = row_table([0.0] + [edge**7 * math.comb(12, k + 6) for k in range(1, 7)], shape)
    near_at = jnp.where(rows == 7, inverse_powers(jnp.full(shape, limit, jnp.float32))[1], 0.0)
    lanes = lax.broadcasted_iota(jnp.int32, (ROWS, count), 1)
    kept = (rows_of((ROWS, count)) >= 4) == (lanes % (2 * ROWS) == 7)

    def spread(line):
        block = region[line]
        high, middle, low = split(block)
        sigma = jnp.broadcast_to(region[line, 5:6, :], shape)
        root = jnp.broadcast_to(region[line, 6:7, :], shape)
        charge = jnp.broadcast_to(region[line, 7:8, :], shape)
        falling = rising_powers(sigma, 6 - jnp.minimum(rows, 6))
        square = sigma * sigma
        top, rest, _ = split(ways * falling)
        sources[line] = stacked([high, middle, high, middle, high, low, top, rest, top, rest])
        place = jnp.where(rows < 4, block, pltpu.roll(block, 4, 0))
        top, rest, _ = split(place * jnp.where(rows < 4, root, charge))
        weights[line] = stacked([top, rest])
        first = split(falling * (high_at * (square * square * square) + low_at) + near_at)
        second = split(falling * wide_at)
        edge_terms[line] = stacked([first[0], second[0], first[1], second[1]])

    def summed(line):
        both = lax.dot_general(
            weights[line],
            edge_terms[line],
            (((1,), (1,)), ((), ())),
            preferred_element_type=jnp.float32,
        )
        moments[line] = jnp.where(kept, both[:ROWS] + both[ROWS:], 0.0)

    lines = region.shape[0]
    group = max(n for n in range(1, 25) if lines % n == 0)

    def one(index, carry):
        for k in range(group):
            summed((index - 1) * group + k)
        for k in range(group):
            spread(index * group + k)
        return carry

    for k in range(group):
        spread(k)
    lax.fori_loop(1, lines // group, one, 0)
    for k in range(group):
        summed(lines - group + k)


def prepare_homes(region, distances, powers, scales, layers):
    shape = region.shape[1:]
    rows = rows_of(shape)
    blocks = distances.shape[0] - 1

    def one(block, carry):
        line = own_line(block, layers)
        home = region[line]
        distances[block] = jnp.where(rows < 3, -2.0 * home, jnp.where(rows == 4, 1.0, 0.0))
        top, rest, _ = split(rising_powers(jnp.broadcast_to(region[line, 5:6, :], shape), rows))
        powers[block] = stacked([top, top, rest, rest])
        root = jnp.broadcast_to(region[line, 6:7, :], shape)
        charge = jnp.broadcast_to(region[line, 7:8, :], shape)
        scales[block] = 12.0 * jnp.where(rows < 4, root, charge)
        return carry

    lax.fori_loop(0, blocks, one, 0, unroll=4)
    distances[blocks] = jnp.zeros(shape, jnp.float32)
    powers[blocks] = jnp.zeros(powers.shape[1:], powers.dtype)


def own_line(block, layers):
    x = quotient(block, GRID * layers)
    y = remainder(quotient(block, layers), GRID)
    return ((x + 1) * (GRID + 2) + y + 1) * (layers + 2) + remainder(block, layers) + 1


def prepare_steps(offsets, shifts):
    shape = offsets.shape[1:]
    for step, cells in enumerate(itertools.product((-1, 0, 1), repeat=3)):
        moves = [cell_edge * c for c in cells]
        offsets[step] = row_table([2.0 * m for m in moves], shape)
        shifts[step] = row_table(moves + [0.0] + moves, shape)


def pair_terms(pairs, index, sources, distances, powers, offsets, terms):
    home = pairs[0, index]
    distance = distances[home] + offsets[pairs[2, index]]
    rows = rows_of(distance.shape)
    share = jnp.where(rows < 3, 0.25, jnp.where(rows == 4, soft_core, 0.0))
    square = jnp.sum(distance * distance * share, axis=0, keepdims=True)
    distance = jnp.where(rows == 3, square, distance)
    high, middle, low = split(distance)
    near = stacked([high, high, middle, middle, low, high])
    strong = powers[home]
    width = near.shape[1]
    right = jnp.concatenate(
        [
            jnp.concatenate([near, jnp.zeros((strong.shape[0], width), near.dtype)], axis=0),
            jnp.concatenate([jnp.zeros(near.shape, near.dtype), strong], axis=0),
        ],
        axis=1,
    )
    terms[...] = lax.dot_general(
        sources[pairs[1, index]],
        right,
        (((0,), (0,)), ((), ())),
        preferred_element_type=jnp.float32,
    )


def inverse_powers(softened):
    root = lax.rsqrt(softened)
    one = root * root
    return one, one * root


def strengths(terms, nears, strongs):
    width = terms.shape[0]
    for start in range(0, width, 16):
        rows = pl.ds(start, 16)
        one, near = inverse_powers(jnp.minimum(terms[rows, :width], limit))
        sixth = terms[rows, width:] * (near * near)
        for halves, value in ((nears, near), (strongs, one * (sixth * (sixth - 1.0)))):
            top = value.astype(jnp.bfloat16)
            halves[rows, :] = top
            halves[pl.ds(width + start, 16), :] = (value - top.astype(jnp.float32)).astype(jnp.bfloat16)


def add_forces(pairs, index, weights, moments, shifts, nears, strongs, totals, edges):
    line = pairs[1, index]
    left = weights[line]
    both = jnp.dot(
        jnp.concatenate([left, left], axis=1),
        jnp.concatenate([nears[...], strongs[...]], axis=1),
        preferred_element_type=jnp.float32,
    )
    both = both[:ROWS] + both[ROWS:]
    width = left.shape[1]
    rows = rows_of((ROWS, width))
    summed = jnp.where(rows < 4, both[:, width:], both[:, :width])
    plain = jnp.where(rows < 4, summed[3:4], summed[7:8])
    shift = shifts[pairs[2, index]]
    home = pairs[0, index]
    totals[home] += summed + shift * plain
    shape = moments.shape[1:]
    count = shape[1]
    plain = jnp.where(
        rows[:, :count] < 4,
        jnp.broadcast_to(moments[line, 3:4, :], shape),
        jnp.broadcast_to(moments[line, 7:8, :], shape),
    )
    edges[home] += moments[line] + shift[:, :count] * plain


def force_kernel(
    pairs, region, out, totals, sources, weights, moments, distances, powers, scales, edges, edge_terms, offsets, shifts, *slots
):
    blocks = out.shape[1]
    layers = blocks // (GRID * GRID)
    totals[...] = jnp.zeros_like(totals)
    edges[...] = jnp.zeros_like(edges)
    prepare_steps(offsets, shifts)
    prepare_sources(region, sources, weights, moments, edge_terms)
    prepare_homes(region, distances, powers, scales, layers)
    terms, nears, strongs = [
        (slots[k : k + BATCH], slots[k + BATCH : k + 2 * BATCH]) for k in range(0, 6 * BATCH, 2 * BATCH)
    ]

    def step(index, carry):
        for turn in range(2):
            first = (2 * index + turn - 2) * BATCH + EDGE
            for t in range(BATCH):
                add_forces(
                    pairs, first + t, weights, moments, shifts, nears[turn][t], strongs[turn][t], totals, edges
                )
                strengths(terms[1 - turn][t], nears[1 - turn][t], strongs[1 - turn][t])
                pair_terms(pairs, first + 2 * BATCH + t, sources, distances, powers, offsets, terms[turn][t])
        return carry

    groups = -(-(pairs.shape[1] - 2 * EDGE) // BATCH)
    lax.fori_loop(0, (groups + 3) // 2, step, 0)

    def finish(block, carry):
        home = region[own_line(block, layers)]
        rows = rows_of(home.shape)
        place = jnp.where(rows < 4, home, pltpu.roll(home, 4, 0))
        sigma = jnp.broadcast_to(home[5:6], home.shape)
        rising = rising_powers(sigma, rows)
        square = sigma * sigma
        first = split(jnp.where(rows == 7, 1.0, rising))
        second = split(rising * (square * square * square))
        right = stacked([first[0], second[0], first[0], second[0], first[1], second[1], first[1], second[1]])
        edge = edges[block]
        left = stacked([*split(edge), jnp.zeros_like(edge)])
        both = jnp.dot(jnp.concatenate([left, left], axis=1), right, preferred_element_type=jnp.float32)
        summed = totals[block] - (both[:ROWS] + both[ROWS : 2 * ROWS] + both[2 * ROWS : 3 * ROWS])
        plain = jnp.where(rows < 4, summed[3:4], summed[7:8])
        force = (place * plain - summed) * scales[block]
        totals[block] = force + pltpu.roll(force, 4, 0)
        return carry

    lax.fori_loop(0, blocks, finish, 0, unroll=16)
    for axis in range(3):
        out[axis] = totals[:blocks, axis, :]


def brick_forces(region, pairs, blocks):
    lines, _, width = region.shape
    single = pltpu.VMEM((blocks + 1, ROWS, width), jnp.float32)
    table = pltpu.VMEM((27, ROWS, width), jnp.float32)
    return pl.pallas_call(
        force_kernel,
        out_shape=jax.ShapeDtypeStruct((3, blocks, width), jnp.float32),
        in_specs=[
            pl.BlockSpec(memory_space=pltpu.SMEM),
            pl.BlockSpec(memory_space=pltpu.VMEM),
        ],
        out_specs=pl.BlockSpec(memory_space=pltpu.VMEM),
        scratch_shapes=[
            single,
            pltpu.VMEM((lines, 10 * ROWS, width), jnp.bfloat16),
            pltpu.VMEM((lines, 2 * ROWS, width), jnp.bfloat16),
            pltpu.VMEM((lines, ROWS, 4 * ROWS), jnp.float32),
            single,
            pltpu.VMEM((blocks + 1, 4 * ROWS, width), jnp.bfloat16),
            single,
            pltpu.VMEM((blocks + 1, ROWS, 4 * ROWS), jnp.float32),
            pltpu.VMEM((lines, 4 * ROWS, width), jnp.bfloat16),
            table,
            table,
        ]
        + [pltpu.VMEM((width, 2 * width), jnp.float32)] * (2 * BATCH)
        + [pltpu.VMEM((2 * width, width), jnp.bfloat16)] * (4 * BATCH),
        compiler_params=pltpu.CompilerParams(vmem_limit_bytes=40 << 20),
    )(pairs, region)


def per_device(coords, charges, atom_types, lj_sigma, lj_epsilon, tile_list):
    span_y = lax.axis_size("gy")
    span_z = lax.axis_size("gz")
    blocks = coords.shape[2]
    width = coords.shape[3]
    ranks = span_y * span_z
    padded, table = exchanged(
        coords[:, 0],
        charges[0],
        atom_types[0],
        lj_sigma[None],
        lj_epsilon[None],
        tile_list[0, 0, 0],
        ranks,
    )
    forces = brick_forces(padded.reshape(-1, ROWS, width), table, blocks)
    return returned(forces, ranks)


def solution(mesh):
    return jax.shard_map(
        per_device,
        mesh=mesh,
        in_specs=(
            P(None, "gx", ("gy", "gz"), None),
            P("gx", ("gy", "gz"), None),
            P("gx", ("gy", "gz"), None),
            P(),
            P(),
            P("gx", "gy", "gz", None, None),
        ),
        out_specs=P(None, "gx", ("gy", "gz"), None),
        check_vma=False,
    )
```

```python
import itertools
import math

import jax
import jax.numpy as jnp
from jax import lax
from jax.experimental import pallas as pl
from jax.experimental.pallas import tpu as pltpu
from jax.sharding import PartitionSpec as P

GRID = 4
ROWS = 8
BATCH = 8
HALF = BATCH // 2
EDGE = 128

cell_edge = 11.0
cutoff = 9.0
soft_core = 16.0
coulomb = 332.0636
limit = cutoff * cutoff + soft_core
sigma_scale = 0.5 * 2.0 ** (1.0 / 6.0)
charge_scale = (coulomb / 12.0) ** 0.5


def spans_of():
    names = ("gx", "gy", "gz")
    return [lax.axis_size(n) for n in names], [lax.axis_index(n) for n in names]


def plane_peers(spans, here):
    ranks = spans[1] * spans[2]
    me = here[1] * spans[2] + here[2]
    for hop in range(1, ranks):
        to = lax.rem(me + hop, ranks)
        yield hop, to, (here[0], quotient(to, spans[2]), remainder(to, spans[2]))


def brick_neighbours(spans, here):
    for offset in itertools.product((-1, 0, 1), repeat=3):
        if any(offset):
            yield offset, tuple(lax.rem(at + o + n, n) for at, o, n in zip(here, offset, spans))


def greet(devices):
    barrier = pltpu.get_barrier_semaphore()
    for device in devices:
        pl.semaphore_signal(barrier, inc=1, device_id=device, device_id_type=pl.DeviceIdType.MESH)
    return barrier, len(devices)


def looked_up(values, kinds):
    return jnp.take_along_axis(jnp.broadcast_to(values, kinds.shape), kinds, axis=1)


def pack_atoms(coords, charges, kinds, atoms, labels):
    stride, ranks = atoms.shape[:2]
    for group in range(stride):
        rows = pl.ds(group * ranks, ranks)
        for axis in range(3):
            atoms[group, :, axis, :] = coords[axis, rows, :] - 0.5 * cell_edge
        atoms[group, :, 3, :] = charges[rows, :] * charge_scale
        labels[group, :, 0, :] = kinds[rows, :].astype(jnp.float32)


def type_table(sigma, epsilon, types):
    empty = jnp.zeros((1, types.shape[1] - sigma.shape[1]), types.dtype)
    types[0:1, :] = jnp.concatenate([sigma[...] * sigma_scale, empty], axis=1)
    types[1:2, :] = jnp.concatenate([jnp.sqrt(epsilon[...]), empty], axis=1)


def cell_of(member, layers):
    return (
        quotient(member, GRID * layers),
        remainder(quotient(member, layers), GRID),
        remainder(member, layers),
    )


def thirds(value, size):
    return sum((value >= k * size).astype(jnp.int32) for k in (1, 2))


def tile_table(tiles, table, blocks, layers):
    home, other = tiles[0:1, :], tiles[1:2, :]
    dead = home < 0
    slot = quotient(jnp.where(dead, 13 * blocks, other), blocks)
    member = remainder(jnp.where(dead, 0, other), blocks)
    far = thirds(slot, 9)
    slot = slot - 9 * far
    middle = thirds(slot, 3)
    steps = (far - 1, middle - 1, slot - 3 * middle - 1)
    sizes = (GRID, GRID, layers)
    own = cell_of(jnp.where(dead, 0, home), layers)
    there = [c + s * n for c, s, n in zip(cell_of(member, layers), steps, sizes)]
    line = ((there[0] + 1) * (GRID + 2) + there[1] + 1) * (layers + 2) + there[2] + 1
    delta = [t - o + 1 for t, o in zip(there, own)]
    width = tiles.shape[1]
    table[...] = jnp.where(rows_of(table.shape) == 0, blocks, 0)
    table[0:1, EDGE : EDGE + width] = jnp.where(dead, blocks, home)
    table[1:2, EDGE : EDGE + width] = line
    table[2:3, EDGE : EDGE + width] = (delta[0] * 3 + delta[1]) * 3 + delta[2]


def exchange_kernel(*refs):
    given, (region, marks, table, types), scratch = refs[:6], refs[6:10], refs[10:]
    held, (atoms, labels, send_own, recv_own, send_rim, recv_rim, own_sem, load_sem) = scratch[:6], scratch[6:]
    stride, ranks = atoms.shape[:2]
    layers = region.shape[2] - 2
    blocks = stride * ranks
    spans, here = spans_of()
    me = here[1] * spans[2] + here[2]
    loads = [pltpu.make_async_copy(src, dst, load_sem.at[k]) for k, (src, dst) in enumerate(zip(given, held))]
    for load in loads:
        load.start()
    peers = list(plane_peers(spans, here))
    neighbours = list(brick_neighbours(spans, here))
    barrier, greeted = greet([p[2] for p in peers] + [n[1] for n in neighbours])
    coords, charges, kinds, sigma, epsilon, tiles = held
    for load in loads:
        load.wait()
    pack_atoms(coords, charges, kinds, atoms, labels)
    tile_table(tiles, table, blocks, layers)
    type_table(sigma, epsilon, types)
    pl.semaphore_wait(barrier, greeted)
    chunk = math.gcd(stride, layers)
    pieces = stride // chunk
    pairs = ((atoms, region), (labels, marks))

    def place(ref, piece):
        x, y, z = cell_of(me * stride + piece * chunk, layers)
        return ref.at[x + 1, y + 1, pl.ds(z + 1, chunk)]

    copies = []
    for hop, to, device in peers:
        for piece in range(pieces):
            for k, (source, target) in enumerate(pairs):
                sem = ((hop - 1) * pieces + piece) * 2 + k
                copies.append(
                    pltpu.make_async_remote_copy(
                        src_ref=source.at[pl.ds(piece * chunk, chunk), to],
                        dst_ref=place(target, piece),
                        send_sem=send_own.at[sem],
                        recv_sem=recv_own.at[sem],
                        device_id=device,
                        device_id_type=pl.DeviceIdType.MESH,
                    )
                )
                copies[-1].start()
    for piece in range(pieces):
        for k, (source, target) in enumerate(pairs):
            kept = pltpu.make_async_copy(
                source.at[pl.ds(piece * chunk, chunk), me], place(target, piece), own_sem.at[piece * 2 + k]
            )
            kept.start()
            copies.append(kept)
    for copy in copies:
        copy.wait()

    lengths = (GRID, GRID, layers)
    rims = []
    for index, (offset, device) in enumerate(neighbours):
        source = tuple(
            pl.ds(1, n) if o == 0 else pl.ds(n if o > 0 else 1, 1)
            for o, n in zip(offset, lengths)
        )
        target = tuple(
            pl.ds(1, n) if o == 0 else pl.ds(0 if o > 0 else n + 1, 1)
            for o, n in zip(offset, lengths)
        )
        for k, ref in enumerate((region, marks)):
            rims.append(
                pltpu.make_async_remote_copy(
                    src_ref=ref.at[source],
                    dst_ref=ref.at[target],
                    send_sem=send_rim.at[index * 2 + k],
                    recv_sem=recv_rim.at[index * 2 + k],
                    device_id=device,
                    device_id_type=pl.DeviceIdType.MESH,
                )
            )
            rims[-1].start()
    for copy in rims:
        copy.wait()


def exchanged(given, ranks):
    coords, charges, _, _, _, tiles = given
    blocks, width = charges.shape
    layers = blocks // (GRID * GRID)
    stride = blocks // ranks
    pieces = stride // math.gcd(stride, layers)
    own = pltpu.SemaphoreType.DMA(((ranks - 1) * pieces * 2,))
    rim = pltpu.SemaphoreType.DMA((52,))
    vmem = pl.BlockSpec(memory_space=pltpu.VMEM)
    cells = (GRID + 2, GRID + 2, layers + 2)
    return pl.pallas_call(
        exchange_kernel,
        out_shape=(
            jax.ShapeDtypeStruct((*cells, 4, width), coords.dtype),
            jax.ShapeDtypeStruct((*cells, 1, width), coords.dtype),
            jax.ShapeDtypeStruct((ROWS, tiles.shape[1] + 2 * EDGE), jnp.int32),
            jax.ShapeDtypeStruct((ROWS, width), coords.dtype),
        ),
        in_specs=[pl.BlockSpec(memory_space=pltpu.HBM)] * 6,
        out_specs=(vmem,) * 4,
        scratch_shapes=[pltpu.VMEM(x.shape, x.dtype) for x in given]
        + [
            pltpu.VMEM((stride, ranks, 4, width), coords.dtype),
            pltpu.VMEM((stride, ranks, 1, width), coords.dtype),
            own,
            own,
            rim,
            rim,
            pltpu.SemaphoreType.DMA((pieces * 2,)),
            pltpu.SemaphoreType.DMA((6,)),
        ],
        compiler_params=pltpu.CompilerParams(
            has_side_effects=True, collective_id=0, vmem_limit_bytes=8 << 20
        ),
    )(*given)


def return_kernel(forces, out, send, recv, own_sem):
    spans, here = spans_of()
    me = here[1] * spans[2] + here[2]
    peers = list(plane_peers(spans, here))
    barrier, greeted = greet([p[2] for p in peers])
    kept = pltpu.make_async_copy(forces.at[:, me], out.at[:, :, me], own_sem.at[0])
    kept.start()
    pl.semaphore_wait(barrier, greeted)
    copies = [kept]
    for hop, to, device in peers:
        copies.append(
            pltpu.make_async_remote_copy(
                src_ref=forces.at[:, to],
                dst_ref=out.at[:, :, me],
                send_sem=send.at[hop - 1],
                recv_sem=recv.at[hop - 1],
                device_id=device,
                device_id_type=pl.DeviceIdType.MESH,
            )
        )
        copies[-1].start()
    for copy in copies:
        copy.wait()


def returned(forces, ranks):
    axes, blocks, width = forces.shape
    stride = blocks // ranks
    sems = pltpu.SemaphoreType.DMA((ranks - 1,))
    vmem = pl.BlockSpec(memory_space=pltpu.VMEM)
    out = pl.pallas_call(
        return_kernel,
        out_shape=jax.ShapeDtypeStruct((axes, stride, ranks, 1, width), forces.dtype),
        in_specs=[vmem],
        out_specs=vmem,
        scratch_shapes=[sems, sems, pltpu.SemaphoreType.DMA((1,))],
        compiler_params=pltpu.CompilerParams(
            has_side_effects=True, collective_id=1, vmem_limit_bytes=4 << 20
        ),
    )(forces.reshape(axes, ranks, stride, 1, width))
    return out.reshape(axes, 1, blocks, width)


def split(value):
    high = value.astype(jnp.bfloat16).astype(jnp.float32)
    rest = value - high
    middle = rest.astype(jnp.bfloat16).astype(jnp.float32)
    return high, middle, rest - middle


def stacked(parts):
    return jnp.concatenate(parts, axis=0).astype(jnp.bfloat16)


def quotient(value, size):
    if size & (size - 1):
        return lax.div(value, size)
    return lax.shift_right_logical(value, size.bit_length() - 1)


def remainder(value, size):
    if size & (size - 1):
        return lax.rem(value, size)
    return value & (size - 1)


def rows_of(shape):
    return lax.broadcasted_iota(jnp.int32, shape, 0)


def row_table(values, shape):
    rows = rows_of(shape)
    out = jnp.zeros(shape, jnp.float32)
    for k, value in enumerate(values):
        if value:
            out = jnp.where(rows == k, jnp.float32(value), out)
    return out


def rising_powers(base, rows):
    two = base * base
    four = two * two
    out = jnp.where(rows % 2 == 1, base, 1.0)
    out = out * jnp.where(rows // 2 % 2 == 1, two, 1.0)
    return out * jnp.where(rows // 4 % 2 == 1, four, 1.0)


def prepare_types(marks, types, sigmas, roots):
    def one(group, carry):
        rows = pl.ds(pl.multiple_of(group * ROWS, ROWS), ROWS)
        kind = marks[rows, :].astype(jnp.int32)
        sigmas[rows, :] = looked_up(types[0:1, :], kind)
        roots[rows, :] = looked_up(types[1:2, :], kind)
        return carry

    lax.fori_loop(0, marks.shape[0] // ROWS, one, 0, unroll=5)


def spread_row(ref, line, shape):
    return jnp.broadcast_to(ref[pl.ds(line, 1), :], shape)


def places(region, line):
    block = jnp.concatenate([region[line], region[line]], axis=0)
    return jnp.where(rows_of(block.shape) % 4 == 3, 1.0, block)


def scaled(region, roots, line, shape):
    charge = jnp.broadcast_to(region[line, 3:4, :], shape)
    return jnp.where(rows_of(shape) < 4, spread_row(roots, line, shape), charge)


def prepare_sources(region, sigmas, roots, sources, weights, moments, edge_terms):
    shape = (ROWS, region.shape[2])
    rows = rows_of(shape)
    count = moments.shape[2]
    ways = row_table([math.comb(6, k) for k in range(7)], shape)
    edge = 1.0 / limit
    high_at = row_table([edge**7 * math.comb(12, k) for k in range(7)], shape)
    low_at = row_table([-(edge**4) * math.comb(6, k) for k in range(7)], shape)
    wide_at = row_table([0.0] + [edge**7 * math.comb(12, k + 6) for k in range(1, 7)], shape)
    near_at = jnp.where(rows == 7, inverse_powers(jnp.full(shape, limit, jnp.float32))[1], 0.0)
    lanes = lax.broadcasted_iota(jnp.int32, (ROWS, count), 1)
    kept = (rows_of((ROWS, count)) >= 4) == (lanes % (2 * ROWS) == 7)

    def spread(line):
        place = places(region, line)
        high, middle, low = split(place * jnp.where(rows < 4, 1.0, place))
        sigma = spread_row(sigmas, line, shape)
        falling = rising_powers(sigma, 6 - jnp.minimum(rows, 6))
        square = sigma * sigma
        top, rest, _ = split(ways * falling)
        sources[line] = stacked([high, middle, high, middle, high, low, top, rest, top, rest])
        top, rest, _ = split(place * scaled(region, roots, line, shape))
        weights[line] = stacked([top, rest])
        first = split(falling * (high_at * (square * square * square) + low_at) + near_at)
        second = split(falling * wide_at)
        edge_terms[line] = stacked([first[0], second[0], first[1], second[1]])

    def summed(line):
        both = lax.dot_general(
            weights[line],
            edge_terms[line],
            (((1,), (1,)), ((), ())),
            preferred_element_type=jnp.float32,
        )
        moments[line] = jnp.where(kept, both[:ROWS] + both[ROWS:], 0.0)

    lines = region.shape[0]
    group = max(n for n in range(1, 25) if lines % n == 0)

    def one(index, carry):
        for k in range(group):
            summed((index - 1) * group + k)
        for k in range(group):
            spread(index * group + k)
        return carry

    for k in range(group):
        spread(k)
    lax.fori_loop(1, lines // group, one, 0)
    for k in range(group):
        summed(lines - group + k)


def prepare_homes(region, sigmas, roots, distances, powers, scales, layers):
    shape = distances.shape[1:]
    rows = rows_of(shape)
    blocks = distances.shape[0] - 1

    def one(block, carry):
        line = own_line(block, layers)
        home = places(region, line)
        distances[block] = jnp.where(rows < 3, -2.0 * home, jnp.where(rows % 4 < 3, 1.0, 0.0))
        top, rest, _ = split(rising_powers(spread_row(sigmas, line, shape), rows))
        powers[block] = stacked([top, top, rest, rest])
        scales[block] = 12.0 * scaled(region, roots, line, shape)
        return carry

    lax.fori_loop(0, blocks, one, 0, unroll=4)
    distances[blocks] = jnp.zeros(shape, jnp.float32)
    powers[blocks] = jnp.zeros(powers.shape[1:], powers.dtype)


def own_line(block, layers):
    x = quotient(block, GRID * layers)
    y = remainder(quotient(block, layers), GRID)
    return ((x + 1) * (GRID + 2) + y + 1) * (layers + 2) + remainder(block, layers) + 1


def prepare_steps(offsets, shifts):
    shape = offsets.shape[1:]
    for step, cells in enumerate(itertools.product((-1, 0, 1), repeat=3)):
        moves = [cell_edge * c for c in cells]
        offsets[step] = row_table([2.0 * m for m in moves], shape)
        shifts[step] = row_table(moves + [0.0] + moves, shape)


def pair_terms(pairs, index, sources, distances, powers, offsets, terms):
    home = pairs[0, index]
    distance = distances[home] + offsets[pairs[2, index]]
    rows = rows_of(distance.shape)
    share = jnp.where(rows < 3, 0.25, jnp.where(rows == 4, soft_core, 0.0))
    square = jnp.sum(distance * distance * share, axis=0, keepdims=True)
    distance = jnp.where(rows == 3, square, distance)
    high, middle, low = split(distance)
    near = stacked([high, high, middle, middle, low, high])
    strong = powers[home]
    width = near.shape[1]
    right = jnp.concatenate(
        [
            jnp.concatenate([near, jnp.zeros((strong.shape[0], width), near.dtype)], axis=0),
            jnp.concatenate([jnp.zeros(near.shape, near.dtype), strong], axis=0),
        ],
        axis=1,
    )
    terms[...] = lax.dot_general(
        sources[pairs[1, index]],
        right,
        (((0,), (0,)), ((), ())),
        preferred_element_type=jnp.float32,
    )


def inverse_powers(softened):
    root = lax.rsqrt(softened)
    one = root * root
    return one, one * root


def strengths(terms, nears, strongs):
    width = terms.shape[0]
    for start in range(0, width, 16):
        rows = pl.ds(start, 16)
        one, near = inverse_powers(jnp.minimum(terms[rows, :width], limit))
        sixth = terms[rows, width:] * (near * near)
        for halves, value in ((nears, near), (strongs, one * (sixth * (sixth - 1.0)))):
            top = value.astype(jnp.bfloat16)
            halves[rows, :] = top
            halves[pl.ds(width + start, 16), :] = (value - top.astype(jnp.float32)).astype(jnp.bfloat16)


def add_forces(pairs, index, weights, moments, shifts, nears, strongs, totals, edges):
    line = pairs[1, index]
    left = weights[line]
    both = jnp.dot(
        jnp.concatenate([left, left], axis=1),
        jnp.concatenate([nears[...], strongs[...]], axis=1),
        preferred_element_type=jnp.float32,
    )
    both = both[:ROWS] + both[ROWS:]
    width = left.shape[1]
    rows = rows_of((ROWS, width))
    summed = jnp.where(rows < 4, both[:, width:], both[:, :width])
    plain = jnp.where(rows < 4, summed[3:4], summed[7:8])
    shift = shifts[pairs[2, index]]
    home = pairs[0, index]
    totals[home] += summed + shift * plain
    shape = moments.shape[1:]
    count = shape[1]
    plain = jnp.where(
        rows[:, :count] < 4,
        jnp.broadcast_to(moments[line, 3:4, :], shape),
        jnp.broadcast_to(moments[line, 7:8, :], shape),
    )
    edges[home] += moments[line] + shift[:, :count] * plain


def force_kernel(
    pairs, region, marks, types, out, totals, sources, weights, moments, distances, powers, scales, edges, edge_terms,
    sigmas, roots, offsets, shifts, *slots
):
    blocks = out.shape[1]
    layers = blocks // (GRID * GRID)
    totals[...] = jnp.zeros_like(totals)
    edges[...] = jnp.zeros_like(edges)
    prepare_types(marks, types, sigmas, roots)
    prepare_steps(offsets, shifts)
    prepare_sources(region, sigmas, roots, sources, weights, moments, edge_terms)
    prepare_homes(region, sigmas, roots, distances, powers, scales, layers)
    terms, nears, strongs = [slots[k : k + BATCH] for k in range(0, 3 * BATCH, BATCH)]

    def step(index, carry):
        first = (index - 1) * BATCH + EDGE

        def push(t, lag):
            add_forces(
                pairs, first - lag + t, weights, moments, shifts, nears[t], strongs[t], totals, edges
            )

        def pull(t):
            strengths(terms[t], nears[t], strongs[t])

        def pair(t):
            pair_terms(pairs, first + BATCH + t, sources, distances, powers, offsets, terms[t])

        for t in range(HALF):
            pull(t)
            push(HALF + t, BATCH)
            pair(t)
        for t in range(HALF):
            pull(HALF + t)
            push(t, 0)
            pair(HALF + t)
        return carry

    groups = -(-(pairs.shape[1] - 2 * EDGE) // BATCH)
    lax.fori_loop(0, groups + 2, step, 0)

    def finish(block, carry):
        line = own_line(block, layers)
        place = places(region, line)
        rows = rows_of(place.shape)
        sigma = spread_row(sigmas, line, place.shape)
        rising = rising_powers(sigma, rows)
        square = sigma * sigma
        first = split(jnp.where(rows == 7, 1.0, rising))
        second = split(rising * (square * square * square))
        right = stacked([first[0], second[0], first[0], second[0], first[1], second[1], first[1], second[1]])
        edge = edges[block]
        left = stacked([*split(edge), jnp.zeros_like(edge)])
        both = jnp.dot(jnp.concatenate([left, left], axis=1), right, preferred_element_type=jnp.float32)
        summed = totals[block] - (both[:ROWS] + both[ROWS : 2 * ROWS] + both[2 * ROWS : 3 * ROWS])
        plain = jnp.where(rows < 4, summed[3:4], summed[7:8])
        force = (place * plain - summed) * scales[block]
        totals[block] = force + pltpu.roll(force, 4, 0)
        return carry

    lax.fori_loop(0, blocks, finish, 0, unroll=16)
    for axis in range(3):
        out[axis] = totals[:blocks, axis, :]


def brick_forces(region, marks, pairs, types, blocks):
    lines, _, width = region.shape
    single = pltpu.VMEM((blocks + 1, ROWS, width), jnp.float32)
    table = pltpu.VMEM((27, ROWS, width), jnp.float32)
    return pl.pallas_call(
        force_kernel,
        out_shape=jax.ShapeDtypeStruct((3, blocks, width), jnp.float32),
        in_specs=[
            pl.BlockSpec(memory_space=pltpu.SMEM),
            pl.BlockSpec(memory_space=pltpu.VMEM),
            pl.BlockSpec(memory_space=pltpu.VMEM),
            pl.BlockSpec(memory_space=pltpu.VMEM),
        ],
        out_specs=pl.BlockSpec(memory_space=pltpu.VMEM),
        scratch_shapes=[
            single,
            pltpu.VMEM((lines, 10 * ROWS, width), jnp.bfloat16),
            pltpu.VMEM((lines, 2 * ROWS, width), jnp.bfloat16),
            pltpu.VMEM((lines, ROWS, 4 * ROWS), jnp.float32),
            single,
            pltpu.VMEM((blocks + 1, 4 * ROWS, width), jnp.bfloat16),
            single,
            pltpu.VMEM((blocks + 1, ROWS, 4 * ROWS), jnp.float32),
            pltpu.VMEM((lines, 4 * ROWS, width), jnp.bfloat16),
            pltpu.VMEM((lines, width), jnp.float32),
            pltpu.VMEM((lines, width), jnp.float32),
            table,
            table,
        ]
        + [pltpu.VMEM((width, 2 * width), jnp.float32)] * BATCH
        + [pltpu.VMEM((2 * width, width), jnp.bfloat16)] * (2 * BATCH),
        compiler_params=pltpu.CompilerParams(vmem_limit_bytes=40 << 20),
    )(pairs, region, marks, types)


def per_device(coords, charges, atom_types, lj_sigma, lj_epsilon, tile_list):
    span_y = lax.axis_size("gy")
    span_z = lax.axis_size("gz")
    blocks = coords.shape[2]
    width = coords.shape[3]
    ranks = span_y * span_z
    given = (coords[:, 0], charges[0], atom_types[0], lj_sigma[None], lj_epsilon[None], tile_list[0, 0, 0])
    region, marks, table, types = exchanged(given, ranks)
    forces = brick_forces(
        region.reshape(-1, 4, width), marks.reshape(-1, width), table, types, blocks
    )
    return returned(forces, ranks)


def solution(mesh):
    return jax.shard_map(
        per_device,
        mesh=mesh,
        in_specs=(
            P(None, "gx", ("gy", "gz"), None),
            P("gx", ("gy", "gz"), None),
            P("gx", ("gy", "gz"), None),
            P(),
            P(),
            P("gx", "gy", "gz", None, None),
        ),
        out_specs=P(None, "gx", ("gy", "gz"), None),
        check_vma=False,
    )
```

```python
import itertools
import math

import jax
import jax.numpy as jnp
from jax import lax
from jax.experimental import pallas as pl
from jax.experimental.pallas import tpu as pltpu
from jax.sharding import PartitionSpec as P

GRID = 4
ROWS = 8
BATCH = 8
LAG = 4
EDGE = 128
STEPS = 32
SHARE = 4096

cell_edge = 11.0
cutoff = 9.0
soft_core = 16.0
coulomb = 332.0636
limit = cutoff * cutoff + soft_core
sigma_scale = 0.5 * 2.0 ** (1.0 / 6.0)
charge_scale = (coulomb / 12.0) ** 0.5


def spans_of():
    names = ("gx", "gy", "gz")
    return [lax.axis_size(n) for n in names], [lax.axis_index(n) for n in names]


def plane_peers(spans, here):
    ranks = spans[1] * spans[2]
    me = here[1] * spans[2] + here[2]
    for hop in range(1, ranks):
        to = lax.rem(me + hop, ranks)
        yield hop, to, (here[0], quotient(to, spans[2]), remainder(to, spans[2]))


def brick_neighbours(spans, here):
    for offset in itertools.product((-1, 0, 1), repeat=3):
        if any(offset):
            yield offset, tuple(lax.rem(at + o + n, n) for at, o, n in zip(here, offset, spans))


def greet(devices):
    barrier = pltpu.get_barrier_semaphore()
    for device in devices:
        pl.semaphore_signal(barrier, inc=1, device_id=device, device_id_type=pl.DeviceIdType.MESH)
    return barrier, len(devices)


def looked_up(values, kinds):
    return jnp.take_along_axis(jnp.broadcast_to(values, kinds.shape), kinds, axis=1)


def pack_atoms(raw, atoms, labels):
    stride, ranks = atoms.shape[:2]
    for group in range(stride):
        rows = pl.ds(group * ranks, ranks)
        for axis in range(3):
            atoms[group, :, axis, :] = raw[axis, rows, :] - 0.5 * cell_edge
        atoms[group, :, 3, :] = raw[3, rows, :] * charge_scale
        labels[group, :, 0, :] = raw[4, rows, :]


def type_table(sigma, epsilon, types):
    empty = jnp.zeros((1, types.shape[1] - sigma.shape[1]), types.dtype)
    types[0:1, :] = jnp.concatenate([sigma[...] * sigma_scale, empty], axis=1)
    types[1:2, :] = jnp.concatenate([jnp.sqrt(epsilon[...]), empty], axis=1)


def cell_of(member, layers):
    return (
        quotient(member, GRID * layers),
        remainder(quotient(member, layers), GRID),
        remainder(member, layers),
    )


def thirds(value, size):
    return sum((value >= k * size).astype(jnp.int32) for k in (1, 2))


def tile_table(tiles, table, blocks, layers):
    home, other = tiles[0:1, :], tiles[1:2, :]
    dead = home < 0
    slot = quotient(jnp.where(dead, 13 * blocks, other), blocks)
    member = remainder(jnp.where(dead, 0, other), blocks)
    far = thirds(slot, 9)
    slot = slot - 9 * far
    middle = thirds(slot, 3)
    steps = (far - 1, middle - 1, slot - 3 * middle - 1)
    sizes = (GRID, GRID, layers)
    own = cell_of(jnp.where(dead, 0, home), layers)
    there = [c + s * n for c, s, n in zip(cell_of(member, layers), steps, sizes)]
    line = ((there[0] + 1) * (GRID + 2) + there[1] + 1) * (layers + 2) + there[2] + 1
    delta = [t - o + 1 for t, o in zip(there, own)]
    width = tiles.shape[1]
    step = (delta[0] * 3 + delta[1]) * 3 + delta[2]
    table[...] = jnp.full(table.shape, blocks * STEPS, jnp.int32)
    table[:, EDGE : EDGE + width] = (line * SHARE + jnp.where(dead, blocks, home)) * STEPS + step


def exchange_kernel(*refs):
    given, (region, marks, table, types), scratch = refs[:4], refs[4:8], refs[8:]
    held, (atoms, labels, send_own, recv_own, send_rim, recv_rim, own_sem, load_sem) = scratch[:4], scratch[4:]
    stride, ranks = atoms.shape[:2]
    layers = region.shape[2] - 2
    blocks = stride * ranks
    spans, here = spans_of()
    me = here[1] * spans[2] + here[2]
    loads = [pltpu.make_async_copy(src, dst, load_sem.at[k]) for k, (src, dst) in enumerate(zip(given, held))]
    for load in loads:
        load.start()
    peers = list(plane_peers(spans, here))
    neighbours = list(brick_neighbours(spans, here))
    barrier, greeted = greet([p[2] for p in peers] + [n[1] for n in neighbours])
    raw, sigma, epsilon, tiles = held
    for load in loads:
        load.wait()
    pack_atoms(raw, atoms, labels)
    tile_table(tiles, table, blocks, layers)
    type_table(sigma, epsilon, types)
    pl.semaphore_wait(barrier, greeted)
    chunk = math.gcd(stride, layers)
    pieces = stride // chunk
    pairs = ((atoms, region), (labels, marks))

    def place(ref, piece):
        x, y, z = cell_of(me * stride + piece * chunk, layers)
        return ref.at[x + 1, y + 1, pl.ds(z + 1, chunk)]

    copies = []
    for hop, to, device in peers:
        for piece in range(pieces):
            for k, (source, target) in enumerate(pairs):
                sem = ((hop - 1) * pieces + piece) * 2 + k
                copies.append(
                    pltpu.make_async_remote_copy(
                        src_ref=source.at[pl.ds(piece * chunk, chunk), to],
                        dst_ref=place(target, piece),
                        send_sem=send_own.at[sem],
                        recv_sem=recv_own.at[sem],
                        device_id=device,
                        device_id_type=pl.DeviceIdType.MESH,
                    )
                )
                copies[-1].start()
    for piece in range(pieces):
        for k, (source, target) in enumerate(pairs):
            kept = pltpu.make_async_copy(
                source.at[pl.ds(piece * chunk, chunk), me], place(target, piece), own_sem.at[piece * 2 + k]
            )
            kept.start()
            copies.append(kept)
    for copy in copies:
        copy.wait()

    lengths = (GRID, GRID, layers)
    rims = []
    for index, (offset, device) in enumerate(neighbours):
        source = tuple(
            pl.ds(1, n) if o == 0 else pl.ds(n if o > 0 else 1, 1)
            for o, n in zip(offset, lengths)
        )
        target = tuple(
            pl.ds(1, n) if o == 0 else pl.ds(0 if o > 0 else n + 1, 1)
            for o, n in zip(offset, lengths)
        )
        for k, ref in enumerate((region, marks)):
            rims.append(
                pltpu.make_async_remote_copy(
                    src_ref=ref.at[source],
                    dst_ref=ref.at[target],
                    send_sem=send_rim.at[index * 2 + k],
                    recv_sem=recv_rim.at[index * 2 + k],
                    device_id=device,
                    device_id_type=pl.DeviceIdType.MESH,
                )
            )
            rims[-1].start()
    for copy in rims:
        copy.wait()


def exchanged(given, ranks):
    raw, _, _, tiles = given
    blocks, width = raw.shape[1:]
    layers = blocks // (GRID * GRID)
    stride = blocks // ranks
    pieces = stride // math.gcd(stride, layers)
    own = pltpu.SemaphoreType.DMA(((ranks - 1) * pieces * 2,))
    rim = pltpu.SemaphoreType.DMA((52,))
    vmem = pl.BlockSpec(memory_space=pltpu.VMEM)
    cells = (GRID + 2, GRID + 2, layers + 2)
    return pl.pallas_call(
        exchange_kernel,
        out_shape=(
            jax.ShapeDtypeStruct((*cells, 4, width), raw.dtype),
            jax.ShapeDtypeStruct((*cells, 1, width), raw.dtype),
            jax.ShapeDtypeStruct((1, tiles.shape[1] + 2 * EDGE), jnp.int32),
            jax.ShapeDtypeStruct((ROWS, width), raw.dtype),
        ),
        in_specs=[pl.BlockSpec(memory_space=pltpu.HBM)] * 4,
        out_specs=(vmem,) * 4,
        scratch_shapes=[pltpu.VMEM(x.shape, x.dtype) for x in given]
        + [
            pltpu.VMEM((stride, ranks, 4, width), raw.dtype),
            pltpu.VMEM((stride, ranks, 1, width), raw.dtype),
            own,
            own,
            rim,
            rim,
            pltpu.SemaphoreType.DMA((pieces * 2,)),
            pltpu.SemaphoreType.DMA((4,)),
        ],
        compiler_params=pltpu.CompilerParams(
            has_side_effects=True, collective_id=0, vmem_limit_bytes=8 << 20
        ),
    )(*given)


def return_kernel(forces, out, send, recv, own_sem):
    spans, here = spans_of()
    me = here[1] * spans[2] + here[2]
    peers = list(plane_peers(spans, here))
    barrier, greeted = greet([p[2] for p in peers])
    kept = pltpu.make_async_copy(forces.at[:, me], out.at[:, :, me], own_sem.at[0])
    kept.start()
    pl.semaphore_wait(barrier, greeted)
    copies = [kept]
    for hop, to, device in peers:
        copies.append(
            pltpu.make_async_remote_copy(
                src_ref=forces.at[:, to],
                dst_ref=out.at[:, :, me],
                send_sem=send.at[hop - 1],
                recv_sem=recv.at[hop - 1],
                device_id=device,
                device_id_type=pl.DeviceIdType.MESH,
            )
        )
        copies[-1].start()
    for copy in copies:
        copy.wait()


def returned(forces, ranks):
    axes, blocks, width = forces.shape
    stride = blocks // ranks
    sems = pltpu.SemaphoreType.DMA((ranks - 1,))
    vmem = pl.BlockSpec(memory_space=pltpu.VMEM)
    out = pl.pallas_call(
        return_kernel,
        out_shape=jax.ShapeDtypeStruct((axes, stride, ranks, 1, width), forces.dtype),
        in_specs=[vmem],
        out_specs=vmem,
        scratch_shapes=[sems, sems, pltpu.SemaphoreType.DMA((1,))],
        compiler_params=pltpu.CompilerParams(
            has_side_effects=True, collective_id=1, vmem_limit_bytes=4 << 20
        ),
    )(forces.reshape(axes, ranks, stride, 1, width))
    return out.reshape(axes, 1, blocks, width)


def split(value):
    high = value.astype(jnp.bfloat16).astype(jnp.float32)
    rest = value - high
    middle = rest.astype(jnp.bfloat16).astype(jnp.float32)
    return high, middle, rest - middle


def stacked(parts):
    return jnp.concatenate(parts, axis=0).astype(jnp.bfloat16)


def quotient(value, size):
    if size & (size - 1):
        return lax.div(value, size)
    return lax.shift_right_logical(value, size.bit_length() - 1)


def remainder(value, size):
    if size & (size - 1):
        return lax.rem(value, size)
    return value & (size - 1)


def rows_of(shape):
    return lax.broadcasted_iota(jnp.int32, shape, 0)


def row_table(values, shape):
    rows = rows_of(shape)
    out = jnp.zeros(shape, jnp.float32)
    for k, value in enumerate(values):
        if value:
            out = jnp.where(rows == k, jnp.float32(value), out)
    return out


def rising_powers(base, rows):
    two = base * base
    four = two * two
    out = jnp.where(rows % 2 == 1, base, 1.0)
    out = out * jnp.where(rows // 2 % 2 == 1, two, 1.0)
    return out * jnp.where(rows // 4 % 2 == 1, four, 1.0)


def prepare_types(marks, types, sigmas, roots):
    def one(group, carry):
        rows = pl.ds(pl.multiple_of(group * ROWS, ROWS), ROWS)
        kind = marks[rows, :].astype(jnp.int32)
        sigmas[rows, :] = looked_up(types[0:1, :], kind)
        roots[rows, :] = looked_up(types[1:2, :], kind)
        return carry

    lax.fori_loop(0, marks.shape[0] // ROWS, one, 0, unroll=15)


def spread_row(ref, line, shape):
    return jnp.broadcast_to(ref[pl.ds(line, 1), :], shape)


def places(region, line):
    block = jnp.concatenate([region[line], region[line]], axis=0)
    return jnp.where(rows_of(block.shape) % 4 == 3, 1.0, block)


def scaled(region, roots, line, shape):
    charge = jnp.broadcast_to(region[line, 3:4, :], shape)
    return jnp.where(rows_of(shape) < 4, spread_row(roots, line, shape), charge)


def prepare_sources(region, sigmas, roots, sources, weights, moments, edge_terms):
    shape = (ROWS, region.shape[2])
    rows = rows_of(shape)
    count = moments.shape[2]
    ways = row_table([math.comb(6, k) for k in range(7)], shape)
    edge = 1.0 / limit
    high_at = row_table([edge**7 * math.comb(12, k) for k in range(7)], shape)
    low_at = row_table([-(edge**4) * math.comb(6, k) for k in range(7)], shape)
    wide_at = row_table([0.0] + [edge**7 * math.comb(12, k + 6) for k in range(1, 7)], shape)
    near_at = jnp.where(rows == 7, inverse_powers(jnp.full(shape, limit, jnp.float32))[1], 0.0)
    lanes = lax.broadcasted_iota(jnp.int32, (ROWS, count), 1)
    kept = (rows_of((ROWS, count)) >= 4) == (lanes % (2 * ROWS) == 7)

    def spread(line):
        place = places(region, line)
        high, middle, low = split(place * jnp.where(rows < 4, 1.0, place))
        sigma = spread_row(sigmas, line, shape)
        falling = rising_powers(sigma, 6 - jnp.minimum(rows, 6))
        square = sigma * sigma
        top, rest, _ = split(ways * falling)
        sources[line] = stacked([high, middle, high, middle, high, low, top, rest, top, rest])
        top, rest, _ = split(place * scaled(region, roots, line, shape))
        weights[line] = stacked([top, rest])
        first = split(falling * (high_at * (square * square * square) + low_at) + near_at)
        second = split(falling * wide_at)
        edge_terms[line] = stacked([first[0], second[0], first[1], second[1]])

    def summed(line):
        both = lax.dot_general(
            weights[line],
            edge_terms[line],
            (((1,), (1,)), ((), ())),
            preferred_element_type=jnp.float32,
        )
        moments[line] = jnp.where(kept, both[:ROWS] + both[ROWS:], 0.0)

    lines = region.shape[0]
    group = max(n for n in range(1, 41) if lines % n == 0)

    def one(index, carry):
        for k in range(group):
            summed((index - 1) * group + k)
        for k in range(group):
            spread(index * group + k)
        return carry

    for k in range(group):
        spread(k)
    lax.fori_loop(1, lines // group, one, 0)
    for k in range(group):
        summed(lines - group + k)


def prepare_homes(region, sigmas, roots, distances, powers, scales, layers):
    shape = distances.shape[1:]
    rows = rows_of(shape)
    blocks = distances.shape[0] - 1

    def one(block, carry):
        line = own_line(block, layers)
        home = places(region, line)
        distances[block] = jnp.where(rows < 3, -2.0 * home, jnp.where(rows % 4 < 3, 1.0, 0.0))
        top, rest, _ = split(rising_powers(spread_row(sigmas, line, shape), rows))
        powers[block] = stacked([top, top, rest, rest])
        scales[block] = 12.0 * scaled(region, roots, line, shape)
        return carry

    lax.fori_loop(0, blocks, one, 0, unroll=16)
    distances[blocks] = jnp.zeros(shape, jnp.float32)
    powers[blocks] = jnp.zeros(powers.shape[1:], powers.dtype)


def own_line(block, layers):
    x = quotient(block, GRID * layers)
    y = remainder(quotient(block, layers), GRID)
    return ((x + 1) * (GRID + 2) + y + 1) * (layers + 2) + remainder(block, layers) + 1


def prepare_steps(offsets, shifts):
    shape = offsets.shape[1:]
    for step, cells in enumerate(itertools.product((-1, 0, 1), repeat=3)):
        moves = [cell_edge * c for c in cells]
        offsets[step] = row_table([2.0 * m for m in moves], shape)
        shifts[step] = row_table(moves + [0.0] + moves, shape)


def unpacked(pairs, index):
    entry = pairs[index]
    return remainder(quotient(entry, STEPS), SHARE), quotient(entry, STEPS * SHARE), remainder(entry, STEPS)


def pair_terms(pairs, index, sources, distances, powers, offsets, terms):
    home, line, step = unpacked(pairs, index)
    distance = distances[home] + offsets[step]
    rows = rows_of(distance.shape)
    share = jnp.where(rows < 3, 0.25, jnp.where(rows == 4, soft_core, 0.0))
    square = jnp.sum(distance * distance * share, axis=0, keepdims=True)
    distance = jnp.where(rows == 3, square, distance)
    high, middle, low = split(distance)
    near = stacked([high, high, middle, middle, low, high])
    strong = powers[home]
    width = near.shape[1]
    right = jnp.concatenate(
        [
            jnp.concatenate([near, jnp.zeros((strong.shape[0], width), near.dtype)], axis=0),
            jnp.concatenate([jnp.zeros(near.shape, near.dtype), strong], axis=0),
        ],
        axis=1,
    )
    terms[...] = lax.dot_general(
        sources[line],
        right,
        (((0,), (0,)), ((), ())),
        preferred_element_type=jnp.float32,
    )


def inverse_powers(softened):
    root = lax.rsqrt(softened)
    one = root * root
    return one, one * root


def strengths(terms, nears, strongs):
    width = terms.shape[0]
    for start in range(0, width, 16):
        rows = pl.ds(start, 16)
        one, near = inverse_powers(jnp.minimum(terms[rows, :width], limit))
        sixth = terms[rows, width:] * (near * near)
        for halves, value in ((nears, near), (strongs, one * (sixth * (sixth - 1.0)))):
            top = value.astype(jnp.bfloat16)
            halves[rows, :] = top
            halves[pl.ds(width + start, 16), :] = (value - top.astype(jnp.float32)).astype(jnp.bfloat16)


def add_forces(pairs, index, weights, moments, shifts, nears, strongs, totals, edges):
    home, line, step = unpacked(pairs, index)
    left = weights[line]
    both = jnp.dot(
        jnp.concatenate([left, left], axis=1),
        jnp.concatenate([nears[...], strongs[...]], axis=1),
        preferred_element_type=jnp.float32,
    )
    both = both[:ROWS] + both[ROWS:]
    width = left.shape[1]
    rows = rows_of((ROWS, width))
    summed = jnp.where(rows < 4, both[:, width:], both[:, :width])
    plain = jnp.where(rows < 4, summed[3:4], summed[7:8])
    shift = shifts[step]
    totals[home] += summed + shift * plain
    shape = moments.shape[1:]
    count = shape[1]
    plain = jnp.where(
        rows[:, :count] < 4,
        jnp.broadcast_to(moments[line, 3:4, :], shape),
        jnp.broadcast_to(moments[line, 7:8, :], shape),
    )
    edges[home] += moments[line] + shift[:, :count] * plain


def force_kernel(
    pairs, region, marks, types, out, totals, sources, weights, moments, distances, powers, scales, edges, edge_terms,
    sigmas, roots, offsets, shifts, *slots
):
    blocks = out.shape[1]
    layers = blocks // (GRID * GRID)
    totals[...] = jnp.zeros_like(totals)
    edges[...] = jnp.zeros_like(edges)
    prepare_types(marks, types, sigmas, roots)
    prepare_steps(offsets, shifts)
    prepare_sources(region, sigmas, roots, sources, weights, moments, edge_terms)
    prepare_homes(region, sigmas, roots, distances, powers, scales, layers)
    terms, nears, strongs = [slots[k : k + BATCH] for k in range(0, 3 * BATCH, BATCH)]

    def step(index, carry):
        first = (index - 1) * BATCH + EDGE

        def push(t, lag):
            add_forces(
                pairs, first - lag + t, weights, moments, shifts, nears[t], strongs[t], totals, edges
            )

        def pull(t):
            strengths(terms[t], nears[t], strongs[t])

        def pair(t):
            pair_terms(pairs, first + BATCH + t, sources, distances, powers, offsets, terms[t])

        for t in range(BATCH):
            pull(t)
            push((t - LAG) % BATCH, BATCH if t < LAG else 0)
            pair(t)
        return carry

    groups = -(-(pairs.shape[0] - 2 * EDGE) // BATCH)
    lax.fori_loop(0, groups + 2, step, 0)

    def finish(block, carry):
        line = own_line(block, layers)
        place = places(region, line)
        rows = rows_of(place.shape)
        sigma = spread_row(sigmas, line, place.shape)
        rising = rising_powers(sigma, rows)
        square = sigma * sigma
        first = split(jnp.where(rows == 7, 1.0, rising))
        second = split(rising * (square * square * square))
        right = stacked([first[0], second[0], first[0], second[0], first[1], second[1], first[1], second[1]])
        edge = edges[block]
        left = stacked([*split(edge), jnp.zeros_like(edge)])
        both = jnp.dot(jnp.concatenate([left, left], axis=1), right, preferred_element_type=jnp.float32)
        summed = totals[block] - (both[:ROWS] + both[ROWS : 2 * ROWS] + both[2 * ROWS : 3 * ROWS])
        plain = jnp.where(rows < 4, summed[3:4], summed[7:8])
        force = (place * plain - summed) * scales[block]
        totals[block] = force + pltpu.roll(force, 4, 0)
        return carry

    lax.fori_loop(0, blocks, finish, 0, unroll=64)
    for axis in range(3):
        out[axis] = totals[:blocks, axis, :]


def brick_forces(region, marks, pairs, types, blocks):
    lines, _, width = region.shape
    single = pltpu.VMEM((blocks + 1, ROWS, width), jnp.float32)
    table = pltpu.VMEM((27, ROWS, width), jnp.float32)
    return pl.pallas_call(
        force_kernel,
        out_shape=jax.ShapeDtypeStruct((3, blocks, width), jnp.float32),
        in_specs=[
            pl.BlockSpec(memory_space=pltpu.SMEM),
            pl.BlockSpec(memory_space=pltpu.VMEM),
            pl.BlockSpec(memory_space=pltpu.VMEM),
            pl.BlockSpec(memory_space=pltpu.VMEM),
        ],
        out_specs=pl.BlockSpec(memory_space=pltpu.VMEM),
        scratch_shapes=[
            single,
            pltpu.VMEM((lines, 10 * ROWS, width), jnp.bfloat16),
            pltpu.VMEM((lines, 2 * ROWS, width), jnp.bfloat16),
            pltpu.VMEM((lines, ROWS, 4 * ROWS), jnp.float32),
            single,
            pltpu.VMEM((blocks + 1, 4 * ROWS, width), jnp.bfloat16),
            single,
            pltpu.VMEM((blocks + 1, ROWS, 4 * ROWS), jnp.float32),
            pltpu.VMEM((lines, 4 * ROWS, width), jnp.bfloat16),
            pltpu.VMEM((lines, width), jnp.float32),
            pltpu.VMEM((lines, width), jnp.float32),
            table,
            table,
        ]
        + [pltpu.VMEM((width, 2 * width), jnp.float32)] * BATCH
        + [pltpu.VMEM((2 * width, width), jnp.bfloat16)] * (2 * BATCH),
        compiler_params=pltpu.CompilerParams(vmem_limit_bytes=40 << 20),
    )(pairs, region, marks, types)


def per_device(coords, charges, atom_types, lj_sigma, lj_epsilon, tile_list):
    span_y = lax.axis_size("gy")
    span_z = lax.axis_size("gz")
    blocks = coords.shape[2]
    width = coords.shape[3]
    ranks = span_y * span_z
    raw = jnp.concatenate([coords[:, 0], charges, atom_types.astype(coords.dtype)], axis=0)
    given = (raw, lj_sigma[None], lj_epsilon[None], tile_list[0, 0, 0])
    region, marks, table, types = exchanged(given, ranks)
    forces = brick_forces(
        region.reshape(-1, 4, width), marks.reshape(-1, width), table.reshape(-1), types, blocks
    )
    return returned(forces, ranks)


def solution(mesh):
    return jax.shard_map(
        per_device,
        mesh=mesh,
        in_specs=(
            P(None, "gx", ("gy", "gz"), None),
            P("gx", ("gy", "gz"), None),
            P("gx", ("gy", "gz"), None),
            P(),
            P(),
            P("gx", "gy", "gz", None, None),
        ),
        out_specs=P(None, "gx", ("gy", "gz"), None),
        check_vma=False,
    )
```

```python
import itertools
import math

import jax
import jax.numpy as jnp
from jax import lax
from jax.experimental import pallas as pl
from jax.experimental.pallas import tpu as pltpu
from jax.sharding import PartitionSpec as P

GRID = 4
ROWS = 8
BATCH = 8
LAG = 4
EDGE = 128
STEPS = 32
SHARE = 4096

cell_edge = 11.0
cutoff = 9.0
soft_core = 16.0
coulomb = 332.0636
limit = cutoff * cutoff + soft_core
sigma_scale = 0.5 * 2.0 ** (1.0 / 6.0)
charge_scale = (coulomb / 12.0) ** 0.5


def spans_of():
    names = ("gx", "gy", "gz")
    return [lax.axis_size(n) for n in names], [lax.axis_index(n) for n in names]


def plane_peers(spans, here):
    ranks = spans[1] * spans[2]
    me = here[1] * spans[2] + here[2]
    for hop in range(1, ranks):
        to = lax.rem(me + hop, ranks)
        yield hop, to, (here[0], quotient(to, spans[2]), remainder(to, spans[2]))


def brick_neighbours(spans, here):
    for offset in itertools.product((-1, 0, 1), repeat=3):
        if any(offset):
            yield offset, tuple(lax.rem(at + o + n, n) for at, o, n in zip(here, offset, spans))


def greet(devices):
    barrier = pltpu.get_barrier_semaphore()
    for device in devices:
        pl.semaphore_signal(barrier, inc=1, device_id=device, device_id_type=pl.DeviceIdType.MESH)
    return barrier, len(devices)


def looked_up(values, kinds):
    return jnp.take_along_axis(jnp.broadcast_to(values, kinds.shape), kinds, axis=1)


def pack_atoms(raw, kinds, atoms, labels):
    stride, ranks = atoms.shape[:2]
    for group in range(stride):
        rows = pl.ds(group * ranks, ranks)
        for axis in range(3):
            atoms[group, :, axis, :] = raw[axis, rows, :] - 0.5 * cell_edge
        atoms[group, :, 3, :] = raw[3, rows, :] * charge_scale
        labels[group, :, 0, :] = kinds[rows, :].astype(jnp.float32)


def type_table(sigma, epsilon, types):
    empty = jnp.zeros((1, types.shape[1] - sigma.shape[1]), types.dtype)
    types[0:1, :] = jnp.concatenate([sigma[...] * sigma_scale, empty], axis=1)
    types[1:2, :] = jnp.concatenate([jnp.sqrt(epsilon[...]), empty], axis=1)


def cell_of(member, layers):
    return (
        quotient(member, GRID * layers),
        remainder(quotient(member, layers), GRID),
        remainder(member, layers),
    )


def thirds(value, size):
    return sum((value >= k * size).astype(jnp.int32) for k in (1, 2))


def tile_table(tiles, table, blocks, layers):
    home, other = tiles[0:1, :], tiles[1:2, :]
    dead = home < 0
    slot = quotient(jnp.where(dead, 13 * blocks, other), blocks)
    member = remainder(jnp.where(dead, 0, other), blocks)
    far = thirds(slot, 9)
    slot = slot - 9 * far
    middle = thirds(slot, 3)
    steps = (far - 1, middle - 1, slot - 3 * middle - 1)
    sizes = (GRID, GRID, layers)
    own = cell_of(jnp.where(dead, 0, home), layers)
    there = [c + s * n for c, s, n in zip(cell_of(member, layers), steps, sizes)]
    line = ((there[0] + 1) * (GRID + 2) + there[1] + 1) * (layers + 2) + there[2] + 1
    delta = [t - o + 1 for t, o in zip(there, own)]
    width = tiles.shape[1]
    step = (delta[0] * 3 + delta[1]) * 3 + delta[2]
    table[...] = jnp.full(table.shape, blocks * STEPS, jnp.int32)
    table[:, EDGE : EDGE + width] = (line * SHARE + jnp.where(dead, blocks, home)) * STEPS + step


def exchange_kernel(*refs):
    given, outs, scratch = refs[:5], refs[5:18], refs[18:]
    region, marks, table, types, sources, weights, edge_terms, moments, *homes, offsets, shifts = outs
    held, (atoms, labels, send_own, recv_own, send_rim, recv_rim, own_sem, load_sem) = scratch[:5], scratch[5:]
    stride, ranks = atoms.shape[:2]
    layers = region.shape[2] - 2
    blocks = stride * ranks
    spans, here = spans_of()
    me = here[1] * spans[2] + here[2]
    loads = [pltpu.make_async_copy(src, dst, load_sem.at[k]) for k, (src, dst) in enumerate(zip(given, held))]
    for load in loads:
        load.start()
    peers = list(plane_peers(spans, here))
    neighbours = list(brick_neighbours(spans, here))
    barrier, greeted = greet([p[2] for p in peers] + [n[1] for n in neighbours])
    raw, kinds, sigma, epsilon, tiles = held
    for load in loads:
        load.wait()
    pack_atoms(raw, kinds, atoms, labels)
    tile_table(tiles, table, blocks, layers)
    type_table(sigma, epsilon, types)
    pl.semaphore_wait(barrier, greeted)
    chunk = math.gcd(stride, layers)
    pieces = stride // chunk
    pairs = ((atoms, region), (labels, marks))

    def place(ref, piece):
        x, y, z = cell_of(me * stride + piece * chunk, layers)
        return ref.at[x + 1, y + 1, pl.ds(z + 1, chunk)]

    copies = []
    for hop, to, device in peers:
        for piece in range(pieces):
            for k, (source, target) in enumerate(pairs):
                sem = ((hop - 1) * pieces + piece) * 2 + k
                copies.append(
                    pltpu.make_async_remote_copy(
                        src_ref=source.at[pl.ds(piece * chunk, chunk), to],
                        dst_ref=place(target, piece),
                        send_sem=send_own.at[sem],
                        recv_sem=recv_own.at[sem],
                        device_id=device,
                        device_id_type=pl.DeviceIdType.MESH,
                    )
                )
                copies[-1].start()
    for piece in range(pieces):
        for k, (source, target) in enumerate(pairs):
            kept = pltpu.make_async_copy(
                source.at[pl.ds(piece * chunk, chunk), me], place(target, piece), own_sem.at[piece * 2 + k]
            )
            kept.start()
            copies.append(kept)
    for copy in copies:
        copy.wait()

    lengths = (GRID, GRID, layers)
    rims = []
    for index, (offset, device) in enumerate(neighbours):
        source = tuple(
            pl.ds(1, n) if o == 0 else pl.ds(n if o > 0 else 1, 1)
            for o, n in zip(offset, lengths)
        )
        target = tuple(
            pl.ds(1, n) if o == 0 else pl.ds(0 if o > 0 else n + 1, 1)
            for o, n in zip(offset, lengths)
        )
        for k, ref in enumerate((region, marks)):
            rims.append(
                pltpu.make_async_remote_copy(
                    src_ref=ref.at[source],
                    dst_ref=ref.at[target],
                    send_sem=send_rim.at[index * 2 + k],
                    recv_sem=recv_rim.at[index * 2 + k],
                    device_id=device,
                    device_id_type=pl.DeviceIdType.MESH,
                )
            )
            rims[-1].start()
    prepare_steps(offsets, shifts)
    prepare_own(region, marks, types, sources, weights, edge_terms, moments, *homes)
    for copy in rims:
        copy.wait()


def exchanged(given, ranks):
    raw, _, _, _, tiles = given
    blocks, width = raw.shape[1:]
    layers = blocks // (GRID * GRID)
    stride = blocks // ranks
    pieces = stride // math.gcd(stride, layers)
    own = pltpu.SemaphoreType.DMA(((ranks - 1) * pieces * 2,))
    rim = pltpu.SemaphoreType.DMA((52,))
    vmem = pl.BlockSpec(memory_space=pltpu.VMEM)
    cells = (GRID + 2, GRID + 2, layers + 2)
    lines = math.prod(cells)
    entries = blocks + 4
    single = jax.ShapeDtypeStruct((entries, ROWS, width), jnp.float32)
    steps = jax.ShapeDtypeStruct((28, ROWS, width), jnp.float32)
    return pl.pallas_call(
        exchange_kernel,
        out_shape=(
            jax.ShapeDtypeStruct((*cells, 4, width), raw.dtype),
            jax.ShapeDtypeStruct((*cells, 1, width), raw.dtype),
            jax.ShapeDtypeStruct((1, tiles.shape[1] + 2 * EDGE), jnp.int32),
            jax.ShapeDtypeStruct((ROWS, width), raw.dtype),
            jax.ShapeDtypeStruct((lines, 10 * ROWS, width), jnp.bfloat16),
            jax.ShapeDtypeStruct((lines, 2 * ROWS, width), jnp.bfloat16),
            jax.ShapeDtypeStruct((lines, 4 * ROWS, width), jnp.bfloat16),
            jax.ShapeDtypeStruct((lines, ROWS, 4 * ROWS), jnp.float32),
            single,
            jax.ShapeDtypeStruct((entries, 4 * ROWS, width), jnp.bfloat16),
            single,
            steps,
            steps,
        ),
        in_specs=[pl.BlockSpec(memory_space=pltpu.HBM)] * 5,
        out_specs=(vmem,) * 13,
        scratch_shapes=[pltpu.VMEM(x.shape, x.dtype) for x in given]
        + [
            pltpu.VMEM((stride, ranks, 4, width), raw.dtype),
            pltpu.VMEM((stride, ranks, 1, width), raw.dtype),
            own,
            own,
            rim,
            rim,
            pltpu.SemaphoreType.DMA((pieces * 2,)),
            pltpu.SemaphoreType.DMA((5,)),
        ],
        compiler_params=pltpu.CompilerParams(
            has_side_effects=True, collective_id=0, vmem_limit_bytes=8 << 20
        ),
    )(*given)


def return_kernel(forces, out, send, recv, own_sem):
    spans, here = spans_of()
    me = here[1] * spans[2] + here[2]
    peers = list(plane_peers(spans, here))
    barrier, greeted = greet([p[2] for p in peers])
    kept = pltpu.make_async_copy(forces.at[:, me], out.at[:, :, me], own_sem.at[0])
    kept.start()
    pl.semaphore_wait(barrier, greeted)
    copies = [kept]
    for hop, to, device in peers:
        copies.append(
            pltpu.make_async_remote_copy(
                src_ref=forces.at[:, to],
                dst_ref=out.at[:, :, me],
                send_sem=send.at[hop - 1],
                recv_sem=recv.at[hop - 1],
                device_id=device,
                device_id_type=pl.DeviceIdType.MESH,
            )
        )
        copies[-1].start()
    for copy in copies:
        copy.wait()


def returned(forces, ranks):
    axes, blocks, width = forces.shape
    stride = blocks // ranks
    sems = pltpu.SemaphoreType.DMA((ranks - 1,))
    vmem = pl.BlockSpec(memory_space=pltpu.VMEM)
    out = pl.pallas_call(
        return_kernel,
        out_shape=jax.ShapeDtypeStruct((axes, stride, ranks, 1, width), forces.dtype),
        in_specs=[vmem],
        out_specs=vmem,
        scratch_shapes=[sems, sems, pltpu.SemaphoreType.DMA((1,))],
        compiler_params=pltpu.CompilerParams(
            has_side_effects=True, collective_id=1, vmem_limit_bytes=4 << 20
        ),
    )(forces.reshape(axes, ranks, stride, 1, width))
    return out.reshape(axes, 1, blocks, width)


def split(value):
    high = value.astype(jnp.bfloat16).astype(jnp.float32)
    rest = value - high
    middle = rest.astype(jnp.bfloat16).astype(jnp.float32)
    return high, middle, rest - middle


def stacked(parts):
    return jnp.concatenate(parts, axis=0).astype(jnp.bfloat16)


def quotient(value, size):
    if size & (size - 1):
        return lax.div(value, size)
    return lax.shift_right_logical(value, size.bit_length() - 1)


def remainder(value, size):
    if size & (size - 1):
        return lax.rem(value, size)
    return value & (size - 1)


def rows_of(shape):
    return lax.broadcasted_iota(jnp.int32, shape, 0)


def row_table(values, shape):
    rows = rows_of(shape)
    out = jnp.zeros(shape, jnp.float32)
    for k, value in enumerate(values):
        if value:
            out = jnp.where(rows == k, jnp.float32(value), out)
    return out


def rising_powers(base, rows):
    two = base * base
    four = two * two
    out = jnp.where(rows % 2 == 1, base, 1.0)
    out = out * jnp.where(rows // 2 % 2 == 1, two, 1.0)
    return out * jnp.where(rows // 4 % 2 == 1, four, 1.0)


def places(region, at):
    block = region[at]
    block = jnp.concatenate([block, block], axis=0)
    return jnp.where(rows_of(block.shape) % 4 == 3, 1.0, block)


def type_rows(marks, types, at, shape):
    kind = jnp.broadcast_to(marks[(*at, slice(0, 1))], shape).astype(jnp.int32)
    return looked_up(types[0:1, :], kind), looked_up(types[1:2, :], kind)


class Preparation:
    def __init__(self, region, marks, types, sources, weights, edge_terms, moments):
        self.refs = region, marks, types, sources, weights, edge_terms, moments
        self.shape = shape = (ROWS, region.shape[-1])
        self.rows = rows = rows_of(shape)
        edge = 1.0 / limit
        self.ways = row_table([math.comb(6, k) for k in range(7)], shape)
        self.high_at = row_table([edge**7 * math.comb(12, k) for k in range(7)], shape)
        self.low_at = row_table([-(edge**4) * math.comb(6, k) for k in range(7)], shape)
        self.wide_at = row_table([0.0] + [edge**7 * math.comb(12, k + 6) for k in range(1, 7)], shape)
        self.near_at = jnp.where(rows == 7, inverse_powers(jnp.full(shape, limit, jnp.float32))[1], 0.0)
        count = moments.shape[2]
        lanes = lax.broadcasted_iota(jnp.int32, (ROWS, count), 1)
        self.kept = (rows_of((ROWS, count)) >= 4) == (lanes % (2 * ROWS) == 7)

    def source(self, at, line):
        region, marks, types, sources, weights, edge_terms, _ = self.refs
        rows = self.rows
        place = places(region, at)
        sigma, root = type_rows(marks, types, at, self.shape)
        charge = jnp.broadcast_to(region[(*at, slice(3, 4))], self.shape)
        scale = jnp.where(rows < 4, root, charge)
        high, middle, low = split(place * jnp.where(rows < 4, 1.0, place))
        falling = rising_powers(sigma, 6 - jnp.minimum(rows, 6))
        square = sigma * sigma
        top, rest, _ = split(self.ways * falling)
        sources[line] = stacked([high, middle, high, middle, high, low, top, rest, top, rest])
        top, rest, _ = split(place * scale)
        weights[line] = stacked([top, rest])
        first = split(falling * (self.high_at * (square * square * square) + self.low_at) + self.near_at)
        second = split(falling * self.wide_at)
        edge_terms[line] = stacked([first[0], second[0], first[1], second[1]])
        return place, sigma, scale

    def moment(self, line):
        _, _, _, _, weights, edge_terms, moments = self.refs
        both = lax.dot_general(
            weights[line],
            edge_terms[line],
            (((1,), (1,)), ((), ())),
            preferred_element_type=jnp.float32,
        )
        moments[line] = jnp.where(self.kept, both[:ROWS] + both[ROWS:], 0.0)


def prepare_own(region, marks, types, sources, weights, edge_terms, moments, distances, powers, scales):
    prepared = Preparation(region, marks, types, sources, weights, edge_terms, moments)
    rows = prepared.rows
    layers = region.shape[2] - 2
    column = [(y, z) for y in range(GRID) for z in range(layers)]

    def line_of(x, y, z):
        return ((x + 1) * (GRID + 2) + y + 1) * (layers + 2) + z + 1

    def fill(x):
        for k, (y, z) in enumerate(column):
            home, sigma, scale = prepared.source((x + 1, y + 1, z + 1), line_of(x, y, z))
            block = x * len(column) + k
            distances[block] = jnp.where(rows < 3, -2.0 * home, jnp.where(rows % 4 < 3, 1.0, 0.0))
            top, rest, _ = split(rising_powers(sigma, rows))
            powers[block] = stacked([top, top, rest, rest])
            scales[block] = 12.0 * scale

    def add(x):
        for y, z in column:
            prepared.moment(line_of(x, y, z))

    def one(x, carry):
        add(x - 1)
        fill(x)
        return carry

    fill(0)
    lax.fori_loop(1, GRID, one, 0)
    add(GRID - 1)
    blocks = GRID * len(column)
    distances[blocks] = jnp.zeros(distances.shape[1:], jnp.float32)
    powers[blocks] = jnp.zeros(powers.shape[1:], powers.dtype)


def prepare_rim(region, marks, types, sources, weights, edge_terms, moments, layers):
    prepared = Preparation(region, marks, types, sources, weights, edge_terms, moments)
    depth = layers + 2
    side = (GRID + 2) * depth
    part = -(-side // GRID)
    inner = [y * depth + z for y in range(GRID + 2) for z in range(depth)]
    inner = [k for k in inner if k // depth in (0, GRID + 1) or k % depth in (0, depth - 1)]

    def lines(index):
        ends = [jnp.minimum(index * part + k, side - 1) for k in range(part)]
        far = [k + (GRID + 1) * side for k in ends]
        return ends + far + [(index + 1) * side + k for k in inner]

    def one(index, carry):
        for line in lines(index - 1):
            prepared.moment(line)
        for line in lines(index):
            prepared.source((line,), line)
        return carry

    for line in lines(0):
        prepared.source((line,), line)
    lax.fori_loop(1, GRID, one, 0)
    for line in lines(GRID - 1):
        prepared.moment(line)


def own_line(block, layers):
    x = quotient(block, GRID * layers)
    y = remainder(quotient(block, layers), GRID)
    return ((x + 1) * (GRID + 2) + y + 1) * (layers + 2) + remainder(block, layers) + 1


def prepare_steps(offsets, shifts):
    shape = offsets.shape[1:]
    for step, cells in enumerate(itertools.product((-1, 0, 1), repeat=3)):
        moves = [cell_edge * c for c in cells]
        offsets[step] = row_table([2.0 * m for m in moves], shape)
        shifts[step] = row_table(moves + [0.0] + moves, shape)


def unpacked(pairs, index):
    entry = pairs[0, index]
    return remainder(quotient(entry, STEPS), SHARE), quotient(entry, STEPS * SHARE), remainder(entry, STEPS)


def pair_terms(pairs, index, sources, distances, powers, offsets, terms):
    home, line, step = unpacked(pairs, index)
    distance = distances[home] + offsets[step]
    rows = rows_of(distance.shape)
    share = jnp.where(rows < 3, 0.25, jnp.where(rows == 4, soft_core, 0.0))
    square = jnp.sum(distance * distance * share, axis=0, keepdims=True)
    distance = jnp.where(rows == 3, square, distance)
    high, middle, low = split(distance)
    near = stacked([high, high, middle, middle, low, high])
    strong = powers[home]
    width = near.shape[1]
    right = jnp.concatenate(
        [
            jnp.concatenate([near, jnp.zeros((strong.shape[0], width), near.dtype)], axis=0),
            jnp.concatenate([jnp.zeros(near.shape, near.dtype), strong], axis=0),
        ],
        axis=1,
    )
    terms[...] = lax.dot_general(
        sources[line],
        right,
        (((0,), (0,)), ((), ())),
        preferred_element_type=jnp.float32,
    )


def inverse_powers(softened):
    root = lax.rsqrt(softened)
    one = root * root
    return one, one * root


def strengths(terms, nears, strongs):
    width = terms.shape[0]
    for start in range(0, width, 16):
        rows = pl.ds(start, 16)
        one, near = inverse_powers(jnp.minimum(terms[rows, :width], limit))
        sixth = terms[rows, width:] * (near * near)
        for halves, value in ((nears, near), (strongs, one * (sixth * (sixth - 1.0)))):
            top = value.astype(jnp.bfloat16)
            halves[rows, :] = top
            halves[pl.ds(width + start, 16), :] = (value - top.astype(jnp.float32)).astype(jnp.bfloat16)


def add_forces(pairs, index, weights, moments, shifts, nears, strongs, totals, edges):
    home, line, step = unpacked(pairs, index)
    left = weights[line]
    both = jnp.dot(
        jnp.concatenate([left, left], axis=1),
        jnp.concatenate([nears[...], strongs[...]], axis=1),
        preferred_element_type=jnp.float32,
    )
    both = both[:ROWS] + both[ROWS:]
    width = left.shape[1]
    rows = rows_of((ROWS, width))
    summed = jnp.where(rows < 4, both[:, width:], both[:, :width])
    plain = jnp.where(rows < 4, summed[3:4], summed[7:8])
    shift = shifts[step]
    totals[home] += summed + shift * plain
    shape = moments.shape[1:]
    count = shape[1]
    plain = jnp.where(
        rows[:, :count] < 4,
        jnp.broadcast_to(moments[line, 3:4, :], shape),
        jnp.broadcast_to(moments[line, 7:8, :], shape),
    )
    edges[home] += moments[line] + shift[:, :count] * plain


def force_kernel(
    pairs, region, marks, types, _, _w, _t, _m, distances, powers, scales, offsets, shifts,
    out, sources, weights, edge_terms, moments, totals, edges, *slots
):
    blocks = out.shape[1]
    layers = blocks // (GRID * GRID)
    totals[...] = jnp.zeros_like(totals)
    edges[...] = jnp.zeros_like(edges)
    prepare_rim(region, marks, types, sources, weights, edge_terms, moments, layers)
    terms, nears, strongs = [slots[k : k + BATCH] for k in range(0, 3 * BATCH, BATCH)]

    def step(index, carry):
        first = (index - 1) * BATCH + EDGE

        def push(t, lag):
            add_forces(
                pairs, first - lag + t, weights, moments, shifts, nears[t], strongs[t], totals, edges
            )

        def pull(t):
            strengths(terms[t], nears[t], strongs[t])

        def pair(t):
            pair_terms(pairs, first + BATCH + t, sources, distances, powers, offsets, terms[t])

        for t in range(BATCH):
            pull(t)
            push((t - LAG) % BATCH, BATCH if t < LAG else 0)
            pair(t)
        return carry

    groups = -(-(pairs.shape[1] - 2 * EDGE) // BATCH)
    lax.fori_loop(0, groups + 2, step, 0)

    def finish(block, carry):
        line = own_line(block, layers)
        place = places(region, (line,))
        rows = rows_of(place.shape)
        sigma, _ = type_rows(marks, types, (line,), place.shape)
        rising = rising_powers(sigma, rows)
        square = sigma * sigma
        first = split(jnp.where(rows == 7, 1.0, rising))
        second = split(rising * (square * square * square))
        right = stacked([first[0], second[0], first[0], second[0], first[1], second[1], first[1], second[1]])
        edge = edges[block]
        left = stacked([*split(edge), jnp.zeros_like(edge)])
        both = jnp.dot(jnp.concatenate([left, left], axis=1), right, preferred_element_type=jnp.float32)
        summed = totals[block] - (both[:ROWS] + both[ROWS : 2 * ROWS] + both[2 * ROWS : 3 * ROWS])
        plain = jnp.where(rows < 4, summed[3:4], summed[7:8])
        force = (place * plain - summed) * scales[block]
        totals[block] = force + pltpu.roll(force, 4, 0)
        return carry

    lax.fori_loop(0, blocks, finish, 0, unroll=64)
    for axis in range(3):
        out[axis] = totals[:blocks, axis, :]


def brick_forces(pairs, region, marks, types, prepared, homes, blocks):
    width = region.shape[2]
    entries = homes[0].shape[0]
    vmem = pl.BlockSpec(memory_space=pltpu.VMEM)
    return pl.pallas_call(
        force_kernel,
        out_shape=(jax.ShapeDtypeStruct((3, blocks, width), jnp.float32),)
        + tuple(jax.ShapeDtypeStruct(x.shape, x.dtype) for x in prepared),
        in_specs=[pl.BlockSpec(memory_space=pltpu.SMEM)] + [vmem] * (3 + len(prepared) + len(homes)),
        out_specs=(vmem,) * (1 + len(prepared)),
        input_output_aliases={4 + k: 1 + k for k in range(len(prepared))},
        scratch_shapes=[
            pltpu.VMEM((entries, ROWS, width), jnp.float32),
            pltpu.VMEM((entries, ROWS, 4 * ROWS), jnp.float32),
        ]
        + [pltpu.VMEM((width, 2 * width), jnp.float32)] * BATCH
        + [pltpu.VMEM((2 * width, width), jnp.bfloat16)] * (2 * BATCH),
        compiler_params=pltpu.CompilerParams(vmem_limit_bytes=16 << 20),
    )(pairs, region, marks, types, *prepared, *homes)[0]


def per_device(coords, charges, atom_types, lj_sigma, lj_epsilon, tile_list):
    span_y = lax.axis_size("gy")
    span_z = lax.axis_size("gz")
    blocks = coords.shape[2]
    width = coords.shape[3]
    ranks = span_y * span_z
    raw = jnp.concatenate([coords[:, 0], charges], axis=0)
    given = (raw, atom_types[0], lj_sigma[None], lj_epsilon[None], tile_list[0, 0, 0])
    region, marks, table, types, *rest = exchanged(given, ranks)
    forces = brick_forces(
        table,
        region.reshape(-1, 4, width),
        marks.reshape(-1, 1, width),
        types,
        rest[:4],
        rest[4:],
        blocks,
    )
    return returned(forces, ranks)


def solution(mesh):
    return jax.shard_map(
        per_device,
        mesh=mesh,
        in_specs=(
            P(None, "gx", ("gy", "gz"), None),
            P("gx", ("gy", "gz"), None),
            P("gx", ("gy", "gz"), None),
            P(),
            P(),
            P("gx", "gy", "gz", None, None),
        ),
        out_specs=P(None, "gx", ("gy", "gz"), None),
        check_vma=False,
    )
```

```python
import itertools
import math

import jax
import jax.numpy as jnp
from jax import lax
from jax.experimental import pallas as pl
from jax.experimental.pallas import tpu as pltpu
from jax.sharding import PartitionSpec as P

GRID = 4
ROWS = 8
BATCH = 8
LAG = 4
EDGE = 128
STEPS = 32
SHARE = 4096

cell_edge = 11.0
cutoff = 9.0
soft_core = 16.0
coulomb = 332.0636
limit = cutoff * cutoff + soft_core
sigma_scale = 0.5 * 2.0 ** (1.0 / 6.0)
charge_scale = (coulomb / 12.0) ** 0.5


def spans_of():
    names = ("gx", "gy", "gz")
    return [lax.axis_size(n) for n in names], [lax.axis_index(n) for n in names]


def plane_peers(spans, here):
    ranks = spans[1] * spans[2]
    me = here[1] * spans[2] + here[2]
    for hop in range(1, ranks):
        to = lax.rem(me + hop, ranks)
        yield hop, to, (here[0], quotient(to, spans[2]), remainder(to, spans[2]))


def brick_neighbours(spans, here):
    for offset in itertools.product((-1, 0, 1), repeat=3):
        if any(offset):
            yield offset, tuple(lax.rem(at + o + n, n) for at, o, n in zip(here, offset, spans))


def greet(devices):
    barrier = pltpu.get_barrier_semaphore()
    for device in devices:
        pl.semaphore_signal(barrier, inc=1, device_id=device, device_id_type=pl.DeviceIdType.MESH)
    return barrier, len(devices)


def looked_up(values, kinds):
    return jnp.take_along_axis(jnp.broadcast_to(values, kinds.shape), kinds, axis=1)


def pack_atoms(raw, atoms, labels):
    stride, ranks = atoms.shape[:2]
    for group in range(stride):
        rows = pl.ds(group * ranks, ranks)
        for axis in range(3):
            atoms[group, :, axis, :] = raw[axis, rows, :] - 0.5 * cell_edge
        atoms[group, :, 3, :] = raw[3, rows, :] * charge_scale
        labels[group, :, 0, :] = raw[4, rows, :]


def type_table(raw, types):
    types[0:1, :] = raw[5, 0:1, :] * sigma_scale
    types[1:2, :] = jnp.sqrt(raw[5, 1:2, :])


def cell_of(member, layers):
    return (
        quotient(member, GRID * layers),
        remainder(quotient(member, layers), GRID),
        remainder(member, layers),
    )


def thirds(value, size):
    return sum((value >= k * size).astype(jnp.int32) for k in (1, 2))


def tile_table(tiles, table, blocks, layers):
    home, other = tiles[0:1, :], tiles[1:2, :]
    width = tiles.shape[1]
    dead = home < 0
    slot = quotient(jnp.where(dead, 13 * blocks, other), blocks)
    member = remainder(jnp.where(dead, 0, other), blocks)
    far = thirds(slot, 9)
    slot = slot - 9 * far
    middle = thirds(slot, 3)
    steps = (far - 1, middle - 1, slot - 3 * middle - 1)
    sizes = (GRID, GRID, layers)
    own = cell_of(jnp.where(dead, 0, home), layers)
    there = [c + s * n for c, s, n in zip(cell_of(member, layers), steps, sizes)]
    line = ((there[0] + 1) * (GRID + 2) + there[1] + 1) * (layers + 2) + there[2] + 1
    delta = [t - o + 1 for t, o in zip(there, own)]
    step = (delta[0] * 3 + delta[1]) * 3 + delta[2]
    table[...] = jnp.full(table.shape, blocks * STEPS, jnp.int32)
    table[:, EDGE : EDGE + width] = (line * SHARE + jnp.where(dead, blocks, home)) * STEPS + step


def exchange_kernel(*refs):
    given, outs, scratch = refs[0], refs[1:13], refs[13:]
    region, marks, types, sources, weights, edge_terms, moments, *homes, offsets, shifts = outs
    raw, (atoms, labels, send_own, recv_own, send_rim, recv_rim, own_sem, load_sem) = scratch[0], scratch[1:]
    stride, ranks = atoms.shape[:2]
    layers = region.shape[2] - 2
    spans, here = spans_of()
    me = here[1] * spans[2] + here[2]
    load = pltpu.make_async_copy(given, raw, load_sem.at[0])
    load.start()
    peers = list(plane_peers(spans, here))
    neighbours = list(brick_neighbours(spans, here))
    barrier, greeted = greet([p[2] for p in peers] + [n[1] for n in neighbours])
    load.wait()
    pack_atoms(raw, atoms, labels)
    type_table(raw, types)
    pl.semaphore_wait(barrier, greeted)
    chunk = math.gcd(stride, layers)
    pieces = stride // chunk
    pairs = ((atoms, region), (labels, marks))

    def place(ref, piece):
        x, y, z = cell_of(me * stride + piece * chunk, layers)
        return ref.at[x + 1, y + 1, pl.ds(z + 1, chunk)]

    copies = []
    for hop, to, device in peers:
        for piece in range(pieces):
            for k, (source, target) in enumerate(pairs):
                sem = ((hop - 1) * pieces + piece) * 2 + k
                copies.append(
                    pltpu.make_async_remote_copy(
                        src_ref=source.at[pl.ds(piece * chunk, chunk), to],
                        dst_ref=place(target, piece),
                        send_sem=send_own.at[sem],
                        recv_sem=recv_own.at[sem],
                        device_id=device,
                        device_id_type=pl.DeviceIdType.MESH,
                    )
                )
                copies[-1].start()
    for piece in range(pieces):
        for k, (source, target) in enumerate(pairs):
            kept = pltpu.make_async_copy(
                source.at[pl.ds(piece * chunk, chunk), me], place(target, piece), own_sem.at[piece * 2 + k]
            )
            kept.start()
            copies.append(kept)
    for copy in copies:
        copy.wait()

    lengths = (GRID, GRID, layers)
    rims = []
    for index, (offset, device) in enumerate(neighbours):
        source = tuple(
            pl.ds(1, n) if o == 0 else pl.ds(n if o > 0 else 1, 1)
            for o, n in zip(offset, lengths)
        )
        target = tuple(
            pl.ds(1, n) if o == 0 else pl.ds(0 if o > 0 else n + 1, 1)
            for o, n in zip(offset, lengths)
        )
        for k, ref in enumerate((region, marks)):
            rims.append(
                pltpu.make_async_remote_copy(
                    src_ref=ref.at[source],
                    dst_ref=ref.at[target],
                    send_sem=send_rim.at[index * 2 + k],
                    recv_sem=recv_rim.at[index * 2 + k],
                    device_id=device,
                    device_id_type=pl.DeviceIdType.MESH,
                )
            )
            rims[-1].start()
    prepare_steps(offsets, shifts)
    prepare_own(region, marks, types, sources, weights, edge_terms, moments, *homes)
    for copy in rims:
        copy.wait()


def exchanged(raw, ranks):
    blocks, width = raw.shape[1:]
    layers = blocks // (GRID * GRID)
    stride = blocks // ranks
    pieces = stride // math.gcd(stride, layers)
    own = pltpu.SemaphoreType.DMA(((ranks - 1) * pieces * 2,))
    rim = pltpu.SemaphoreType.DMA((52,))
    vmem = pl.BlockSpec(memory_space=pltpu.VMEM)
    cells = (GRID + 2, GRID + 2, layers + 2)
    lines = math.prod(cells)
    entries = blocks + 4
    single = jax.ShapeDtypeStruct((entries, ROWS, width), jnp.float32)
    steps = jax.ShapeDtypeStruct((28, ROWS, width), jnp.float32)
    return pl.pallas_call(
        exchange_kernel,
        out_shape=(
            jax.ShapeDtypeStruct((*cells, 4, width), raw.dtype),
            jax.ShapeDtypeStruct((*cells, 1, width), raw.dtype),
            jax.ShapeDtypeStruct((ROWS, width), raw.dtype),
            jax.ShapeDtypeStruct((lines, 10 * ROWS, width), jnp.bfloat16),
            jax.ShapeDtypeStruct((lines, 2 * ROWS, width), jnp.bfloat16),
            jax.ShapeDtypeStruct((lines, 4 * ROWS, width), jnp.bfloat16),
            jax.ShapeDtypeStruct((lines, ROWS, 4 * ROWS), jnp.float32),
            single,
            jax.ShapeDtypeStruct((entries, 4 * ROWS, width), jnp.bfloat16),
            single,
            steps,
            steps,
        ),
        in_specs=[pl.BlockSpec(memory_space=pltpu.HBM)],
        out_specs=(vmem,) * 12,
        scratch_shapes=[
            pltpu.VMEM(raw.shape, raw.dtype),
            pltpu.VMEM((stride, ranks, 4, width), raw.dtype),
            pltpu.VMEM((stride, ranks, 1, width), raw.dtype),
            own,
            own,
            rim,
            rim,
            pltpu.SemaphoreType.DMA((pieces * 2,)),
            pltpu.SemaphoreType.DMA((1,)),
        ],
        compiler_params=pltpu.CompilerParams(
            has_side_effects=True, collective_id=0, vmem_limit_bytes=8 << 20
        ),
    )(raw)


def return_kernel(forces, out, send, recv, own_sem):
    spans, here = spans_of()
    me = here[1] * spans[2] + here[2]
    peers = list(plane_peers(spans, here))
    barrier, greeted = greet([p[2] for p in peers])
    kept = pltpu.make_async_copy(forces.at[:, me], out.at[:, :, me], own_sem.at[0])
    kept.start()
    pl.semaphore_wait(barrier, greeted)
    copies = [kept]
    for hop, to, device in peers:
        copies.append(
            pltpu.make_async_remote_copy(
                src_ref=forces.at[:, to],
                dst_ref=out.at[:, :, me],
                send_sem=send.at[hop - 1],
                recv_sem=recv.at[hop - 1],
                device_id=device,
                device_id_type=pl.DeviceIdType.MESH,
            )
        )
        copies[-1].start()
    for copy in copies:
        copy.wait()


def returned(forces, ranks):
    axes, blocks, width = forces.shape
    stride = blocks // ranks
    sems = pltpu.SemaphoreType.DMA((ranks - 1,))
    vmem = pl.BlockSpec(memory_space=pltpu.VMEM)
    out = pl.pallas_call(
        return_kernel,
        out_shape=jax.ShapeDtypeStruct((axes, stride, ranks, 1, width), forces.dtype),
        in_specs=[vmem],
        out_specs=vmem,
        scratch_shapes=[sems, sems, pltpu.SemaphoreType.DMA((1,))],
        compiler_params=pltpu.CompilerParams(
            has_side_effects=True, collective_id=1, vmem_limit_bytes=4 << 20
        ),
    )(forces.reshape(axes, ranks, stride, 1, width))
    return out.reshape(axes, 1, blocks, width)


def split(value):
    high = value.astype(jnp.bfloat16).astype(jnp.float32)
    rest = value - high
    middle = rest.astype(jnp.bfloat16).astype(jnp.float32)
    return high, middle, rest - middle


def stacked(parts):
    return jnp.concatenate(parts, axis=0).astype(jnp.bfloat16)


def quotient(value, size):
    if size & (size - 1):
        return lax.div(value, size)
    return lax.shift_right_logical(value, size.bit_length() - 1)


def remainder(value, size):
    if size & (size - 1):
        return lax.rem(value, size)
    return value & (size - 1)


def rows_of(shape):
    return lax.broadcasted_iota(jnp.int32, shape, 0)


def row_table(values, shape):
    rows = rows_of(shape)
    out = jnp.zeros(shape, jnp.float32)
    for k, value in enumerate(values):
        if value:
            out = jnp.where(rows == k, jnp.float32(value), out)
    return out


def rising_powers(base, rows):
    two = base * base
    four = two * two
    out = jnp.where(rows % 2 == 1, base, 1.0)
    out = out * jnp.where(rows // 2 % 2 == 1, two, 1.0)
    return out * jnp.where(rows // 4 % 2 == 1, four, 1.0)


def places(region, at):
    block = region[at]
    block = jnp.concatenate([block, block], axis=0)
    return jnp.where(rows_of(block.shape) % 4 == 3, 1.0, block)


def type_rows(marks, types, at, shape):
    kind = jnp.broadcast_to(marks[(*at, slice(0, 1))], shape).astype(jnp.int32)
    return looked_up(types[0:1, :], kind), looked_up(types[1:2, :], kind)


class Preparation:
    def __init__(self, region, marks, types, sources, weights, edge_terms, moments):
        self.refs = region, marks, types, sources, weights, edge_terms, moments
        self.shape = shape = (ROWS, region.shape[-1])
        self.rows = rows = rows_of(shape)
        edge = 1.0 / limit
        self.ways = row_table([math.comb(6, k) for k in range(7)], shape)
        self.high_at = row_table([edge**7 * math.comb(12, k) for k in range(7)], shape)
        self.low_at = row_table([-(edge**4) * math.comb(6, k) for k in range(7)], shape)
        self.wide_at = row_table([0.0] + [edge**7 * math.comb(12, k + 6) for k in range(1, 7)], shape)
        self.near_at = jnp.where(rows == 7, inverse_powers(jnp.full(shape, limit, jnp.float32))[1], 0.0)
        count = moments.shape[2]
        lanes = lax.broadcasted_iota(jnp.int32, (ROWS, count), 1)
        self.kept = (rows_of((ROWS, count)) >= 4) == (lanes % (2 * ROWS) == 7)

    def source(self, at, line):
        region, marks, types, sources, weights, edge_terms, _ = self.refs
        rows = self.rows
        place = places(region, at)
        sigma, root = type_rows(marks, types, at, self.shape)
        charge = jnp.broadcast_to(region[(*at, slice(3, 4))], self.shape)
        scale = jnp.where(rows < 4, root, charge)
        high, middle, low = split(place * jnp.where(rows < 4, 1.0, place))
        falling = rising_powers(sigma, 6 - jnp.minimum(rows, 6))
        square = sigma * sigma
        top, rest, _ = split(self.ways * falling)
        sources[line] = stacked([high, middle, high, middle, high, low, top, rest, top, rest])
        top, rest, _ = split(place * scale)
        weights[line] = stacked([top, rest])
        first = split(falling * (self.high_at * (square * square * square) + self.low_at) + self.near_at)
        second = split(falling * self.wide_at)
        edge_terms[line] = stacked([first[0], second[0], first[1], second[1]])
        return place, sigma, scale

    def moment(self, line):
        _, _, _, _, weights, edge_terms, moments = self.refs
        both = lax.dot_general(
            weights[line],
            edge_terms[line],
            (((1,), (1,)), ((), ())),
            preferred_element_type=jnp.float32,
        )
        moments[line] = jnp.where(self.kept, both[:ROWS] + both[ROWS:], 0.0)


def prepare_own(region, marks, types, sources, weights, edge_terms, moments, distances, powers, scales):
    prepared = Preparation(region, marks, types, sources, weights, edge_terms, moments)
    rows = prepared.rows
    layers = region.shape[2] - 2
    column = [(y, z) for y in range(GRID) for z in range(layers)]

    def line_of(x, y, z):
        return ((x + 1) * (GRID + 2) + y + 1) * (layers + 2) + z + 1

    def fill(x):
        for k, (y, z) in enumerate(column):
            home, sigma, scale = prepared.source((x + 1, y + 1, z + 1), line_of(x, y, z))
            block = x * len(column) + k
            distances[block] = jnp.where(rows < 3, -2.0 * home, jnp.where(rows % 4 < 3, 1.0, 0.0))
            top, rest, _ = split(rising_powers(sigma, rows))
            powers[block] = stacked([top, top, rest, rest])
            scales[block] = 12.0 * scale

    def add(x):
        for y, z in column:
            prepared.moment(line_of(x, y, z))

    def one(x, carry):
        add(x - 1)
        fill(x)
        return carry

    fill(0)
    lax.fori_loop(1, GRID, one, 0)
    add(GRID - 1)
    blocks = GRID * len(column)
    distances[blocks] = jnp.zeros(distances.shape[1:], jnp.float32)
    powers[blocks] = jnp.zeros(powers.shape[1:], powers.dtype)


def prepare_rim(region, marks, types, sources, weights, edge_terms, moments, layers):
    prepared = Preparation(region, marks, types, sources, weights, edge_terms, moments)
    depth = layers + 2
    side = (GRID + 2) * depth
    part = -(-side // GRID)
    inner = [y * depth + z for y in range(GRID + 2) for z in range(depth)]
    inner = [k for k in inner if k // depth in (0, GRID + 1) or k % depth in (0, depth - 1)]

    def lines(index):
        ends = [jnp.minimum(index * part + k, side - 1) for k in range(part)]
        far = [k + (GRID + 1) * side for k in ends]
        return ends + far + [(index + 1) * side + k for k in inner]

    def one(index, carry):
        for line in lines(index - 1):
            prepared.moment(line)
        for line in lines(index):
            prepared.source((line,), line)
        return carry

    for line in lines(0):
        prepared.source((line,), line)
    lax.fori_loop(1, GRID, one, 0)
    for line in lines(GRID - 1):
        prepared.moment(line)


def own_line(block, layers):
    x = quotient(block, GRID * layers)
    y = remainder(quotient(block, layers), GRID)
    return ((x + 1) * (GRID + 2) + y + 1) * (layers + 2) + remainder(block, layers) + 1


def prepare_steps(offsets, shifts):
    shape = offsets.shape[1:]
    for step, cells in enumerate(itertools.product((-1, 0, 1), repeat=3)):
        moves = [cell_edge * c for c in cells]
        offsets[step] = row_table([2.0 * m for m in moves], shape)
        shifts[step] = row_table(moves + [0.0] + moves, shape)


def unpacked(pairs, index):
    entry = pairs[0, index]
    return remainder(quotient(entry, STEPS), SHARE), quotient(entry, STEPS * SHARE), remainder(entry, STEPS)


def pair_terms(pairs, index, sources, distances, powers, offsets, terms):
    home, line, step = unpacked(pairs, index)
    distance = distances[home] + offsets[step]
    rows = rows_of(distance.shape)
    share = jnp.where(rows < 3, 0.25, jnp.where(rows == 4, soft_core, 0.0))
    square = jnp.sum(distance * distance * share, axis=0, keepdims=True)
    distance = jnp.where(rows == 3, square, distance)
    high, middle, low = split(distance)
    near = stacked([high, high, middle, middle, low, high])
    strong = powers[home]
    width = near.shape[1]
    right = jnp.concatenate(
        [
            jnp.concatenate([near, jnp.zeros((strong.shape[0], width), near.dtype)], axis=0),
            jnp.concatenate([jnp.zeros(near.shape, near.dtype), strong], axis=0),
        ],
        axis=1,
    )
    terms[...] = lax.dot_general(
        sources[line],
        right,
        (((0,), (0,)), ((), ())),
        preferred_element_type=jnp.float32,
    )


def inverse_powers(softened):
    root = lax.rsqrt(softened)
    one = root * root
    return one, one * root


def strengths(terms, nears, strongs):
    width = terms.shape[0]
    for start in range(0, width, 16):
        rows = pl.ds(start, 16)
        one, near = inverse_powers(jnp.minimum(terms[rows, :width], limit))
        sixth = terms[rows, width:] * (near * near)
        for halves, value in ((nears, near), (strongs, one * (sixth * (sixth - 1.0)))):
            top = value.astype(jnp.bfloat16)
            halves[rows, :] = top
            halves[pl.ds(width + start, 16), :] = (value - top.astype(jnp.float32)).astype(jnp.bfloat16)


def add_forces(pairs, index, weights, moments, shifts, nears, strongs, totals, edges):
    home, line, step = unpacked(pairs, index)
    left = weights[line]
    both = jnp.dot(
        jnp.concatenate([left, left], axis=1),
        jnp.concatenate([nears[...], strongs[...]], axis=1),
        preferred_element_type=jnp.float32,
    )
    both = both[:ROWS] + both[ROWS:]
    width = left.shape[1]
    rows = rows_of((ROWS, width))
    summed = jnp.where(rows < 4, both[:, width:], both[:, :width])
    plain = jnp.where(rows < 4, summed[3:4], summed[7:8])
    shift = shifts[step]
    totals[home] += summed + shift * plain
    shape = moments.shape[1:]
    count = shape[1]
    plain = jnp.where(
        rows[:, :count] < 4,
        jnp.broadcast_to(moments[line, 3:4, :], shape),
        jnp.broadcast_to(moments[line, 7:8, :], shape),
    )
    edges[home] += moments[line] + shift[:, :count] * plain


def force_kernel(
    tiles, region, marks, types, _, _w, _t, _m, distances, powers, scales, offsets, shifts,
    out, sources, weights, edge_terms, moments, totals, edges, table, pairs, table_sem, *slots
):
    blocks = out.shape[1]
    layers = blocks // (GRID * GRID)
    tile_table(tiles, table, blocks, layers)
    totals[...] = jnp.zeros_like(totals)
    edges[...] = jnp.zeros_like(edges)
    load = pltpu.make_async_copy(table, pairs, table_sem.at[0])
    load.start()
    prepare_rim(region, marks, types, sources, weights, edge_terms, moments, layers)
    load.wait()
    terms, nears, strongs = [slots[k : k + BATCH] for k in range(0, 3 * BATCH, BATCH)]

    def step(index, carry):
        first = (index - 1) * BATCH + EDGE

        def push(t, lag):
            add_forces(
                pairs, first - lag + t, weights, moments, shifts, nears[t], strongs[t], totals, edges
            )

        def pull(t):
            strengths(terms[t], nears[t], strongs[t])

        def pair(t):
            pair_terms(pairs, first + BATCH + t, sources, distances, powers, offsets, terms[t])

        for t in range(BATCH):
            pull(t)
            push((t - LAG) % BATCH, BATCH if t < LAG else 0)
            pair(t)
        return carry

    groups = -(-(pairs.shape[1] - 2 * EDGE) // BATCH)
    lax.fori_loop(0, groups + 2, step, 0)

    def finish(block, carry):
        line = own_line(block, layers)
        place = places(region, (line,))
        rows = rows_of(place.shape)
        sigma, _ = type_rows(marks, types, (line,), place.shape)
        rising = rising_powers(sigma, rows)
        square = sigma * sigma
        first = split(jnp.where(rows == 7, 1.0, rising))
        second = split(rising * (square * square * square))
        right = stacked([first[0], second[0], first[0], second[0], first[1], second[1], first[1], second[1]])
        edge = edges[block]
        left = stacked([*split(edge), jnp.zeros_like(edge)])
        both = jnp.dot(jnp.concatenate([left, left], axis=1), right, preferred_element_type=jnp.float32)
        summed = totals[block] - (both[:ROWS] + both[ROWS : 2 * ROWS] + both[2 * ROWS : 3 * ROWS])
        plain = jnp.where(rows < 4, summed[3:4], summed[7:8])
        force = (place * plain - summed) * scales[block]
        totals[block] = force + pltpu.roll(force, 4, 0)
        return carry

    lax.fori_loop(0, blocks, finish, 0, unroll=64)
    for axis in range(3):
        out[axis] = totals[:blocks, axis, :]


def brick_forces(tiles, region, marks, types, prepared, homes, blocks):
    width = region.shape[2]
    entries = homes[0].shape[0]
    vmem = pl.BlockSpec(memory_space=pltpu.VMEM)
    return pl.pallas_call(
        force_kernel,
        out_shape=(jax.ShapeDtypeStruct((3, blocks, width), jnp.float32),)
        + tuple(jax.ShapeDtypeStruct(x.shape, x.dtype) for x in prepared),
        in_specs=[vmem] * (4 + len(prepared) + len(homes)),
        out_specs=(vmem,) * (1 + len(prepared)),
        input_output_aliases={4 + k: 1 + k for k in range(len(prepared))},
        scratch_shapes=[
            pltpu.VMEM((entries, ROWS, width), jnp.float32),
            pltpu.VMEM((entries, ROWS, 4 * ROWS), jnp.float32),
            pltpu.VMEM((1, tiles.shape[1] + 2 * EDGE), jnp.int32),
            pltpu.SMEM((1, tiles.shape[1] + 2 * EDGE), jnp.int32),
            pltpu.SemaphoreType.DMA((1,)),
        ]
        + [pltpu.VMEM((width, 2 * width), jnp.float32)] * BATCH
        + [pltpu.VMEM((2 * width, width), jnp.bfloat16)] * (2 * BATCH),
        compiler_params=pltpu.CompilerParams(vmem_limit_bytes=16 << 20),
    )(tiles, region, marks, types, *prepared, *homes)[0]


def joined(coords, charges, kinds, sigma, epsilon):
    _, blocks, width = coords.shape

    def put(part, slab, row=0):
        sizes = zip((slab, row, 0), part.shape, (6, blocks, width))
        return lax.pad(part, jnp.zeros((), part.dtype), [(low, n - low - size, 0) for low, size, n in sizes])

    types = put(sigma[None, None], 5) + put(epsilon[None, None], 5, 1)
    return put(coords, 0) + put(charges, 3) + put(kinds, 4).astype(coords.dtype) + types


def per_device(coords, charges, atom_types, lj_sigma, lj_epsilon, tile_list):
    span_y = lax.axis_size("gy")
    span_z = lax.axis_size("gz")
    blocks = coords.shape[2]
    width = coords.shape[3]
    ranks = span_y * span_z
    raw = joined(coords[:, 0], charges, atom_types, lj_sigma, lj_epsilon)
    region, marks, types, *rest = exchanged(raw, ranks)
    forces = brick_forces(
        tile_list[0, 0, 0],
        region.reshape(-1, 4, width),
        marks.reshape(-1, 1, width),
        types,
        rest[:4],
        rest[4:],
        blocks,
    )
    return returned(forces, ranks)


def solution(mesh):
    return jax.shard_map(
        per_device,
        mesh=mesh,
        in_specs=(
            P(None, "gx", ("gy", "gz"), None),
            P("gx", ("gy", "gz"), None),
            P("gx", ("gy", "gz"), None),
            P(),
            P(),
            P("gx", "gy", "gz", None, None),
        ),
        out_specs=P(None, "gx", ("gy", "gz"), None),
        check_vma=False,
    )
```

```python
import itertools
import math

import jax
import jax.numpy as jnp
from jax import lax
from jax.experimental import pallas as pl
from jax.experimental.pallas import tpu as pltpu
from jax.sharding import PartitionSpec as P

GRID = 4
ROWS = 8
BATCH = 8
LAG = 4
EDGE = 128
STEPS = 32
SHARE = 1024
LINES = 16384
EARLY = 64

cell_edge = 11.0
cutoff = 9.0
soft_core = 16.0
coulomb = 332.0636
limit = cutoff * cutoff + soft_core
sigma_scale = 0.5 * 2.0 ** (1.0 / 6.0)
charge_scale = (coulomb / 12.0) ** 0.5


def spans_of():
    names = ("gx", "gy", "gz")
    return [lax.axis_size(n) for n in names], [lax.axis_index(n) for n in names]


def plane_peers(spans, here):
    ranks = spans[1] * spans[2]
    me = here[1] * spans[2] + here[2]
    for hop in range(1, ranks):
        to = lax.rem(me + hop, ranks)
        yield hop, to, (here[0], quotient(to, spans[2]), remainder(to, spans[2]))


def brick_neighbours(spans, here):
    for offset in itertools.product((-1, 0, 1), repeat=3):
        if any(offset):
            yield offset, tuple(lax.rem(at + o + n, n) for at, o, n in zip(here, offset, spans))


def greet(devices):
    barrier = pltpu.get_barrier_semaphore()
    for device in devices:
        pl.semaphore_signal(barrier, inc=1, device_id=device, device_id_type=pl.DeviceIdType.MESH)
    return barrier, len(devices)


def looked_up(values, kinds):
    return jnp.take_along_axis(jnp.broadcast_to(values, kinds.shape), kinds, axis=1)


def pack_atoms(raw, atoms, labels):
    stride, ranks = atoms.shape[:2]
    for group in range(stride):
        rows = pl.ds(group * ranks, ranks)
        for axis in range(3):
            atoms[group, :, axis, :] = raw[axis, rows, :] - 0.5 * cell_edge
        atoms[group, :, 3, :] = raw[3, rows, :] * charge_scale
        labels[group, :, 0, :] = raw[4, rows, :]


def type_table(raw, types):
    types[0:1, :] = raw[5, 0:1, :] * sigma_scale
    types[1:2, :] = jnp.sqrt(raw[5, 1:2, :])


def cell_of(member, layers):
    return (
        quotient(member, GRID * layers),
        remainder(quotient(member, layers), GRID),
        remainder(member, layers),
    )


def thirds(value, size):
    return sum((value >= k * size).astype(jnp.int32) for k in (1, 2))


def tile_table(tiles, table, blocks, layers):
    home, other = tiles[0:1, :], tiles[1:2, :]
    width = tiles.shape[1]
    dead = home < 0
    slot = quotient(jnp.where(dead, 13 * blocks, other), blocks)
    member = remainder(jnp.where(dead, 0, other), blocks)
    far = thirds(slot, 9)
    slot = slot - 9 * far
    middle = thirds(slot, 3)
    steps = (far - 1, middle - 1, slot - 3 * middle - 1)
    sizes = (GRID, GRID, layers)
    own = cell_of(jnp.where(dead, 0, home), layers)
    there = [c + s * n for c, s, n in zip(cell_of(member, layers), steps, sizes)]
    line = ((there[0] + 1) * (GRID + 2) + there[1] + 1) * (layers + 2) + there[2] + 1
    delta = [t - o + 1 for t, o in zip(there, own)]
    step = jnp.clip((delta[0] * 3 + delta[1]) * 3 + delta[2], 0, 26)
    line = jnp.clip(line, 0, (GRID + 2) ** 2 * (layers + 2) - 1)
    inside = [(t >= 0) & (t < n) for t, n in zip(there, sizes)]
    near = jnp.where(inside[0] & inside[1] & inside[2] & ~dead, LINES, 0)
    table[...] = jnp.full(table.shape, blocks * STEPS, jnp.int32)
    table[:, EDGE : EDGE + width] = ((near + line) * SHARE + jnp.where(dead, blocks, home)) * STEPS + step


def exchange_kernel(*refs):
    (given, tiles), outs, scratch = refs[:2], refs[2:16], refs[16:]
    region, marks, types, table, partial, sources, weights, edge_terms, moments, *homes, offsets, shifts = outs
    (raw, pairs), (atoms, labels, send_own, recv_own, send_rim, recv_rim, own_sem, load_sem, *slots) = scratch[:2], scratch[2:]
    stride, ranks = atoms.shape[:2]
    layers = region.shape[2] - 2
    spans, here = spans_of()
    me = here[1] * spans[2] + here[2]
    load = pltpu.make_async_copy(given, raw, load_sem.at[0])
    load.start()
    peers = list(plane_peers(spans, here))
    neighbours = list(brick_neighbours(spans, here))
    barrier, greeted = greet([p[2] for p in peers] + [n[1] for n in neighbours])
    load.wait()
    pack_atoms(raw, atoms, labels)
    tile_table(tiles, table, stride * ranks, layers)
    type_table(raw, types)
    pl.semaphore_wait(barrier, greeted)
    chunk = math.gcd(stride, layers)
    pieces = stride // chunk
    flows = ((atoms, region), (labels, marks))

    def place(ref, piece):
        x, y, z = cell_of(me * stride + piece * chunk, layers)
        return ref.at[x + 1, y + 1, pl.ds(z + 1, chunk)]

    load = pltpu.make_async_copy(table, pairs, load_sem.at[0])
    load.start()
    copies = []
    for hop, to, device in peers:
        for piece in range(pieces):
            for k, (source, target) in enumerate(flows):
                sem = ((hop - 1) * pieces + piece) * 2 + k
                copies.append(
                    pltpu.make_async_remote_copy(
                        src_ref=source.at[pl.ds(piece * chunk, chunk), to],
                        dst_ref=place(target, piece),
                        send_sem=send_own.at[sem],
                        recv_sem=recv_own.at[sem],
                        device_id=device,
                        device_id_type=pl.DeviceIdType.MESH,
                    )
                )
                copies[-1].start()
    for piece in range(pieces):
        for k, (source, target) in enumerate(flows):
            kept = pltpu.make_async_copy(
                source.at[pl.ds(piece * chunk, chunk), me], place(target, piece), own_sem.at[piece * 2 + k]
            )
            kept.start()
            copies.append(kept)
    for copy in copies:
        copy.wait()

    lengths = (GRID, GRID, layers)
    rims = []
    for index, (offset, device) in enumerate(neighbours):
        source = tuple(
            pl.ds(1, n) if o == 0 else pl.ds(n if o > 0 else 1, 1)
            for o, n in zip(offset, lengths)
        )
        target = tuple(
            pl.ds(1, n) if o == 0 else pl.ds(0 if o > 0 else n + 1, 1)
            for o, n in zip(offset, lengths)
        )
        for k, ref in enumerate((region, marks)):
            rims.append(
                pltpu.make_async_remote_copy(
                    src_ref=ref.at[source],
                    dst_ref=ref.at[target],
                    send_sem=send_rim.at[index * 2 + k],
                    recv_sem=recv_rim.at[index * 2 + k],
                    device_id=device,
                    device_id_type=pl.DeviceIdType.MESH,
                )
            )
            rims[-1].start()
    prepare_steps(offsets, shifts)
    prepare_own(region, marks, types, sources, weights, edge_terms, moments, *homes)
    load.wait()

    def take(at, summed):
        partial[at + 2 * BATCH] = summed

    tile_loop(
        0,
        early_tiles(tiles.shape[1]) // BATCH,
        pairs,
        sources,
        weights,
        homes[0],
        homes[1],
        offsets,
        slots,
        take,
    )
    for copy in rims:
        copy.wait()


def early_tiles(count):
    return min(EARLY, count) // BATCH * BATCH


def exchanged(raw, tiles, ranks):
    blocks, width = raw.shape[1:]
    layers = blocks // (GRID * GRID)
    stride = blocks // ranks
    pieces = stride // math.gcd(stride, layers)
    own = pltpu.SemaphoreType.DMA(((ranks - 1) * pieces * 2,))
    rim = pltpu.SemaphoreType.DMA((52,))
    vmem = pl.BlockSpec(memory_space=pltpu.VMEM)
    cells = (GRID + 2, GRID + 2, layers + 2)
    lines = math.prod(cells)
    entries = blocks + 4
    single = jax.ShapeDtypeStruct((entries, ROWS, width), jnp.float32)
    steps = jax.ShapeDtypeStruct((28, ROWS, width), jnp.float32)
    return pl.pallas_call(
        exchange_kernel,
        out_shape=(
            jax.ShapeDtypeStruct((*cells, 4, width), raw.dtype),
            jax.ShapeDtypeStruct((*cells, 1, width), raw.dtype),
            jax.ShapeDtypeStruct((ROWS, width), raw.dtype),
            jax.ShapeDtypeStruct((1, tiles.shape[1] + 2 * EDGE), jnp.int32),
            jax.ShapeDtypeStruct((early_tiles(tiles.shape[1]) + 3 * BATCH, ROWS, width), jnp.float32),
            jax.ShapeDtypeStruct((lines, 10 * ROWS, width), jnp.bfloat16),
            jax.ShapeDtypeStruct((lines, 2 * ROWS, width), jnp.bfloat16),
            jax.ShapeDtypeStruct((lines, 4 * ROWS, width), jnp.bfloat16),
            jax.ShapeDtypeStruct((lines, ROWS, 4 * ROWS), jnp.float32),
            single,
            jax.ShapeDtypeStruct((entries, 4 * ROWS, width), jnp.bfloat16),
            single,
            steps,
            steps,
        ),
        in_specs=[pl.BlockSpec(memory_space=pltpu.HBM), vmem],
        out_specs=(vmem,) * 14,
        scratch_shapes=[
            pltpu.VMEM(raw.shape, raw.dtype),
            pltpu.SMEM((1, tiles.shape[1] + 2 * EDGE), jnp.int32),
            pltpu.VMEM((stride, ranks, 4, width), raw.dtype),
            pltpu.VMEM((stride, ranks, 1, width), raw.dtype),
            own,
            own,
            rim,
            rim,
            pltpu.SemaphoreType.DMA((pieces * 2,)),
            pltpu.SemaphoreType.DMA((1,)),
        ]
        + tile_slots(width),
        compiler_params=pltpu.CompilerParams(
            has_side_effects=True, collective_id=0, vmem_limit_bytes=12 << 20
        ),
    )(raw, tiles)


def return_kernel(forces, out, send, recv, own_sem):
    spans, here = spans_of()
    me = here[1] * spans[2] + here[2]
    peers = list(plane_peers(spans, here))
    barrier, greeted = greet([p[2] for p in peers])
    kept = pltpu.make_async_copy(forces.at[:, me], out.at[:, :, me], own_sem.at[0])
    kept.start()
    pl.semaphore_wait(barrier, greeted)
    copies = [kept]
    for hop, to, device in peers:
        copies.append(
            pltpu.make_async_remote_copy(
                src_ref=forces.at[:, to],
                dst_ref=out.at[:, :, me],
                send_sem=send.at[hop - 1],
                recv_sem=recv.at[hop - 1],
                device_id=device,
                device_id_type=pl.DeviceIdType.MESH,
            )
        )
        copies[-1].start()
    for copy in copies:
        copy.wait()


def returned(forces, ranks):
    axes, blocks, width = forces.shape
    stride = blocks // ranks
    sems = pltpu.SemaphoreType.DMA((ranks - 1,))
    vmem = pl.BlockSpec(memory_space=pltpu.VMEM)
    out = pl.pallas_call(
        return_kernel,
        out_shape=jax.ShapeDtypeStruct((axes, stride, ranks, 1, width), forces.dtype),
        in_specs=[vmem],
        out_specs=vmem,
        scratch_shapes=[sems, sems, pltpu.SemaphoreType.DMA((1,))],
        compiler_params=pltpu.CompilerParams(
            has_side_effects=True, collective_id=1, vmem_limit_bytes=4 << 20
        ),
    )(forces.reshape(axes, ranks, stride, 1, width))
    return out.reshape(axes, 1, blocks, width)


def split(value):
    high = value.astype(jnp.bfloat16).astype(jnp.float32)
    rest = value - high
    middle = rest.astype(jnp.bfloat16).astype(jnp.float32)
    return high, middle, rest - middle


def stacked(parts):
    return jnp.concatenate(parts, axis=0).astype(jnp.bfloat16)


def quotient(value, size):
    if size & (size - 1):
        return lax.div(value, size)
    return lax.shift_right_logical(value, size.bit_length() - 1)


def remainder(value, size):
    if size & (size - 1):
        return lax.rem(value, size)
    return value & (size - 1)


def rows_of(shape):
    return lax.broadcasted_iota(jnp.int32, shape, 0)


def row_table(values, shape):
    rows = rows_of(shape)
    out = jnp.zeros(shape, jnp.float32)
    for k, value in enumerate(values):
        if value:
            out = jnp.where(rows == k, jnp.float32(value), out)
    return out


def rising_powers(base, rows):
    two = base * base
    four = two * two
    out = jnp.where(rows % 2 == 1, base, 1.0)
    out = out * jnp.where(rows // 2 % 2 == 1, two, 1.0)
    return out * jnp.where(rows // 4 % 2 == 1, four, 1.0)


def places(region, at):
    block = region[at]
    block = jnp.concatenate([block, block], axis=0)
    return jnp.where(rows_of(block.shape) % 4 == 3, 1.0, block)


def type_rows(marks, types, at, shape):
    kind = jnp.broadcast_to(marks[(*at, slice(0, 1))], shape).astype(jnp.int32)
    return looked_up(types[0:1, :], kind), looked_up(types[1:2, :], kind)


class Preparation:
    def __init__(self, region, marks, types, sources, weights, edge_terms, moments):
        self.refs = region, marks, types, sources, weights, edge_terms, moments
        self.shape = shape = (ROWS, region.shape[-1])
        self.rows = rows = rows_of(shape)
        edge = 1.0 / limit
        self.ways = row_table([math.comb(6, k) for k in range(7)], shape)
        self.high_at = row_table([edge**7 * math.comb(12, k) for k in range(7)], shape)
        self.low_at = row_table([-(edge**4) * math.comb(6, k) for k in range(7)], shape)
        self.wide_at = row_table([0.0] + [edge**7 * math.comb(12, k + 6) for k in range(1, 7)], shape)
        self.near_at = jnp.where(rows == 7, inverse_powers(jnp.full(shape, limit, jnp.float32))[1], 0.0)
        count = moments.shape[2]
        lanes = lax.broadcasted_iota(jnp.int32, (ROWS, count), 1)
        self.kept = (rows_of((ROWS, count)) >= 4) == (lanes % (2 * ROWS) == 7)

    def source(self, at, line):
        region, marks, types, sources, weights, edge_terms, _ = self.refs
        rows = self.rows
        place = places(region, at)
        sigma, root = type_rows(marks, types, at, self.shape)
        charge = jnp.broadcast_to(region[(*at, slice(3, 4))], self.shape)
        scale = jnp.where(rows < 4, root, charge)
        high, middle, low = split(place * jnp.where(rows < 4, 1.0, place))
        falling = rising_powers(sigma, 6 - jnp.minimum(rows, 6))
        square = sigma * sigma
        top, rest, _ = split(self.ways * falling)
        sources[line] = stacked([high, middle, high, middle, high, low, top, rest, top, rest])
        top, rest, _ = split(place * scale)
        weights[line] = stacked([top, rest])
        first = split(falling * (self.high_at * (square * square * square) + self.low_at) + self.near_at)
        second = split(falling * self.wide_at)
        edge_terms[line] = stacked([first[0], second[0], first[1], second[1]])
        return place, sigma, scale

    def moment(self, line):
        _, _, _, _, weights, edge_terms, moments = self.refs
        both = lax.dot_general(
            weights[line],
            edge_terms[line],
            (((1,), (1,)), ((), ())),
            preferred_element_type=jnp.float32,
        )
        moments[line] = jnp.where(self.kept, both[:ROWS] + both[ROWS:], 0.0)


def prepare_own(region, marks, types, sources, weights, edge_terms, moments, distances, powers, scales):
    prepared = Preparation(region, marks, types, sources, weights, edge_terms, moments)
    rows = prepared.rows
    layers = region.shape[2] - 2
    column = [(y, z) for y in range(GRID) for z in range(layers)]

    def line_of(x, y, z):
        return ((x + 1) * (GRID + 2) + y + 1) * (layers + 2) + z + 1

    def fill(x):
        for k, (y, z) in enumerate(column):
            home, sigma, scale = prepared.source((x + 1, y + 1, z + 1), line_of(x, y, z))
            block = x * len(column) + k
            distances[block] = jnp.where(rows < 3, -2.0 * home, jnp.where(rows % 4 < 3, 1.0, 0.0))
            top, rest, _ = split(rising_powers(sigma, rows))
            powers[block] = stacked([top, top, rest, rest])
            scales[block] = 12.0 * scale

    def add(x):
        for y, z in column:
            prepared.moment(line_of(x, y, z))

    def one(x, carry):
        add(x - 1)
        fill(x)
        return carry

    fill(0)
    lax.fori_loop(1, GRID, one, 0)
    add(GRID - 1)
    blocks = GRID * len(column)
    distances[blocks] = jnp.zeros(distances.shape[1:], jnp.float32)
    powers[blocks] = jnp.zeros(powers.shape[1:], powers.dtype)


def prepare_rim(region, marks, types, sources, weights, edge_terms, moments, layers):
    prepared = Preparation(region, marks, types, sources, weights, edge_terms, moments)
    depth = layers + 2
    side = (GRID + 2) * depth
    part = -(-side // GRID)
    inner = [y * depth + z for y in range(GRID + 2) for z in range(depth)]
    inner = [k for k in inner if k // depth in (0, GRID + 1) or k % depth in (0, depth - 1)]

    def lines(index):
        ends = [jnp.minimum(index * part + k, side - 1) for k in range(part)]
        far = [k + (GRID + 1) * side for k in ends]
        return ends + far + [(index + 1) * side + k for k in inner]

    def one(index, carry):
        for line in lines(index - 1):
            prepared.moment(line)
        for line in lines(index):
            prepared.source((line,), line)
        return carry

    for line in lines(0):
        prepared.source((line,), line)
    lax.fori_loop(1, GRID, one, 0)
    for line in lines(GRID - 1):
        prepared.moment(line)


def own_line(block, layers):
    x = quotient(block, GRID * layers)
    y = remainder(quotient(block, layers), GRID)
    return ((x + 1) * (GRID + 2) + y + 1) * (layers + 2) + remainder(block, layers) + 1


def prepare_steps(offsets, shifts):
    shape = offsets.shape[1:]
    for step, cells in enumerate(itertools.product((-1, 0, 1), repeat=3)):
        moves = [cell_edge * c for c in cells]
        offsets[step] = row_table([2.0 * m for m in moves], shape)
        shifts[step] = row_table(moves + [0.0] + moves, shape)


def unpacked(pairs, index):
    entry = pairs[0, index]
    line = remainder(quotient(entry, STEPS * SHARE), LINES)
    return remainder(quotient(entry, STEPS), SHARE), line, remainder(entry, STEPS)


def pair_terms(pairs, index, sources, distances, powers, offsets, terms):
    home, line, step = unpacked(pairs, index)
    distance = distances[home] + offsets[step]
    rows = rows_of(distance.shape)
    share = jnp.where(rows < 3, 0.25, jnp.where(rows == 4, soft_core, 0.0))
    square = jnp.sum(distance * distance * share, axis=0, keepdims=True)
    distance = jnp.where(rows == 3, square, distance)
    high, middle, low = split(distance)
    near = stacked([high, high, middle, middle, low, high])
    strong = powers[home]
    width = near.shape[1]
    right = jnp.concatenate(
        [
            jnp.concatenate([near, jnp.zeros((strong.shape[0], width), near.dtype)], axis=0),
            jnp.concatenate([jnp.zeros(near.shape, near.dtype), strong], axis=0),
        ],
        axis=1,
    )
    terms[...] = lax.dot_general(
        sources[line],
        right,
        (((0,), (0,)), ((), ())),
        preferred_element_type=jnp.float32,
    )


def inverse_powers(softened):
    root = lax.rsqrt(softened)
    one = root * root
    return one, one * root


def strengths(terms, nears, strongs):
    width = terms.shape[0]
    for start in range(0, width, 16):
        rows = pl.ds(start, 16)
        one, near = inverse_powers(jnp.minimum(terms[rows, :width], limit))
        sixth = terms[rows, width:] * (near * near)
        for halves, value in ((nears, near), (strongs, one * (sixth * (sixth - 1.0)))):
            top = value.astype(jnp.bfloat16)
            halves[rows, :] = top
            halves[pl.ds(width + start, 16), :] = (value - top.astype(jnp.float32)).astype(jnp.bfloat16)


def tile_forces(pairs, index, weights, nears, strongs):
    _, line, _ = unpacked(pairs, index)
    left = weights[line]
    both = jnp.dot(
        jnp.concatenate([left, left], axis=1),
        jnp.concatenate([nears[...], strongs[...]], axis=1),
        preferred_element_type=jnp.float32,
    )
    both = both[:ROWS] + both[ROWS:]
    width = left.shape[1]
    return jnp.where(rows_of((ROWS, width)) < 4, both[:, width:], both[:, :width])


def add_forces(summed, home, line, step, moments, shifts, totals, edges):
    rows = rows_of(summed.shape)
    plain = jnp.where(rows < 4, summed[3:4], summed[7:8])
    shift = shifts[step]
    totals[home] += summed + shift * plain
    shape = moments.shape[1:]
    count = shape[1]
    plain = jnp.where(
        rows[:, :count] < 4,
        jnp.broadcast_to(moments[line, 3:4, :], shape),
        jnp.broadcast_to(moments[line, 7:8, :], shape),
    )
    edges[home] += moments[line] + shift[:, :count] * plain


def tile_loop(start, groups, pairs, sources, weights, distances, powers, offsets, slots, take):
    terms, nears, strongs = [slots[k : k + BATCH] for k in range(0, 3 * BATCH, BATCH)]

    def step(index, carry):
        first = (index - 1) * BATCH

        def push(t, lag):
            at = first - lag + t
            take(at, tile_forces(pairs, at + EDGE, weights, nears[t], strongs[t]))

        for t in range(BATCH):
            strengths(terms[t], nears[t], strongs[t])
            push((t - LAG) % BATCH, BATCH if t < LAG else 0)
            pair_terms(pairs, first + BATCH + t + EDGE, sources, distances, powers, offsets, terms[t])
        return carry

    lax.fori_loop(start, groups + 2, step, 0)


def tile_slots(width):
    return [pltpu.VMEM((width, 2 * width), jnp.float32)] * BATCH + [
        pltpu.VMEM((2 * width, width), jnp.bfloat16)
    ] * (2 * BATCH)


def force_kernel(
    table, partial, region, marks, types, _, _w, _t, _m, distances, powers, scales, offsets, shifts,
    out, sources, weights, edge_terms, moments, totals, edges, pairs, table_sem, *slots
):
    blocks = out.shape[1]
    layers = blocks // (GRID * GRID)
    totals[...] = jnp.zeros_like(totals)
    edges[...] = jnp.zeros_like(edges)
    load = pltpu.make_async_copy(table, pairs, table_sem.at[0])
    load.start()
    prepare_rim(region, marks, types, sources, weights, edge_terms, moments, layers)
    load.wait()
    count = table.shape[1] - 2 * EDGE
    early = early_tiles(count)

    def merge(index, at):
        place = early - 1 - index
        entry = pairs[0, place + EDGE]
        home, line, step = unpacked(pairs, place + EDGE)
        near = quotient(entry, STEPS * SHARE * LINES)
        summed = partial[place + 2 * BATCH]
        add_forces(summed, jnp.where(near == 1, home, blocks), line, step, moments, shifts, totals, edges)
        pairs[0, at + EDGE] = entry
        return at - (1 - near)

    first = lax.fori_loop(0, early, merge, jnp.int32(early - 1), unroll=4) + 1
    for k in range(3 * BATCH):
        pairs[0, first - 1 - k + EDGE] = blocks * STEPS

    def take(at, summed):
        home, line, step = unpacked(pairs, at + EDGE)
        add_forces(summed, home, line, step, moments, shifts, totals, edges)

    groups = -(-count // BATCH)
    tile_loop(
        quotient(first, BATCH), groups, pairs, sources, weights, distances, powers, offsets, slots, take
    )

    def finish(block, carry):
        line = own_line(block, layers)
        place = places(region, (line,))
        rows = rows_of(place.shape)
        sigma, _ = type_rows(marks, types, (line,), place.shape)
        rising = rising_powers(sigma, rows)
        square = sigma * sigma
        first = split(jnp.where(rows == 7, 1.0, rising))
        second = split(rising * (square * square * square))
        right = stacked([first[0], second[0], first[0], second[0], first[1], second[1], first[1], second[1]])
        edge = edges[block]
        left = stacked([*split(edge), jnp.zeros_like(edge)])
        both = jnp.dot(jnp.concatenate([left, left], axis=1), right, preferred_element_type=jnp.float32)
        summed = totals[block] - (both[:ROWS] + both[ROWS : 2 * ROWS] + both[2 * ROWS : 3 * ROWS])
        plain = jnp.where(rows < 4, summed[3:4], summed[7:8])
        force = (place * plain - summed) * scales[block]
        totals[block] = force + pltpu.roll(force, 4, 0)
        return carry

    lax.fori_loop(0, blocks, finish, 0, unroll=64)
    for axis in range(3):
        out[axis] = totals[:blocks, axis, :]


def brick_forces(table, partial, region, marks, types, prepared, homes, blocks):
    width = region.shape[2]
    entries = homes[0].shape[0]
    vmem = pl.BlockSpec(memory_space=pltpu.VMEM)
    return pl.pallas_call(
        force_kernel,
        out_shape=(jax.ShapeDtypeStruct((3, blocks, width), jnp.float32),)
        + tuple(jax.ShapeDtypeStruct(x.shape, x.dtype) for x in prepared),
        in_specs=[vmem] * (5 + len(prepared) + len(homes)),
        out_specs=(vmem,) * (1 + len(prepared)),
        input_output_aliases={5 + k: 1 + k for k in range(len(prepared))},
        scratch_shapes=[
            pltpu.VMEM((entries, ROWS, width), jnp.float32),
            pltpu.VMEM((entries, ROWS, 4 * ROWS), jnp.float32),
            pltpu.SMEM(table.shape, jnp.int32),
            pltpu.SemaphoreType.DMA((1,)),
        ]
        + tile_slots(width),
        compiler_params=pltpu.CompilerParams(vmem_limit_bytes=16 << 20),
    )(table, partial, region, marks, types, *prepared, *homes)[0]


def joined(coords, charges, kinds, sigma, epsilon):
    _, blocks, width = coords.shape

    def put(part, slab, row=0):
        sizes = zip((slab, row, 0), part.shape, (6, blocks, width))
        return lax.pad(part, jnp.zeros((), part.dtype), [(low, n - low - size, 0) for low, size, n in sizes])

    types = put(sigma[None, None], 5) + put(epsilon[None, None], 5, 1)
    return put(coords, 0) + put(charges, 3) + put(kinds, 4).astype(coords.dtype) + types


def per_device(coords, charges, atom_types, lj_sigma, lj_epsilon, tile_list):
    span_y = lax.axis_size("gy")
    span_z = lax.axis_size("gz")
    blocks = coords.shape[2]
    width = coords.shape[3]
    ranks = span_y * span_z
    raw = joined(coords[:, 0], charges, atom_types, lj_sigma, lj_epsilon)
    tiles = tile_list[0, 0, 0]
    region, marks, types, table, partial, *rest = exchanged(raw, tiles, ranks)
    forces = brick_forces(
        table,
        partial,
        region.reshape(-1, 4, width),
        marks.reshape(-1, 1, width),
        types,
        rest[:4],
        rest[4:],
        blocks,
    )
    return returned(forces, ranks)


def solution(mesh):
    return jax.shard_map(
        per_device,
        mesh=mesh,
        in_specs=(
            P(None, "gx", ("gy", "gz"), None),
            P("gx", ("gy", "gz"), None),
            P("gx", ("gy", "gz"), None),
            P(),
            P(),
            P("gx", "gy", "gz", None, None),
        ),
        out_specs=P(None, "gx", ("gy", "gz"), None),
        check_vma=False,
    )
```

```python
import itertools
import math

import jax
import jax.numpy as jnp
from jax import lax
from jax.experimental import pallas as pl
from jax.experimental.pallas import tpu as pltpu
from jax.sharding import PartitionSpec as P

GRID = 4
ROWS = 8
BATCH = 8
LAG = 4
EDGE = 128
STEPS = 32
SHARE = 1024
LINES = 16384
EARLY = 112

cell_edge = 11.0
cutoff = 9.0
soft_core = 16.0
coulomb = 332.0636
limit = cutoff * cutoff + soft_core
sigma_scale = 0.5 * 2.0 ** (1.0 / 6.0)
charge_scale = (coulomb / 12.0) ** 0.5


def spans_of():
    names = ("gx", "gy", "gz")
    return [lax.axis_size(n) for n in names], [lax.axis_index(n) for n in names]


def plane_peers(spans, here):
    ranks = spans[1] * spans[2]
    me = here[1] * spans[2] + here[2]
    for hop in range(1, ranks):
        to = lax.rem(me + hop, ranks)
        yield hop, to, (here[0], quotient(to, spans[2]), remainder(to, spans[2]))


def brick_neighbours(spans, here):
    for offset in itertools.product((-1, 0, 1), repeat=3):
        if any(offset):
            yield offset, tuple(lax.rem(at + o + n, n) for at, o, n in zip(here, offset, spans))


def greet(devices):
    barrier = pltpu.get_barrier_semaphore()
    for device in devices:
        pl.semaphore_signal(barrier, inc=1, device_id=device, device_id_type=pl.DeviceIdType.MESH)
    return barrier, len(devices)


def looked_up(values, kinds):
    return jnp.take_along_axis(jnp.broadcast_to(values, kinds.shape), kinds, axis=1)


def pack_atoms(raw, atoms, labels):
    stride, ranks = atoms.shape[:2]
    for group in range(stride):
        rows = pl.ds(group * ranks, ranks)
        for axis in range(3):
            atoms[group, :, axis, :] = raw[axis, rows, :] - 0.5 * cell_edge
        atoms[group, :, 3, :] = raw[3, rows, :] * charge_scale
        labels[group, :, 0, :] = raw[4, rows, :]


def type_table(raw, types):
    types[0:1, :] = raw[5, 0:1, :] * sigma_scale
    types[1:2, :] = jnp.sqrt(raw[5, 1:2, :])


def cell_of(member, layers):
    return (
        quotient(member, GRID * layers),
        remainder(quotient(member, layers), GRID),
        remainder(member, layers),
    )


def thirds(value, size):
    return sum((value >= k * size).astype(jnp.int32) for k in (1, 2))


def tile_table(tiles, table, blocks, layers):
    home, other = tiles[0:1, :], tiles[1:2, :]
    width = tiles.shape[1]
    dead = home < 0
    slot = quotient(jnp.where(dead, 13 * blocks, other), blocks)
    member = remainder(jnp.where(dead, 0, other), blocks)
    far = thirds(slot, 9)
    slot = slot - 9 * far
    middle = thirds(slot, 3)
    steps = (far - 1, middle - 1, slot - 3 * middle - 1)
    sizes = (GRID, GRID, layers)
    own = cell_of(jnp.where(dead, 0, home), layers)
    there = [c + s * n for c, s, n in zip(cell_of(member, layers), steps, sizes)]
    line = ((there[0] + 1) * (GRID + 2) + there[1] + 1) * (layers + 2) + there[2] + 1
    delta = [t - o + 1 for t, o in zip(there, own)]
    step = jnp.clip((delta[0] * 3 + delta[1]) * 3 + delta[2], 0, 26)
    line = jnp.clip(line, 0, (GRID + 2) ** 2 * (layers + 2) - 1)
    inside = [(t >= 0) & (t < n) for t, n in zip(there, sizes)]
    near = jnp.where(inside[0] & inside[1] & inside[2] & ~dead, LINES, 0)
    table[...] = jnp.full(table.shape, blocks * STEPS, jnp.int32)
    table[:, EDGE : EDGE + width] = ((near + line) * SHARE + jnp.where(dead, blocks, home)) * STEPS + step


def exchange_kernel(*refs):
    (given, tiles), outs, scratch = refs[:2], refs[2:16], refs[16:]
    region, marks, types, table, partial, sources, weights, edge_terms, moments, *homes, offsets, shifts = outs
    (raw, pairs), (atoms, labels, send_own, recv_own, send_rim, recv_rim, own_sem, load_sem, *slots) = scratch[:2], scratch[2:]
    stride, ranks = atoms.shape[:2]
    layers = region.shape[2] - 2
    spans, here = spans_of()
    me = here[1] * spans[2] + here[2]
    load = pltpu.make_async_copy(given, raw, load_sem.at[0])
    load.start()
    peers = list(plane_peers(spans, here))
    neighbours = list(brick_neighbours(spans, here))
    barrier, greeted = greet([p[2] for p in peers] + [n[1] for n in neighbours])
    load.wait()
    pack_atoms(raw, atoms, labels)
    tile_table(tiles, table, stride * ranks, layers)
    type_table(raw, types)
    pl.semaphore_wait(barrier, greeted)
    chunk = math.gcd(stride, layers)
    pieces = stride // chunk
    flows = ((atoms, region), (labels, marks))

    def place(ref, piece):
        x, y, z = cell_of(me * stride + piece * chunk, layers)
        return ref.at[x + 1, y + 1, pl.ds(z + 1, chunk)]

    load = pltpu.make_async_copy(table, pairs, load_sem.at[0])
    load.start()
    copies = []
    for hop, to, device in peers:
        for piece in range(pieces):
            for k, (source, target) in enumerate(flows):
                sem = ((hop - 1) * pieces + piece) * 2 + k
                copies.append(
                    pltpu.make_async_remote_copy(
                        src_ref=source.at[pl.ds(piece * chunk, chunk), to],
                        dst_ref=place(target, piece),
                        send_sem=send_own.at[sem],
                        recv_sem=recv_own.at[sem],
                        device_id=device,
                        device_id_type=pl.DeviceIdType.MESH,
                    )
                )
                copies[-1].start()
    for piece in range(pieces):
        for k, (source, target) in enumerate(flows):
            kept = pltpu.make_async_copy(
                source.at[pl.ds(piece * chunk, chunk), me], place(target, piece), own_sem.at[piece * 2 + k]
            )
            kept.start()
            copies.append(kept)
    for copy in copies:
        copy.wait()

    lengths = (GRID, GRID, layers)
    rims = []
    for index, (offset, device) in enumerate(neighbours):
        source = tuple(
            pl.ds(1, n) if o == 0 else pl.ds(n if o > 0 else 1, 1)
            for o, n in zip(offset, lengths)
        )
        target = tuple(
            pl.ds(1, n) if o == 0 else pl.ds(0 if o > 0 else n + 1, 1)
            for o, n in zip(offset, lengths)
        )
        for k, ref in enumerate((region, marks)):
            rims.append(
                pltpu.make_async_remote_copy(
                    src_ref=ref.at[source],
                    dst_ref=ref.at[target],
                    send_sem=send_rim.at[index * 2 + k],
                    recv_sem=recv_rim.at[index * 2 + k],
                    device_id=device,
                    device_id_type=pl.DeviceIdType.MESH,
                )
            )
            rims[-1].start()
    prepare_steps(offsets, shifts)
    prepare_own(region, marks, types, sources, weights, edge_terms, moments, *homes)
    load.wait()

    def take(at, summed):
        partial[at + 2 * BATCH] = summed

    tile_loop(
        0,
        early_tiles(tiles.shape[1]) // BATCH,
        pairs,
        sources,
        weights,
        homes[0],
        homes[1],
        offsets,
        slots,
        take,
    )
    for copy in rims:
        copy.wait()


def early_tiles(count):
    return min(EARLY, count) // BATCH * BATCH


def exchanged(raw, tiles, ranks):
    blocks, width = raw.shape[1:]
    layers = blocks // (GRID * GRID)
    stride = blocks // ranks
    pieces = stride // math.gcd(stride, layers)
    own = pltpu.SemaphoreType.DMA(((ranks - 1) * pieces * 2,))
    rim = pltpu.SemaphoreType.DMA((52,))
    vmem = pl.BlockSpec(memory_space=pltpu.VMEM)
    cells = (GRID + 2, GRID + 2, layers + 2)
    lines = math.prod(cells)
    entries = blocks + 4
    single = jax.ShapeDtypeStruct((entries, ROWS, width), jnp.float32)
    steps = jax.ShapeDtypeStruct((28, ROWS, width), jnp.float32)
    return pl.pallas_call(
        exchange_kernel,
        out_shape=(
            jax.ShapeDtypeStruct((*cells, 4, width), raw.dtype),
            jax.ShapeDtypeStruct((*cells, 1, width), raw.dtype),
            jax.ShapeDtypeStruct((ROWS, width), raw.dtype),
            jax.ShapeDtypeStruct((1, tiles.shape[1] + 2 * EDGE), jnp.int32),
            jax.ShapeDtypeStruct((early_tiles(tiles.shape[1]) + 3 * BATCH, ROWS, width), jnp.float32),
            jax.ShapeDtypeStruct((lines, 10 * ROWS, width), jnp.bfloat16),
            jax.ShapeDtypeStruct((lines, 2 * ROWS, width), jnp.bfloat16),
            jax.ShapeDtypeStruct((lines, 4 * ROWS, width), jnp.bfloat16),
            jax.ShapeDtypeStruct((lines, ROWS, 4 * ROWS), jnp.float32),
            single,
            jax.ShapeDtypeStruct((entries, 4 * ROWS, width), jnp.bfloat16),
            single,
            steps,
            steps,
        ),
        in_specs=[pl.BlockSpec(memory_space=pltpu.HBM), vmem],
        out_specs=(vmem,) * 14,
        scratch_shapes=[
            pltpu.VMEM(raw.shape, raw.dtype),
            pltpu.SMEM((1, tiles.shape[1] + 2 * EDGE), jnp.int32),
            pltpu.VMEM((stride, ranks, 4, width), raw.dtype),
            pltpu.VMEM((stride, ranks, 1, width), raw.dtype),
            own,
            own,
            rim,
            rim,
            pltpu.SemaphoreType.DMA((pieces * 2,)),
            pltpu.SemaphoreType.DMA((1,)),
        ]
        + tile_slots(width),
        compiler_params=pltpu.CompilerParams(
            has_side_effects=True, collective_id=0, vmem_limit_bytes=12 << 20
        ),
    )(raw, tiles)


def return_kernel(forces, out, send, recv, own_sem):
    spans, here = spans_of()
    me = here[1] * spans[2] + here[2]
    peers = list(plane_peers(spans, here))
    barrier, greeted = greet([p[2] for p in peers])
    kept = pltpu.make_async_copy(forces.at[:, me], out.at[:, :, me], own_sem.at[0])
    kept.start()
    pl.semaphore_wait(barrier, greeted)
    copies = [kept]
    for hop, to, device in peers:
        copies.append(
            pltpu.make_async_remote_copy(
                src_ref=forces.at[:, to],
                dst_ref=out.at[:, :, me],
                send_sem=send.at[hop - 1],
                recv_sem=recv.at[hop - 1],
                device_id=device,
                device_id_type=pl.DeviceIdType.MESH,
            )
        )
        copies[-1].start()
    for copy in copies:
        copy.wait()


def returned(forces, ranks):
    axes, blocks, width = forces.shape
    stride = blocks // ranks
    sems = pltpu.SemaphoreType.DMA((ranks - 1,))
    vmem = pl.BlockSpec(memory_space=pltpu.VMEM)
    out = pl.pallas_call(
        return_kernel,
        out_shape=jax.ShapeDtypeStruct((axes, stride, ranks, 1, width), forces.dtype),
        in_specs=[vmem],
        out_specs=vmem,
        scratch_shapes=[sems, sems, pltpu.SemaphoreType.DMA((1,))],
        compiler_params=pltpu.CompilerParams(
            has_side_effects=True, collective_id=1, vmem_limit_bytes=4 << 20
        ),
    )(forces.reshape(axes, ranks, stride, 1, width))
    return out.reshape(axes, 1, blocks, width)


def split(value):
    high = value.astype(jnp.bfloat16).astype(jnp.float32)
    rest = value - high
    middle = rest.astype(jnp.bfloat16).astype(jnp.float32)
    return high, middle, rest - middle


def stacked(parts):
    return jnp.concatenate(parts, axis=0).astype(jnp.bfloat16)


def quotient(value, size):
    if size & (size - 1):
        return lax.div(value, size)
    return lax.shift_right_logical(value, size.bit_length() - 1)


def remainder(value, size):
    if size & (size - 1):
        return lax.rem(value, size)
    return value & (size - 1)


def rows_of(shape):
    return lax.broadcasted_iota(jnp.int32, shape, 0)


def row_table(values, shape):
    rows = rows_of(shape)
    out = jnp.zeros(shape, jnp.float32)
    for k, value in enumerate(values):
        if value:
            out = jnp.where(rows == k, jnp.float32(value), out)
    return out


def rising_powers(base, rows):
    two = base * base
    four = two * two
    out = jnp.where(rows % 2 == 1, base, 1.0)
    out = out * jnp.where(rows // 2 % 2 == 1, two, 1.0)
    return out * jnp.where(rows // 4 % 2 == 1, four, 1.0)


def places(region, at):
    block = region[at]
    block = jnp.concatenate([block, block], axis=0)
    return jnp.where(rows_of(block.shape) % 4 == 3, 1.0, block)


def type_rows(marks, types, at, shape):
    kind = jnp.broadcast_to(marks[(*at, slice(0, 1))], shape).astype(jnp.int32)
    return looked_up(types[0:1, :], kind), looked_up(types[1:2, :], kind)


class Preparation:
    def __init__(self, region, marks, types, sources, weights, edge_terms, moments):
        self.refs = region, marks, types, sources, weights, edge_terms, moments
        self.shape = shape = (ROWS, region.shape[-1])
        self.rows = rows = rows_of(shape)
        edge = 1.0 / limit
        self.ways = row_table([math.comb(6, k) for k in range(7)], shape)
        self.high_at = row_table([edge**7 * math.comb(12, k) for k in range(7)], shape)
        self.low_at = row_table([-(edge**4) * math.comb(6, k) for k in range(7)], shape)
        self.wide_at = row_table([0.0] + [edge**7 * math.comb(12, k + 6) for k in range(1, 7)], shape)
        self.near_at = jnp.where(rows == 7, inverse_powers(jnp.full(shape, limit, jnp.float32))[1], 0.0)
        count = moments.shape[2]
        lanes = lax.broadcasted_iota(jnp.int32, (ROWS, count), 1)
        self.kept = (rows_of((ROWS, count)) >= 4) == (lanes % (2 * ROWS) == 7)

    def source(self, at, line):
        region, marks, types, sources, weights, edge_terms, _ = self.refs
        rows = self.rows
        place = places(region, at)
        sigma, root = type_rows(marks, types, at, self.shape)
        charge = jnp.broadcast_to(region[(*at, slice(3, 4))], self.shape)
        scale = jnp.where(rows < 4, root, charge)
        high, middle, low = split(place * jnp.where(rows < 4, 1.0, place))
        falling = rising_powers(sigma, 6 - jnp.minimum(rows, 6))
        square = sigma * sigma
        top, rest, _ = split(self.ways * falling)
        sources[line] = stacked([high, middle, high, middle, high, low, top, rest, top, rest])
        top, rest, _ = split(place * scale)
        weights[line] = stacked([top, rest])
        first = split(falling * (self.high_at * (square * square * square) + self.low_at) + self.near_at)
        second = split(falling * self.wide_at)
        edge_terms[line] = stacked([first[0], second[0], first[1], second[1]])
        return place, sigma, scale

    def moment(self, line):
        _, _, _, _, weights, edge_terms, moments = self.refs
        both = lax.dot_general(
            weights[line],
            edge_terms[line],
            (((1,), (1,)), ((), ())),
            preferred_element_type=jnp.float32,
        )
        moments[line] = jnp.where(self.kept, both[:ROWS] + both[ROWS:], 0.0)


def prepare_own(region, marks, types, sources, weights, edge_terms, moments, distances, powers, scales):
    prepared = Preparation(region, marks, types, sources, weights, edge_terms, moments)
    rows = prepared.rows
    layers = region.shape[2] - 2
    column = [(y, z) for y in range(GRID) for z in range(layers)]

    def line_of(x, y, z):
        return ((x + 1) * (GRID + 2) + y + 1) * (layers + 2) + z + 1

    def fill(x):
        for k, (y, z) in enumerate(column):
            home, sigma, scale = prepared.source((x + 1, y + 1, z + 1), line_of(x, y, z))
            block = x * len(column) + k
            distances[block] = jnp.where(rows < 3, -2.0 * home, jnp.where(rows % 4 < 3, 1.0, 0.0))
            top, rest, _ = split(rising_powers(sigma, rows))
            powers[block] = stacked([top, top, rest, rest])
            scales[block] = 12.0 * scale

    def add(x):
        for y, z in column:
            prepared.moment(line_of(x, y, z))

    def one(x, carry):
        add(x - 1)
        fill(x)
        return carry

    fill(0)
    lax.fori_loop(1, GRID, one, 0)
    add(GRID - 1)
    blocks = GRID * len(column)
    distances[blocks] = jnp.zeros(distances.shape[1:], jnp.float32)
    powers[blocks] = jnp.zeros(powers.shape[1:], powers.dtype)


def prepare_rim(region, marks, types, sources, weights, edge_terms, moments, layers):
    prepared = Preparation(region, marks, types, sources, weights, edge_terms, moments)
    depth = layers + 2
    side = (GRID + 2) * depth
    part = -(-side // GRID)
    inner = [y * depth + z for y in range(GRID + 2) for z in range(depth)]
    inner = [k for k in inner if k // depth in (0, GRID + 1) or k % depth in (0, depth - 1)]

    def lines(index):
        ends = [jnp.minimum(index * part + k, side - 1) for k in range(part)]
        far = [k + (GRID + 1) * side for k in ends]
        return ends + far + [(index + 1) * side + k for k in inner]

    def one(index, carry):
        for line in lines(index - 1):
            prepared.moment(line)
        for line in lines(index):
            prepared.source((line,), line)
        return carry

    for line in lines(0):
        prepared.source((line,), line)
    lax.fori_loop(1, GRID, one, 0)
    for line in lines(GRID - 1):
        prepared.moment(line)


def own_line(block, layers):
    x = quotient(block, GRID * layers)
    y = remainder(quotient(block, layers), GRID)
    return ((x + 1) * (GRID + 2) + y + 1) * (layers + 2) + remainder(block, layers) + 1


def prepare_steps(offsets, shifts):
    shape = offsets.shape[1:]
    for step, cells in enumerate(itertools.product((-1, 0, 1), repeat=3)):
        moves = [cell_edge * c for c in cells]
        offsets[step] = row_table([2.0 * m for m in moves], shape)
        shifts[step] = row_table(moves + [0.0] + moves, shape)


def unpacked(pairs, index):
    entry = pairs[0, index]
    line = remainder(quotient(entry, STEPS * SHARE), LINES)
    return remainder(quotient(entry, STEPS), SHARE), line, remainder(entry, STEPS)


def pair_terms(pairs, index, sources, distances, powers, offsets, terms):
    home, line, step = unpacked(pairs, index)
    distance = distances[home] + offsets[step]
    rows = rows_of(distance.shape)
    share = jnp.where(rows < 3, 0.25, jnp.where(rows == 4, soft_core, 0.0))
    square = jnp.sum(distance * distance * share, axis=0, keepdims=True)
    distance = jnp.where(rows == 3, square, distance)
    high, middle, low = split(distance)
    near = stacked([high, high, middle, middle, low, high])
    strong = powers[home]
    width = near.shape[1]
    right = jnp.concatenate(
        [
            jnp.concatenate([near, jnp.zeros((strong.shape[0], width), near.dtype)], axis=0),
            jnp.concatenate([jnp.zeros(near.shape, near.dtype), strong], axis=0),
        ],
        axis=1,
    )
    terms[...] = lax.dot_general(
        sources[line],
        right,
        (((0,), (0,)), ((), ())),
        preferred_element_type=jnp.float32,
    )


def inverse_powers(softened):
    root = lax.rsqrt(softened)
    one = root * root
    return one, one * root


def strengths(terms, nears, strongs):
    width = terms.shape[0]
    for start in range(0, width, 16):
        rows = pl.ds(start, 16)
        one, near = inverse_powers(jnp.minimum(terms[rows, :width], limit))
        sixth = terms[rows, width:] * (near * near)
        for halves, value in ((nears, near), (strongs, one * (sixth * (sixth - 1.0)))):
            top = value.astype(jnp.bfloat16)
            halves[rows, :] = top
            halves[pl.ds(width + start, 16), :] = (value - top.astype(jnp.float32)).astype(jnp.bfloat16)


def tile_forces(pairs, index, weights, nears, strongs):
    _, line, _ = unpacked(pairs, index)
    left = weights[line]
    both = jnp.dot(
        jnp.concatenate([left, left], axis=1),
        jnp.concatenate([nears[...], strongs[...]], axis=1),
        preferred_element_type=jnp.float32,
    )
    both = both[:ROWS] + both[ROWS:]
    width = left.shape[1]
    return jnp.where(rows_of((ROWS, width)) < 4, both[:, width:], both[:, :width])


def add_forces(summed, home, line, step, moments, shifts, totals, edges):
    rows = rows_of(summed.shape)
    plain = jnp.where(rows < 4, summed[3:4], summed[7:8])
    shift = shifts[step]
    totals[home] += summed + shift * plain
    shape = moments.shape[1:]
    count = shape[1]
    plain = jnp.where(
        rows[:, :count] < 4,
        jnp.broadcast_to(moments[line, 3:4, :], shape),
        jnp.broadcast_to(moments[line, 7:8, :], shape),
    )
    edges[home] += moments[line] + shift[:, :count] * plain


def tile_loop(start, groups, pairs, sources, weights, distances, powers, offsets, slots, take):
    terms, nears, strongs = [slots[k : k + BATCH] for k in range(0, 3 * BATCH, BATCH)]

    def step(index, carry):
        first = (index - 1) * BATCH

        def push(t, lag):
            at = first - lag + t
            take(at, tile_forces(pairs, at + EDGE, weights, nears[t], strongs[t]))

        for t in range(BATCH):
            strengths(terms[t], nears[t], strongs[t])
            push((t - LAG) % BATCH, BATCH if t < LAG else 0)
            pair_terms(pairs, first + BATCH + t + EDGE, sources, distances, powers, offsets, terms[t])
        return carry

    lax.fori_loop(start, groups + 2, step, 0)


def tile_slots(width):
    return [pltpu.VMEM((width, 2 * width), jnp.float32)] * BATCH + [
        pltpu.VMEM((2 * width, width), jnp.bfloat16)
    ] * (2 * BATCH)


def force_kernel(
    table, partial, region, marks, types, _, _w, _t, _m, distances, powers, scales, offsets, shifts,
    out, sources, weights, edge_terms, moments, totals, edges, pairs, table_sem, *slots
):
    blocks = out.shape[1]
    layers = blocks // (GRID * GRID)
    totals[...] = jnp.zeros_like(totals)
    edges[...] = jnp.zeros_like(edges)
    load = pltpu.make_async_copy(table, pairs, table_sem.at[0])
    load.start()
    prepare_rim(region, marks, types, sources, weights, edge_terms, moments, layers)
    load.wait()
    count = table.shape[1] - 2 * EDGE
    early = early_tiles(count)

    def merge(index, at):
        place = early - 1 - index
        entry = pairs[0, place + EDGE]
        home, line, step = unpacked(pairs, place + EDGE)
        near = quotient(entry, STEPS * SHARE * LINES)
        summed = partial[place + 2 * BATCH]
        add_forces(summed, jnp.where(near == 1, home, blocks), line, step, moments, shifts, totals, edges)
        pairs[0, at + EDGE] = entry
        return at - (1 - near)

    first = lax.fori_loop(0, early, merge, jnp.int32(early - 1), unroll=8) + 1
    for k in range(3 * BATCH):
        pairs[0, first - 1 - k + EDGE] = blocks * STEPS

    def take(at, summed):
        home, line, step = unpacked(pairs, at + EDGE)
        add_forces(summed, home, line, step, moments, shifts, totals, edges)

    groups = -(-count // BATCH)
    tile_loop(
        quotient(first, BATCH), groups, pairs, sources, weights, distances, powers, offsets, slots, take
    )

    def finish(block, carry):
        line = own_line(block, layers)
        place = places(region, (line,))
        rows = rows_of(place.shape)
        sigma, _ = type_rows(marks, types, (line,), place.shape)
        rising = rising_powers(sigma, rows)
        square = sigma * sigma
        first = split(jnp.where(rows == 7, 1.0, rising))
        second = split(rising * (square * square * square))
        right = stacked([first[0], second[0], first[0], second[0], first[1], second[1], first[1], second[1]])
        edge = edges[block]
        left = stacked([*split(edge), jnp.zeros_like(edge)])
        both = jnp.dot(jnp.concatenate([left, left], axis=1), right, preferred_element_type=jnp.float32)
        summed = totals[block] - (both[:ROWS] + both[ROWS : 2 * ROWS] + both[2 * ROWS : 3 * ROWS])
        plain = jnp.where(rows < 4, summed[3:4], summed[7:8])
        force = (place * plain - summed) * scales[block]
        totals[block] = force + pltpu.roll(force, 4, 0)
        return carry

    lax.fori_loop(0, blocks, finish, 0, unroll=64)
    for axis in range(3):
        out[axis] = totals[:blocks, axis, :]


def brick_forces(table, partial, region, marks, types, prepared, homes, blocks):
    width = region.shape[2]
    entries = homes[0].shape[0]
    vmem = pl.BlockSpec(memory_space=pltpu.VMEM)
    return pl.pallas_call(
        force_kernel,
        out_shape=(jax.ShapeDtypeStruct((3, blocks, width), jnp.float32),)
        + tuple(jax.ShapeDtypeStruct(x.shape, x.dtype) for x in prepared),
        in_specs=[vmem] * (5 + len(prepared) + len(homes)),
        out_specs=(vmem,) * (1 + len(prepared)),
        input_output_aliases={5 + k: 1 + k for k in range(len(prepared))},
        scratch_shapes=[
            pltpu.VMEM((entries, ROWS, width), jnp.float32),
            pltpu.VMEM((entries, ROWS, 4 * ROWS), jnp.float32),
            pltpu.SMEM(table.shape, jnp.int32),
            pltpu.SemaphoreType.DMA((1,)),
        ]
        + tile_slots(width),
        compiler_params=pltpu.CompilerParams(vmem_limit_bytes=16 << 20),
    )(table, partial, region, marks, types, *prepared, *homes)[0]


def joined(coords, charges, kinds, sigma, epsilon):
    _, blocks, width = coords.shape

    def put(part, slab, row=0):
        sizes = zip((slab, row, 0), part.shape, (6, blocks, width))
        return lax.pad(part, jnp.zeros((), part.dtype), [(low, n - low - size, 0) for low, size, n in sizes])

    types = put(sigma[None, None], 5) + put(epsilon[None, None], 5, 1)
    return put(coords, 0) + put(charges, 3) + put(kinds, 4).astype(coords.dtype) + types


def per_device(coords, charges, atom_types, lj_sigma, lj_epsilon, tile_list):
    span_y = lax.axis_size("gy")
    span_z = lax.axis_size("gz")
    blocks = coords.shape[2]
    width = coords.shape[3]
    ranks = span_y * span_z
    raw = joined(coords[:, 0], charges, atom_types, lj_sigma, lj_epsilon)
    tiles = tile_list[0, 0, 0]
    region, marks, types, table, partial, *rest = exchanged(raw, tiles, ranks)
    forces = brick_forces(
        table,
        partial,
        region.reshape(-1, 4, width),
        marks.reshape(-1, 1, width),
        types,
        rest[:4],
        rest[4:],
        blocks,
    )
    return returned(forces, ranks)


def solution(mesh):
    return jax.shard_map(
        per_device,
        mesh=mesh,
        in_specs=(
            P(None, "gx", ("gy", "gz"), None),
            P("gx", ("gy", "gz"), None),
            P("gx", ("gy", "gz"), None),
            P(),
            P(),
            P("gx", "gy", "gz", None, None),
        ),
        out_specs=P(None, "gx", ("gy", "gz"), None),
        check_vma=False,
    )
```
